512 devices in a mesh: grp: 2 (over y), band: 32 (over z), mem: 4 (over x), fld: 2 (over core).
Axes of the slice: x: 4, y: 2, z: 32, core: 2. Of those that a mesh axis runs over, the one named last changes fastest.
The devices are a block of a 4x8x32 slice.
Arguments:
- surface_fields: bfloat16 [16, 8, 8, 524288], P(('grp', 'mem'), 'fld', None, 'band'), parts along dimension 0, may hold values from -8 to 8
- land_mask: int32 [524288], P('band'), may hold values from 0 to 1, as said below
- source_area: float32 [524288], P('band'), may hold values from 0.5 to 1.5
- target_area: float32 [131072], P('band'), may hold values from 0.75 to 1.25
- weight_tiles: bfloat16 [16, 128, 128], replicated, may hold values from -1 to 1
- tile_of: int32 [1024, 24], P('band'), may hold values from 0 to 15
- block_of: int32 [1024, 24], P('band'), may hold values from 0 to 191, as said below
- live_slots: int32 [1024], P('band'), may hold values from 1 to 24, as said below
Outputs:
- regridded: float32 [16, 8, 8, 131072], P(('grp', 'mem'), 'fld', None, 'band'), parts along dimension 0
- conserved: float32 [16, 8, 8], P(('grp', 'mem'), 'fld'), parts along dimension 0
- ensemble: float32 [16, 8], P(('grp', 'fld')), parts along dimension 0
The draws below stay inside these ranges and needn't reach their ends.
There are 2 independent parts, one for each index of `grp`. The reference program is written for one: setup_inputs(seed, part) draws one part's arguments, and reference() takes and returns one part's arrays. A program takes and returns all parts, laid end to end along the dimension named above; an argument that names none is the same for every part. Nothing has to cross between parts.
Inputs may be any that keep to these rules, and one draw needn't show every extreme that they name: `land_mask`: 1 marks ocean, 0 land. `block_of`: for the target block at place j (0 to 31) within its band, every entry lies in 4 * j to 4 * j + 4 + 2 * 32 - 1; values under 32 name the lower band's last blocks, values from 160 on the higher band's first blocks. `live_slots`: slots from this count on are unused.
All inputs are finite; a program needn't handle non-finite values.
Results may differ from the reference program's by a relative error of at most 0.0014.
Values may be sent and summed in bfloat16 or wider, within the bound.
A program may use at most 64 MiB of HBM per device.

```python
import jax
import jax.numpy as jnp
from jax import lax

MEMBERS = 8
FIELDS = 8
SNAPSHOTS = 8
TILE_CELLS = 128
TGT_BLK_DEV = 32
STRIDE = 4
HALO_BLK = 32
SLOT_COUNT = 24
TILE_COUNT = 16
SRC_BLK_DEV = 128
SRC_BLOCKS = 4096
TGT_BLOCKS = 1024
SRC_CELLS = 524288
TGT_CELLS = 131072


def draw_surface_fields(key, part):
    first_key, second_key, third_key = jax.random.split(key, 3)
    shape = (MEMBERS, FIELDS, SNAPSHOTS, SRC_BLOCKS, TILE_CELLS)
    offset = jax.random.uniform(first_key, (MEMBERS, FIELDS, SNAPSHOTS, 1, 1), jnp.float32, -1.0, 1.0)
    noise = jnp.clip(jax.random.normal(third_key, shape, jnp.float32), -5.0, 5.0)
    regional = 0.5 * jnp.clip(jax.random.normal(second_key, (MEMBERS, FIELDS, SNAPSHOTS, SRC_BLOCKS, 1), jnp.float32), -2.0, 2.0)
    values = offset + regional + noise
    return values.reshape(MEMBERS, FIELDS, SNAPSHOTS, SRC_CELLS).astype(jnp.bfloat16)


def draw_land_mask(key, part):
    first_key, second_key, third_key = jax.random.split(key, 3)
    band_count = SRC_CELLS // (SRC_BLK_DEV * TILE_CELLS)
    band_level = jax.random.randint(first_key, (band_count, 1, 1), 25, 101)
    region_level = jax.random.randint(second_key, (band_count, SRC_BLK_DEV, 1), 40, 101)
    cell_draw = jax.random.randint(third_key, (band_count, SRC_BLK_DEV, TILE_CELLS), 0, 10000)
    ocean = (cell_draw < band_level * region_level).astype(jnp.int32)
    return ocean.reshape(SRC_CELLS)


def draw_weight_tiles(key, part):
    fan = SLOT_COUNT * TILE_CELLS
    shape = (TILE_COUNT, TILE_CELLS, TILE_CELLS)
    noise = jnp.clip(jax.random.normal(key, shape, jnp.float32), -5.0, 5.0)
    mean_part = 1.0
    return ((mean_part + noise * jnp.sqrt(jnp.float32(fan))) / fan).astype(jnp.bfloat16)


def draw_block_of(key, part):
    position = jnp.arange(TGT_BLOCKS, dtype=jnp.int32) % TGT_BLK_DEV
    offsets = jax.random.randint(key, (TGT_BLOCKS, SLOT_COUNT), 0, STRIDE + 2 * HALO_BLK)
    picks = STRIDE * position[:, None] + offsets
    picks = picks.at[0, 0].set(0)
    picks = picks.at[TGT_BLOCKS - 1, 0].set(STRIDE * TGT_BLK_DEV + 2 * HALO_BLK - 1)
    return picks.astype(jnp.int32)


def draw_live_slots(key, part):
    first_key, second_key = jax.random.split(key, 2)
    band_count = TGT_BLOCKS // TGT_BLK_DEV
    tops = jax.random.randint(first_key, (band_count,), SLOT_COUNT // 4 + 1, SLOT_COUNT + 1)
    band_top = jnp.repeat(tops, TGT_BLK_DEV)
    counts = jax.random.randint(second_key, (TGT_BLOCKS,), 1, band_top + 1)
    return counts.at[0].set(SLOT_COUNT).astype(jnp.int32)


def set_ends(array, stream_key, least, largest):
    longest = array.shape.index(max(array.shape))
    spots = []
    for shift in (0, 1):
        where = [jax.random.randint(jax.random.fold_in(stream_key, axis), (), 0, length) for axis, length in enumerate(array.shape)]
        where[longest] = (where[longest] + shift) % array.shape[longest]
        spots.append(tuple(where))
    return array.at[spots[0]].set(least).at[spots[1]].set(largest)


def level_of(key, extent, pieces, least, high):
    factor_of, own = 1.0, jax.random.fold_in(key, 6)
    for dim, blocks in pieces:
        draws = jnp.exp(jax.random.uniform(jax.random.fold_in(own, dim), (blocks,), jnp.float32, least / len(pieces), high / len(pieces)))
        factor_of = factor_of * jnp.repeat(draws, extent[dim] // blocks).reshape([-1 if axis == dim else 1 for axis in range(len(extent))])
    return factor_of


def setup_inputs(seed: int = 0, part: int = 0) -> dict:
    splits = jax.random.split(jax.random.key(seed), 9)
    own_keys = jax.random.split(jax.random.fold_in(splits[8], part), 9)
    return {
        "surface_fields": draw_surface_fields(jax.random.fold_in(jax.random.fold_in(splits[8], part), 71), part),
        "land_mask": draw_land_mask(jax.random.fold_in(splits[8], 71), part),
        "source_area": jnp.clip(0.5 + 1.0 * jax.random.uniform(splits[2], (SRC_CELLS,), jnp.float32) ** level_of(splits[2], (SRC_CELLS,), ((0, 32),), -0.2, 0.2), 0.5, 1.5),
        "target_area": jnp.clip(0.75 + 0.5 * jax.random.uniform(splits[3], (TGT_CELLS,), jnp.float32) ** level_of(splits[3], (TGT_CELLS,), ((0, 32),), -0.2, 0.2), 0.75, 1.25),
        "weight_tiles": draw_weight_tiles(jax.random.fold_in(splits[8], 71), part),
        "tile_of": set_ends(jax.random.randint(splits[5], (TGT_BLOCKS, SLOT_COUNT), 0, TILE_COUNT), jax.random.fold_in(splits[5], 1), 0, TILE_COUNT - 1).astype(jnp.int32),
        "block_of": draw_block_of(jax.random.fold_in(splits[8], 71), part),
        "live_slots": draw_live_slots(jax.random.fold_in(splits[8], 71), part),
    }


def reference(surface_fields, land_mask, source_area, target_area, weight_tiles, tile_of, block_of, live_slots):
    columns = MEMBERS * FIELDS * SNAPSHOTS
    weighted = (source_area * land_mask.astype(jnp.float32) * surface_fields.astype(jnp.float32)).astype(jnp.bfloat16)
    flat = weighted.reshape(columns, SRC_BLOCKS, TILE_CELLS)
    padding = jnp.zeros((columns, HALO_BLK, TILE_CELLS), jnp.bfloat16)
    padded = jnp.concatenate([padding, flat, padding], axis=1)
    owner = jnp.arange(TGT_BLOCKS, dtype=jnp.int32) // TGT_BLK_DEV
    picks = (owner[:, None] * SRC_BLK_DEV + block_of).astype(jnp.int32)

    def one_slot(running, position):
        chosen = jnp.take(padded, picks[:, position], axis=1).astype(jnp.float32)
        weights = jnp.take(weight_tiles, tile_of[:, position], axis=0).astype(jnp.float32)
        usable = (position < live_slots)[:, None, None]
        weights = jnp.where(usable, weights, jnp.zeros((), jnp.float32))
        running = running + jnp.einsum("cnb,nbd->cnd", chosen, weights, precision=lax.Precision.HIGHEST)
        return running, None

    start = jnp.zeros((columns, TGT_BLOCKS, TILE_CELLS), jnp.float32)
    raw_sums, unused = lax.scan(one_slot, start, jnp.arange(SLOT_COUNT, dtype=jnp.int32))
    raw_sums = raw_sums.reshape(columns, TGT_CELLS)
    source_total = jnp.sum(weighted.reshape(columns, SRC_CELLS).astype(jnp.float32), axis=1)
    target_total = jnp.sum(raw_sums, axis=1)
    area_total = jnp.sum(target_area)
    regridded = raw_sums / target_area[None, :] + ((source_total - target_total) / area_total)[:, None]
    conserved = (source_total / area_total).reshape(MEMBERS, FIELDS, SNAPSHOTS)
    ensemble = jnp.sum(conserved, axis=0) / MEMBERS
    return regridded.reshape(MEMBERS, FIELDS, SNAPSHOTS, TGT_CELLS), conserved, ensemble
```

```python
import functools

import jax
import jax.numpy as jnp
from jax import lax
from jax.experimental import pallas as pl
from jax.experimental.pallas import tpu as pltpu
from jax.sharding import PartitionSpec as P

MESH = pl.DeviceIdType.MESH
HALO = 32
F32, BF16, I32 = jnp.float32, jnp.bfloat16, jnp.int32
HIGHEST = lax.Precision.HIGHEST
WORDS = 384


def row_dot(a, b, precision=None):
    return lax.dot_general(
        a, b, (((1,), (1,)), ((), ())), preferred_element_type=F32, precision=precision
    )


def in_three(x):
    high = jnp.round(x * 0.25) * 4.0
    rest = x - high
    mid = jnp.round(rest * 131072.0) * (1.0 / 131072.0)
    return high, mid, rest - mid


def window(n):
    return [o for o in range(1 - n // 8, n // 8 + 1) if o != 0]


def main_kernel(
    n, mems, shape,
    surf, area, mask, tarea, tiles_in, tile_of, block_of, live_in,
    scaled_out, tot_out,
    surf_v, ext, am_v, mask_v, ta_v, w_v, idx, sm, scaled, psend, prec,
    s_msg, rxm, msg1, rx1, msg2, rx2, msg3, rx3,
    lsem, ssem, isend, irecv, msend, mrecv, s1send, s1recv, s2send, s2recv, s3send, s3recv,
    pssem, prsem, relay, relay_mem,
):
    columns, own, tgt, slots, tiles, members, reach = shape
    me = lax.axis_index("band")
    my_mem = lax.axis_index("mem")

    def band(o):
        return {"band": lax.rem(me + (o + n), n)}

    def mem(o):
        return {"mem": lax.rem(my_mem + o, mems)}

    def remote(src, dst, send, recv, where):
        return pltpu.make_async_remote_copy(
            src_ref=src, dst_ref=dst, send_sem=send, recv_sem=recv,
            device_id=where, device_id_type=MESH,
        )

    def tell(sem, where):
        pl.semaphore_signal(sem, inc=1, device_id=where, device_id_type=MESH)

    barrier = pltpu.get_barrier_semaphore()
    for where in (band(-1), band(1), mem(1), mem(mems - 1)):
        tell(barrier, where)

    loads = [
        pltpu.make_async_copy(block_of, idx.at[0, 0:slots], lsem.at[0]),
        pltpu.make_async_copy(tile_of, idx.at[0, slots : 2 * slots], lsem.at[1]),
        pltpu.make_async_copy(live_in, idx.at[0, 2 * slots : 2 * slots + 1], lsem.at[2]),
        pltpu.make_async_copy(area, am_v, lsem.at[3]),
        pltpu.make_async_copy(mask, mask_v, lsem.at[4]),
        pltpu.make_async_copy(tiles_in, w_v.at[0:tiles], lsem.at[5]),
        pltpu.make_async_copy(tarea, ta_v, lsem.at[6]),
    ]
    parts = 4
    width = own * 128 // parts
    pieces = [
        pltpu.make_async_copy(
            surf.at[:, q * width : (q + 1) * width],
            surf_v.at[:, q * width : (q + 1) * width],
            ssem.at[q],
        )
        for q in range(parts)
    ]
    for c in loads[:5] + pieces[:2] + loads[5:] + pieces[2:]:
        c.start()
    w_v[tiles] = jnp.zeros((128, 128), BF16)

    pl.semaphore_wait(barrier, 4)
    steps = [1 << i for i in range((n // 4).bit_length() - 1)]
    for where in (band(-1), band(1)):
        tell(relay.at[0], where)
    for where in (mem(1), mem(mems - 1)):
        tell(relay_mem, where)

    for c in loads[:3]:
        c.wait()
    to_low = remote(idx.at[0], idx.at[2], isend.at[0], irecv.at[0], band(-1))
    to_up = remote(idx.at[0], idx.at[1], isend.at[1], irecv.at[1], band(1))
    to_low.start()
    to_up.start()
    own_scalars = pltpu.make_async_copy(idx.at[0], sm.at[0], lsem.at[0])
    own_scalars.start()

    loads[3].wait()
    loads[4].wait()
    am_v[...] = am_v[...] * mask_v[...].astype(F32)

    def weigh(s, total):
        at = pl.ds(pl.multiple_of(s * 128, 128), 128)
        value = (am_v[pl.ds(s, 1), :] * surf_v[:, at].astype(F32)).astype(BF16)
        ext[s] = value
        return total + value.astype(F32)

    s_acc = jnp.zeros((columns, 128), F32)
    for q in range(parts):
        pieces[q].wait()
        s_acc = lax.fori_loop(q * own // parts, (q + 1) * own // parts, weigh, s_acc, unroll=4)
    ones = jnp.ones((8, 128), F32)
    s_row = row_dot(ones, s_acc, HIGHEST)[0:1]
    s_msg[...] = jnp.concatenate([s_row, jnp.zeros((1, 128 - columns), F32)], axis=1)

    pl.semaphore_wait(relay.at[0], 2)
    for where in (band(-2), band(2)):
        tell(relay.at[1], where)

    loads[5].wait()
    flat_w = w_v[0:tiles].reshape(tiles * 128, 128)
    sums = row_dot(jnp.ones((8, 128), BF16), flat_w)
    row_sums = jnp.concatenate([sums[0:1, q * 128 : (q + 1) * 128] for q in range(tiles)], axis=0)

    pl.semaphore_wait(relay_mem, 2)
    to_mem = [remote(s_msg, rxm.at[my_mem], msend.at[d], mrecv.at[my_mem], mem(d)) for d in range(1, mems)]
    for c in to_mem:
        c.start()

    to_low.wait_recv()
    to_up.wait_recv()
    far_scalars = [pltpu.make_async_copy(idx.at[i], sm.at[i], lsem.at[i]) for i in (1, 2)]
    for c in far_scalars:
        c.start()

    place = lax.broadcasted_iota(I32, (slots, tgt), 0)
    lane = lax.broadcasted_iota(I32, (slots, tgt), 1)

    def listed(i):
        block = idx[i, 0:slots, :]
        tile = idx[i, slots : 2 * slots, :]
        alive = place < idx[i, 2 * slots : 2 * slots + 1, :]
        return block, jnp.where(alive, tile, -1)

    b0, w0 = listed(0)
    b1, w1 = listed(1)
    b2, w2 = listed(2)
    has_low = me > 0
    has_up = me < n - 1
    from_low = (lane >= tgt - reach) & has_low
    from_up = (lane < reach) & has_up
    blocks_ = (b0 - HALO, jnp.where(from_low, b1 - (HALO + own), b2 - HALO + own))
    tiles_ = (w0, jnp.where(from_low, w1, jnp.where(from_up, w2, -1)))

    def flat(pair):
        return jnp.concatenate([x[k : k + 1] for x in pair for k in range(slots)], axis=1)

    total_slots = 2 * slots * tgt
    block_row, tile_row = flat(blocks_), flat(tiles_)
    at_block = (lax.broadcasted_iota(I32, (own, total_slots), 0) == block_row).astype(F32).astype(BF16)
    at_tile = (lax.broadcasted_iota(I32, (tiles, total_slots), 0) == tile_row).astype(F32).astype(BF16)
    count = row_dot(at_block, at_tile)
    reach_sum = lax.dot_general(
        count, row_sums, (((1,), (0,)), ((), ())), preferred_element_type=F32, precision=HIGHEST
    )
    mask_v_f = am_v
    mask_v_f[...] = reach_sum

    def weigh_target(s, total):
        return total + ext[s].astype(F32) * mask_v_f[pl.ds(s, 1), :]

    t_acc = lax.fori_loop(0, own, weigh_target, jnp.zeros((columns, 128), F32), unroll=4)
    t_row = row_dot(ones, t_acc, HIGHEST)[0:1]

    pl.semaphore_wait(relay.at[1], 2)
    for where in (band(-4), band(4)):
        tell(relay.at[2], where)

    loads[6].wait()
    rxm[my_mem] = s_msg[...]
    for d in range(1, mems):
        other = lax.rem(my_mem + d, mems)
        remote(s_msg, rxm.at[other], msend.at[d], mrecv.at[other], mem(d)).wait_recv()
    e_row = rxm[0]
    for m in range(1, mems):
        e_row = e_row + rxm[m]
    per = columns // members
    e_sum = e_row[:, 0:per]
    for m in range(1, members):
        e_sum = e_sum + e_row[:, m * per : (m + 1) * per]
    a_sum = jnp.sum(jnp.sum(ta_v[...], axis=0, keepdims=True), axis=1, keepdims=True)
    a_high = jnp.round(a_sum * 64.0) * (1.0 / 64.0)
    s_parts, e_parts = in_three(s_row), in_three(e_sum)
    used = 4 * columns + 3 * per + 2
    msg1[...] = jnp.concatenate(
        [s_parts[0], t_row, s_parts[1], s_parts[2], *e_parts, a_high, a_sum - a_high,
         jnp.zeros((1, WORDS - used), F32)],
        axis=1,
    )

    offsets = window(n)
    first = [remote(msg1, rx1.at[i], s1send.at[i], s1recv.at[i], band(-o)) for i, o in enumerate(offsets)]
    for c in first:
        c.start()

    def slot_sum(which, t, shift, alive):
        live = sm[which, 2 * slots, t] * alive
        total = None
        for p in range(slots // 2):
            left, right = [], []
            for k in (2 * p, 2 * p + 1):
                block = sm[which, k, t] + shift
                good = (k < live) & (block >= 0) & (block < own)
                left.append(ext[jnp.clip(block, 0, own - 1)])
                right.append(w_v[jnp.where(good, sm[which, slots + k, t], tiles)])
            term = jnp.dot(
                jnp.concatenate(left, axis=1), jnp.concatenate(right, axis=0), preferred_element_type=F32
            )
            total = term if total is None else total + term
        return total

    own_scalars.wait()
    for c in far_scalars:
        c.wait()

    def part_copy(side, i):
        return remote(
            psend.at[side, i], prec.at[1 - side, i], pssem.at[side, i], prsem.at[1 - side, i],
            band(2 * side - 1),
        )

    def for_neighbours(i, carry):
        psend[0, i] = slot_sum(1, tgt - reach + i, -(HALO + own), has_low.astype(I32))
        psend[1, i] = slot_sum(2, i, own - HALO, has_up.astype(I32))

        @pl.when(i > 0)
        def _():
            part_copy(0, i - 1).start()
            part_copy(1, i - 1).start()

        return carry

    lax.fori_loop(0, reach, for_neighbours, 0)
    for side in (0, 1):
        part_copy(side, reach - 1).start()

    for c in first:
        c.wait_recv()
    running = msg1[...]
    for i in range(len(offsets)):
        running = running + rx1[i]
    msg2[...] = running
    second = [remote(msg2, rx2.at[i], s2send.at[i], s2recv.at[i], band(o)) for i, o in enumerate((-(n // 8), n // 8))]
    for c in second:
        c.start()

    def keep(t, value):
        at = pl.ds(pl.multiple_of(t * 128, 128), 128)
        scaled[:, at] = value / ta_v[pl.ds(t, 1), :]

    def inner(t, carry):
        keep(t, slot_sum(0, t, -HALO, 1))
        return carry

    def put(start, stop, sem):
        c = pltpu.make_async_copy(
            scaled.at[:, start * 128 : stop * 128], scaled_out.at[:, start * 128 : stop * 128], sem
        )
        c.start()
        return c

    lax.fori_loop(reach, tgt - reach, inner, 0)
    puts = [put(reach, tgt - reach, ssem.at[0])]

    for c in second:
        c.wait_recv()
    msg3[...] = rx2[0] + rx2[1]
    pl.semaphore_wait(relay.at[2], 2)
    third = [remote(msg3, rx3.at[i], s3send.at[i], s3recv.at[i], band(o)) for i, o in enumerate((-(n // 4), n // 4))]
    for c in third:
        c.start()

    def edge(i, carry):
        low = slot_sum(0, i, -HALO, 1)
        up = slot_sum(0, tgt - reach + i, -HALO, 1)
        part_copy(1, i).wait_recv()
        part_copy(0, i).wait_recv()
        keep(i, low + prec[0, i])
        keep(tgt - reach + i, up + prec[1, i])
        return carry

    lax.fori_loop(0, reach, edge, 0)
    puts.append(put(0, reach, ssem.at[1]))
    puts.append(put(tgt - reach, tgt, ssem.at[2]))

    for c in third:
        c.wait_recv()
    tot_out[...] = rx3[0] + rx3[1]
    for c in [to_low, to_up, *to_mem, *first, *second, *third]:
        c.wait_send()

    def sent(i, carry):
        part_copy(0, i).wait_send()
        part_copy(1, i).wait_send()
        return carry

    lax.fori_loop(0, reach, sent, 0)
    for c in puts:
        c.wait()


def last_kernel(shape, mems, tot, scaled, out, conserved, ensemble, fix):
    columns, members, fields, snaps = shape
    per = columns // members

    @pl.when(pl.program_id(0) == 0)
    def _():
        def at(start, size):
            return tot[:, start : start + size]

        base = 4 * columns
        s = (at(0, columns) + at(2 * columns, columns)) + at(3 * columns, columns)
        e = (at(base, per) + at(base + per, per)) + at(base + 2 * per, per)
        total_area = at(base + 3 * per, 1) + at(base + 3 * per + 1, 1)
        step = (s - at(columns, columns)) / total_area
        diagonal = lax.broadcasted_iota(I32, (columns, columns), 0) == lax.broadcasted_iota(
            I32, (columns, columns), 1
        )
        column = jnp.sum(jnp.where(diagonal, step, 0.0), axis=1, keepdims=True)
        fix[...] = jnp.broadcast_to(column, (columns, 128))
        mean = s / total_area
        for i in range(members * fields):
            conserved[i // fields, i % fields : i % fields + 1, :] = mean[:, i * snaps : (i + 1) * snaps]
        group = e / total_area / float(members * mems)
        for f in range(fields):
            ensemble[f : f + 1, :] = group[:, f * snaps : (f + 1) * snaps]

    for b in range(out.shape[1] // 128):
        out[:, b * 128 : (b + 1) * 128] = scaled[:, b * 128 : (b + 1) * 128] + fix[...]


def on_device(n, mems, surf, mask, area, tarea, tiles_in, tile_of, block_of, live):
    members, fields, snaps, cells = surf.shape
    columns = members * fields * snaps
    own = cells // 128
    tgt, slots = tile_of.shape
    tiles = tiles_in.shape[0]
    reach = HALO * tgt // own
    any_space = pl.BlockSpec(memory_space=pl.ANY)
    dma, plain = pltpu.SemaphoreType.DMA, pltpu.SemaphoreType.REGULAR
    rows = -(-(2 * slots + 1) // 8) * 8
    count = len(window(n))
    scaled, tot = pl.pallas_call(
        functools.partial(main_kernel, n, mems, (columns, own, tgt, slots, tiles, members, reach)),
        out_shape=(
            jax.ShapeDtypeStruct((columns, tgt * 128), F32),
            jax.ShapeDtypeStruct((1, WORDS), F32),
        ),
        in_specs=[any_space] * 8,
        out_specs=(any_space, pl.BlockSpec(memory_space=pltpu.VMEM)),
        scratch_shapes=[
            pltpu.VMEM((columns, cells), BF16),
            pltpu.VMEM((own, columns, 128), BF16),
            pltpu.VMEM((own, 128), F32),
            pltpu.VMEM((own, 128), I32),
            pltpu.VMEM((tgt, 128), F32),
            pltpu.VMEM((tiles + 1, 128, 128), BF16),
            pltpu.VMEM((3, rows, tgt), I32),
            pltpu.SMEM((3, rows, tgt), I32),
            pltpu.VMEM((columns, tgt * 128), F32),
            pltpu.VMEM((2, reach, columns, 128), F32),
            pltpu.VMEM((2, reach, columns, 128), F32),
            pltpu.VMEM((1, 128), F32),
            pltpu.VMEM((mems, 1, 128), F32),
            pltpu.VMEM((1, WORDS), F32),
            pltpu.VMEM((count, 1, WORDS), F32),
            pltpu.VMEM((1, WORDS), F32),
            pltpu.VMEM((2, 1, WORDS), F32),
            pltpu.VMEM((1, WORDS), F32),
            pltpu.VMEM((2, 1, WORDS), F32),
            dma((7,)), dma((4,)), dma((2,)), dma((2,)), dma((mems,)), dma((mems,)),
            dma((count,)), dma((count,)), dma((2,)), dma((2,)), dma((2,)), dma((2,)),
            dma((2, reach)), dma((2, reach)), plain((3,)), plain,
        ],
        compiler_params=pltpu.CompilerParams(collective_id=0, has_side_effects=True),
        name="regrid",
    )(
        surf.reshape(columns, cells),
        area.reshape(own, 128),
        mask.reshape(own, 128),
        tarea.reshape(tgt, 128),
        tiles_in,
        tile_of.T,
        block_of.T,
        live.reshape(1, tgt),
    )
    steps = 4
    wide = tgt * 128 // steps
    whole = lambda *dims: pl.BlockSpec(dims, lambda i: (0,) * len(dims))
    out, conserved, ensemble = pl.pallas_call(
        functools.partial(last_kernel, (columns, members, fields, snaps), mems),
        grid=(steps,),
        out_shape=(
            jax.ShapeDtypeStruct((columns, tgt * 128), F32),
            jax.ShapeDtypeStruct((members, fields, snaps), F32),
            jax.ShapeDtypeStruct((fields, snaps), F32),
        ),
        in_specs=[whole(1, WORDS), pl.BlockSpec((columns, wide), lambda i: (0, i))],
        out_specs=(
            pl.BlockSpec((columns, wide), lambda i: (0, i)),
            whole(members, fields, snaps),
            whole(fields, snaps),
        ),
        scratch_shapes=[pltpu.VMEM((columns, 128), F32)],
        name="finish",
    )(tot, scaled)
    return out.reshape(members, fields, snaps, tgt * 128), conserved, ensemble


def solution(mesh):
    placed = (
        P(("grp", "mem"), "fld", None, "band"),
        P("band"),
        P("band"),
        P("band"),
        P(),
        P("band", None),
        P("band", None),
        P("band"),
    )
    return jax.shard_map(
        functools.partial(on_device, mesh.shape["band"], mesh.shape["mem"]),
        mesh=mesh,
        in_specs=placed,
        out_specs=(
            P(("grp", "mem"), "fld", None, "band"),
            P(("grp", "mem"), "fld", None),
            P(("grp", "fld"), None),
        ),
        check_vma=False,
    )
```

```python
import functools

import jax
import jax.numpy as jnp
from jax import lax
from jax.experimental import pallas as pl
from jax.experimental.pallas import tpu as pltpu
from jax.sharding import PartitionSpec as P

MESH = pl.DeviceIdType.MESH
HALO = 32
F32, BF16, I32 = jnp.float32, jnp.bfloat16, jnp.int32
HIGHEST = lax.Precision.HIGHEST
WORDS = 384


def row_dot(a, b, precision=None):
    return lax.dot_general(
        a, b, (((1,), (1,)), ((), ())), preferred_element_type=F32, precision=precision
    )


def in_three(x):
    high = jnp.round(x * 0.25) * 4.0
    rest = x - high
    mid = jnp.round(rest * 131072.0) * (1.0 / 131072.0)
    return high, mid, rest - mid


def main_kernel(
    n, mems, shape,
    surf, area, mask, tarea, tiles_in, tile_of, block_of, live_in,
    scaled, tot_out,
    surf_v, ext, am_v, mask_v, ta_v, w_v, idx, sm, s_acc, reach_sum, psend, prec,
    s_msg, rxm, msg, rx, rxw, run, rxp,
    lsem, ssem, isend, irecv, msend, mrecv, dsend, drecv, wsend, wrecv, csend, crecv,
    pssem, prsem, upper_in, lower_in, mem_in,
):
    columns, own, tgt, slots, tiles, members, reach = shape
    me = lax.axis_index("band")
    my_mem = lax.axis_index("mem")
    has_low = me > 0
    has_up = me < n - 1
    half = n // 2

    def band(o):
        return {"band": me + o}

    def mem(o):
        return {"mem": lax.rem(my_mem + o, mems)}

    def remote(src, dst, send, recv, where):
        return pltpu.make_async_remote_copy(
            src_ref=src, dst_ref=dst, send_sem=send, recv_sem=recv,
            device_id=where, device_id_type=MESH,
        )

    def tell(sem, where):
        pl.semaphore_signal(sem, inc=1, device_id=where, device_id_type=MESH)

    barrier = pltpu.get_barrier_semaphore()

    @pl.when(has_low)
    def _():
        tell(barrier, band(-1))

    @pl.when(has_up)
    def _():
        tell(barrier, band(1))

    for where in (mem(1), mem(mems - 1)):
        tell(barrier, where)

    loads = [
        pltpu.make_async_copy(block_of, idx.at[0, 0:slots], lsem.at[0]),
        pltpu.make_async_copy(tile_of, idx.at[0, slots : 2 * slots], lsem.at[1]),
        pltpu.make_async_copy(live_in, idx.at[0, 2 * slots : 2 * slots + 1], lsem.at[2]),
        pltpu.make_async_copy(area, am_v, lsem.at[3]),
        pltpu.make_async_copy(mask, mask_v, lsem.at[4]),
        pltpu.make_async_copy(tiles_in, w_v.at[0:tiles], lsem.at[5]),
        pltpu.make_async_copy(tarea, ta_v, lsem.at[6]),
    ]
    parts = 4
    width = own * 128 // parts
    pieces = [
        pltpu.make_async_copy(
            surf.at[:, q * width : (q + 1) * width],
            surf_v.at[:, q * width : (q + 1) * width],
            ssem.at[q],
        )
        for q in range(parts)
    ]
    for c in loads[:5] + pieces[:2] + loads[5:] + pieces[2:]:
        c.start()
    w_v[tiles] = jnp.zeros((128, 128), BF16)
    for c in loads[:3]:
        c.wait()
    scalars = [pltpu.make_async_copy(idx.at[i], sm.at[i], lsem.at[i]) for i in range(3)]
    scalars[0].start()

    def weigh(s, total):
        at = pl.ds(pl.multiple_of(s * 128, 128), 128)
        value = (am_v[pl.ds(s, 1), :] * surf_v[:, at].astype(F32)).astype(BF16)
        ext[s] = value
        return total + value.astype(F32)

    def local_part():
        loads[3].wait()
        loads[4].wait()
        am_v[...] = am_v[...] * mask_v[...].astype(F32)
        total = jnp.zeros((columns, 128), F32)
        for q in range(parts):
            pieces[q].wait()
            total = lax.fori_loop(q * own // parts, (q + 1) * own // parts, weigh, total, unroll=4)
        s_acc[...] = total
        loads[5].wait()
        loads[6].wait()
        scalars[0].wait()

    def slot_sum(which, t, shift, alive):
        live = sm[which, 2 * slots, t] * alive
        total = None
        for p in range(slots // 2):
            left, right = [], []
            for k in (2 * p, 2 * p + 1):
                block = sm[which, k, t] + shift
                good = (k < live) & (block >= 0) & (block < own)
                left.append(ext[jnp.clip(block, 0, own - 1)])
                right.append(w_v[jnp.where(good, sm[which, slots + k, t], tiles)])
            term = jnp.dot(
                jnp.concatenate(left, axis=1), jnp.concatenate(right, axis=0), preferred_element_type=F32
            )
            total = term if total is None else total + term
        return total

    def columns_of(t):
        return pl.ds(pl.multiple_of(t * 128, 128), 128)

    def own_targets():
        def body(t, carry):
            scaled[:, columns_of(t)] = slot_sum(0, t, -HALO, 1)
            return carry

        lax.fori_loop(0, tgt, body, 0)

    @pl.when(me == 0)
    def _():
        local_part()
        own_targets()

    near = has_low.astype(I32) + has_up.astype(I32)
    pl.semaphore_wait(barrier, near + 2)
    to_low = remote(idx.at[0], idx.at[2], isend.at[0], irecv.at[0], band(-1))
    to_up = remote(idx.at[0], idx.at[1], isend.at[1], irecv.at[1], band(1))

    @pl.when(has_low)
    def _():
        to_low.start()
        tell(upper_in, band(-1))

    @pl.when(has_up)
    def _():
        to_up.start()

    for where in (mem(1), mem(mems - 1)):
        tell(mem_in, where)

    @pl.when(me > 1)
    def _():
        pl.semaphore_wait(lower_in, 1)

    @pl.when((me > 0) & has_up)
    def _():
        tell(lower_in, band(1))

    @pl.when(has_low)
    def _():
        local_part()

    @pl.when(has_low & (me < half))
    def _():
        own_targets()

    ones = jnp.ones((8, 128), F32)
    s_row = row_dot(ones, s_acc[...], HIGHEST)[0:1]
    s_msg[...] = jnp.concatenate([s_row, jnp.zeros((1, 128 - columns), F32)], axis=1)

    flat_w = w_v[0:tiles].reshape(tiles * 128, 128)
    sums = row_dot(jnp.ones((8, 128), BF16), flat_w)
    row_sums = jnp.concatenate([sums[0:1, q * 128 : (q + 1) * 128] for q in range(tiles)], axis=0)

    pl.semaphore_wait(mem_in, 2)
    to_mem = [remote(s_msg, rxm.at[my_mem], msend.at[d], mrecv.at[my_mem], mem(d)) for d in range(1, mems)]
    for c in to_mem:
        c.start()

    place = lax.broadcasted_iota(I32, (slots, tgt), 0)
    lane = lax.broadcasted_iota(I32, (slots, tgt), 1)

    def listed(i):
        block = idx[i, 0:slots, :]
        tile = idx[i, slots : 2 * slots, :]
        alive = place < idx[i, 2 * slots : 2 * slots + 1, :]
        return block, jnp.where(alive, tile, -1)

    def cell_sums(block, tile):
        count = slots * tgt
        block_row = jnp.concatenate([block[k : k + 1] for k in range(slots)], axis=1)
        tile_row = jnp.concatenate([tile[k : k + 1] for k in range(slots)], axis=1)
        at_block = (lax.broadcasted_iota(I32, (own, count), 0) == block_row).astype(F32).astype(BF16)
        at_tile = (lax.broadcasted_iota(I32, (tiles, count), 0) == tile_row).astype(F32).astype(BF16)
        return lax.dot_general(
            row_dot(at_block, at_tile), row_sums, (((1,), (0,)), ((), ())),
            preferred_element_type=F32, precision=HIGHEST,
        )

    def weigh_target(s, total):
        return total + ext[s].astype(F32) * reach_sum[pl.ds(s, 1), :]

    b0, w0 = listed(0)
    reach_sum[...] = cell_sums(b0 - HALO, w0)
    t_acc = lax.fori_loop(0, own, weigh_target, jnp.zeros((columns, 128), F32), unroll=4)

    @pl.when(has_low)
    def _():
        to_up.wait_recv()
        scalars[1].start()

    @pl.when(has_up)
    def _():
        to_low.wait_recv()
        scalars[2].start()

    b1, w1 = listed(1)
    b2, w2 = listed(2)
    from_low = (lane >= tgt - reach) & has_low
    from_up = (lane < reach) & has_up
    reach_sum[...] = cell_sums(
        jnp.where(from_low, b1 - (HALO + own), b2 - HALO + own),
        jnp.where(from_low, w1, jnp.where(from_up, w2, -1)),
    )
    t_acc = lax.fori_loop(0, HALO, weigh_target, t_acc, unroll=4)
    t_acc = lax.fori_loop(own - HALO, own, weigh_target, t_acc, unroll=4)
    t_row = row_dot(ones, t_acc, HIGHEST)[0:1]

    rxm[my_mem] = s_msg[...]
    for d in range(1, mems):
        other = lax.rem(my_mem + d, mems)
        remote(s_msg, rxm.at[other], msend.at[d], mrecv.at[other], mem(d)).wait_recv()
    e_row = rxm[0]
    for m in range(1, mems):
        e_row = e_row + rxm[m]
    per = columns // members
    e_sum = e_row[:, 0:per]
    for m in range(1, members):
        e_sum = e_sum + e_row[:, m * per : (m + 1) * per]
    a_sum = jnp.sum(jnp.sum(ta_v[...], axis=0, keepdims=True), axis=1, keepdims=True)
    a_high = jnp.round(a_sum * 64.0) * (1.0 / 64.0)
    s_parts, e_parts = in_three(s_row), in_three(e_sum)
    used = 4 * columns + 3 * per + 2
    msg[...] = jnp.concatenate(
        [s_parts[0], t_row, s_parts[1], s_parts[2], *e_parts, a_high, a_sum - a_high,
         jnp.zeros((1, WORDS - used), F32)],
        axis=1,
    )

    def direct(q):
        return remote(msg, rx.at[me], dsend.at[q], drecv.at[me], {"band": q})

    def send_down(q, carry):
        direct(q).start()
        return carry

    lax.fori_loop(0, me, send_down, 0)

    stride = n // 8

    @pl.when(has_up)
    def _():
        for _ in range(stride - 2):
            pl.semaphore_wait(upper_in, 1)

            @pl.when(has_low)
            def _():
                tell(upper_in, band(-1))

        pl.semaphore_wait(upper_in, 1)

    @pl.when(me == n - 1)
    def _():
        for _ in range(stride - 2):
            tell(upper_in, band(-1))

    ups = [remote(msg, rxw.at[o - 1], wsend.at[o - 1], wrecv.at[o - 1], band(o)) for o in range(1, stride)]
    for o, c in enumerate(ups, 1):
        pl.when(me + o < n)(c.start)

    @pl.when(has_low)
    def _():
        scalars[1].wait()

    @pl.when(has_up)
    def _():
        scalars[2].wait()

    def part_copy(side, i):
        return remote(
            psend.at[side, i], prec.at[1 - side, i], pssem.at[side, i], prsem.at[1 - side, i],
            band(2 * side - 1),
        )

    def for_side(side):
        def body(i, carry):
            if side == 0:
                psend[0, i] = slot_sum(1, tgt - reach + i, -(HALO + own), 1)
            else:
                psend[1, i] = slot_sum(2, i, own - HALO, 1)

            @pl.when(i > 0)
            def _():
                part_copy(side, i - 1).start()

            return carry

        lax.fori_loop(0, reach, body, 0)
        part_copy(side, reach - 1).start()

    pl.when(has_low)(functools.partial(for_side, 0))
    pl.when(has_up)(functools.partial(for_side, 1))

    @pl.when(me >= half)
    def _():
        own_targets()

    def add_part(side, start):
        def body(i, carry):
            part_copy(1 - side, i).wait_recv()
            at = columns_of(start + i)
            scaled[:, at] = scaled[:, at] + prec[side, i]
            return carry

        lax.fori_loop(0, reach, body, 0)

    def divide(t, carry):
        at = columns_of(t)
        scaled[:, at] = scaled[:, at] / ta_v[pl.ds(t, 1), :]
        return carry

    pl.when(has_low)(functools.partial(add_part, 0, 0))
    pl.when(has_up)(functools.partial(add_part, 1, tgt - reach))
    lax.fori_loop(0, tgt, divide, 0)

    run[...] = msg[...]
    for o, c in enumerate(ups, 1):
        @pl.when(me >= o)
        def _():
            c.wait_recv()
            run[...] = run[...] + rxw[o - 1]

    chain = remote(run, rxp, csend, crecv, band(stride))

    @pl.when(me >= stride)
    def _():
        chain.wait_recv()
        run[...] = run[...] + rxp[...]

    pl.when(me + stride < n)(chain.start)

    def add_upper(q, total):
        remote(msg, rx.at[q], dsend.at[0], drecv.at[q], {"band": q}).wait_recv()
        return total + rx[q]

    tot_out[...] = lax.fori_loop(me + 1, n, add_upper, run[...])

    def sent(q, carry):
        direct(q).wait_send()
        return carry

    lax.fori_loop(0, me, sent, 0)
    pl.when(me + stride < n)(chain.wait_send)
    for o, c in enumerate(ups, 1):
        pl.when(me + o < n)(c.wait_send)
    for c in to_mem:
        c.wait_send()

    def parts_sent(side):
        def body(i, carry):
            part_copy(side, i).wait_send()
            return carry

        lax.fori_loop(0, reach, body, 0)

    @pl.when(has_low)
    def _():
        to_low.wait_send()
        parts_sent(0)

    @pl.when(has_up)
    def _():
        to_up.wait_send()
        parts_sent(1)


def last_kernel(shape, mems, tot, scaled, out, conserved, ensemble, done, sems):
    columns, members, fields, snaps = shape
    per = columns // members

    def at(start, size):
        return tot[:, start : start + size]

    base = 4 * columns
    s = (at(0, columns) + at(2 * columns, columns)) + at(3 * columns, columns)
    e = (at(base, per) + at(base + per, per)) + at(base + 2 * per, per)
    total_area = at(base + 3 * per, 1) + at(base + 3 * per + 1, 1)
    step = (s - at(columns, columns)) / total_area
    diagonal = lax.broadcasted_iota(I32, (columns, columns), 0) == lax.broadcasted_iota(
        I32, (columns, columns), 1
    )
    fix = jnp.broadcast_to(jnp.sum(jnp.where(diagonal, step, 0.0), axis=1, keepdims=True), (columns, 128))
    pieces = 4
    width = out.shape[1] // pieces
    copies = []
    for q in range(pieces):
        for b in range(q * width // 128, (q + 1) * width // 128):
            done[:, b * 128 : (b + 1) * 128] = scaled[:, b * 128 : (b + 1) * 128] + fix
        where = (slice(None), slice(q * width, (q + 1) * width))
        copies.append(pltpu.make_async_copy(done.at[where], out.at[where], sems.at[q]))
        copies[-1].start()
    mean = s / total_area
    for i in range(members * fields):
        conserved[i // fields, i % fields : i % fields + 1, :] = mean[:, i * snaps : (i + 1) * snaps]
    group = e / total_area / float(members * mems)
    for f in range(fields):
        ensemble[f : f + 1, :] = group[:, f * snaps : (f + 1) * snaps]
    for c in copies:
        c.wait()


def on_device(n, mems, surf, mask, area, tarea, tiles_in, tile_of, block_of, live):
    members, fields, snaps, cells = surf.shape
    columns = members * fields * snaps
    own = cells // 128
    tgt, slots = tile_of.shape
    tiles = tiles_in.shape[0]
    reach = HALO * tgt // own
    any_space = pl.BlockSpec(memory_space=pl.ANY)
    dma, plain = pltpu.SemaphoreType.DMA, pltpu.SemaphoreType.REGULAR
    rows = -(-(2 * slots + 1) // 8) * 8
    stride = n // 8
    scaled, tot = pl.pallas_call(
        functools.partial(main_kernel, n, mems, (columns, own, tgt, slots, tiles, members, reach)),
        out_shape=(pltpu.VMEM((columns, tgt * 128), F32), pltpu.VMEM((1, WORDS), F32)),
        in_specs=[any_space] * 8,
        out_specs=(pl.BlockSpec(memory_space=pltpu.VMEM),) * 2,
        scratch_shapes=[
            pltpu.VMEM((columns, cells), BF16),
            pltpu.VMEM((own, columns, 128), BF16),
            pltpu.VMEM((own, 128), F32),
            pltpu.VMEM((own, 128), I32),
            pltpu.VMEM((tgt, 128), F32),
            pltpu.VMEM((tiles + 1, 128, 128), BF16),
            pltpu.VMEM((3, rows, tgt), I32),
            pltpu.SMEM((3, rows, tgt), I32),
            pltpu.VMEM((columns, 128), F32),
            pltpu.VMEM((own, 128), F32),
            pltpu.VMEM((2, reach, columns, 128), F32),
            pltpu.VMEM((2, reach, columns, 128), F32),
            pltpu.VMEM((1, 128), F32),
            pltpu.VMEM((mems, 1, 128), F32),
            pltpu.VMEM((1, WORDS), F32),
            pltpu.VMEM((n, 1, WORDS), F32),
            pltpu.VMEM((stride - 1, 1, WORDS), F32),
            pltpu.VMEM((1, WORDS), F32),
            pltpu.VMEM((1, WORDS), F32),
            dma((7,)), dma((4,)), dma((2,)), dma((2,)), dma((mems,)), dma((mems,)),
            dma((n,)), dma((n,)), dma((stride - 1,)), dma((stride - 1,)), dma, dma,
            dma((2, reach)), dma((2, reach)), plain, plain, plain,
        ],
        compiler_params=pltpu.CompilerParams(collective_id=0, has_side_effects=True),
        name="regrid",
    )(
        surf.reshape(columns, cells),
        area.reshape(own, 128),
        mask.reshape(own, 128),
        tarea.reshape(tgt, 128),
        tiles_in,
        tile_of.T,
        block_of.T,
        live.reshape(1, tgt),
    )
    inside = pl.BlockSpec(memory_space=pltpu.VMEM)
    out, conserved, ensemble = pl.pallas_call(
        functools.partial(last_kernel, (columns, members, fields, snaps), mems),
        out_shape=(
            jax.ShapeDtypeStruct((columns, tgt * 128), F32),
            jax.ShapeDtypeStruct((members, fields, snaps), F32),
            jax.ShapeDtypeStruct((fields, snaps), F32),
        ),
        in_specs=[inside, inside],
        out_specs=(any_space, inside, inside),
        scratch_shapes=[pltpu.VMEM((columns, tgt * 128), F32), dma((4,))],
        name="finish",
    )(tot, scaled)
    return out.reshape(members, fields, snaps, tgt * 128), conserved, ensemble


def solution(mesh):
    placed = (
        P(("grp", "mem"), "fld", None, "band"),
        P("band"),
        P("band"),
        P("band"),
        P(),
        P("band", None),
        P("band", None),
        P("band"),
    )
    return jax.shard_map(
        functools.partial(on_device, mesh.shape["band"], mesh.shape["mem"]),
        mesh=mesh,
        in_specs=placed,
        out_specs=(
            P(("grp", "mem"), "fld", None, "band"),
            P(("grp", "mem"), "fld", None),
            P(("grp", "fld"), None),
        ),
        check_vma=False,
    )
```

```python
import functools

import jax
import jax.numpy as jnp
from jax import lax
from jax.experimental import pallas as pl
from jax.experimental.pallas import tpu as pltpu
from jax.sharding import PartitionSpec as P

MESH = pl.DeviceIdType.MESH
HALO = 32
F32, BF16, I32 = jnp.float32, jnp.bfloat16, jnp.int32
HIGHEST = lax.Precision.HIGHEST
WORDS = 384


def row_dot(a, b, precision=None):
    return lax.dot_general(
        a, b, (((1,), (1,)), ((), ())), preferred_element_type=F32, precision=precision
    )


def in_three(x):
    high = jnp.round(x * 0.25) * 4.0
    rest = x - high
    mid = jnp.round(rest * 131072.0) * (1.0 / 131072.0)
    return high, mid, rest - mid


def main_kernel(
    n, mems, shape,
    surf, area, mask, tarea, tiles_in, tile_of, block_of, live_in,
    scaled, tot_out,
    surf_v, ext, am_v, mask_v, ta_v, w_v, idx, sm, s_acc, reach_sum, psend, prec,
    s_msg, rs0, rxm, msg, rx, mid, rxw, run, rxp,
    lsem, ssem, isend, irecv, msend, mrecv, dsend, drecv, wsend, wrecv, csend, crecv,
    pssem, prsem, zsend, zrecv, hsend, upper_in, mem_in,
):
    columns, own, tgt, slots, tiles, members, reach = shape
    me = lax.axis_index("band")
    my_mem = lax.axis_index("mem")
    has_low = me > 0
    has_up = me < n - 1

    def band(o):
        return {"band": me + o}

    def mem(o):
        return {"mem": lax.rem(my_mem + o, mems)}

    def remote(src, dst, send, recv, where):
        return pltpu.make_async_remote_copy(
            src_ref=src, dst_ref=dst, send_sem=send, recv_sem=recv,
            device_id=where, device_id_type=MESH,
        )

    def tell(sem, where):
        pl.semaphore_signal(sem, inc=1, device_id=where, device_id_type=MESH)

    stride = n // 8
    last = n - n // 4
    barrier = pltpu.get_barrier_semaphore()

    def tell_band(q, carry):
        tell(barrier, {"band": q})
        return carry

    lax.fori_loop(me + 1, jnp.where(me == 0, stride + 1, n), tell_band, 0)
    lax.fori_loop(jnp.where(me == 0, last, n), n, tell_band, 0)

    def tell_mem(m, carry):
        tell(barrier, {"mem": m})
        return carry

    lax.fori_loop(jnp.where(has_low, my_mem + 1, mems), mems, tell_mem, 0)

    loads = [
        pltpu.make_async_copy(block_of, idx.at[0, 0:slots], lsem.at[0]),
        pltpu.make_async_copy(tile_of, idx.at[0, slots : 2 * slots], lsem.at[1]),
        pltpu.make_async_copy(live_in, idx.at[0, 2 * slots : 2 * slots + 1], lsem.at[2]),
        pltpu.make_async_copy(area, am_v, lsem.at[3]),
        pltpu.make_async_copy(mask, mask_v, lsem.at[4]),
        pltpu.make_async_copy(tiles_in, w_v.at[0:tiles], lsem.at[5]),
        pltpu.make_async_copy(tarea, ta_v, lsem.at[6]),
    ]
    parts = 4
    width = own * 128 // parts
    pieces = [
        pltpu.make_async_copy(
            surf.at[:, q * width : (q + 1) * width],
            surf_v.at[:, q * width : (q + 1) * width],
            ssem.at[q],
        )
        for q in range(parts)
    ]
    for c in loads[:5] + pieces + loads[5:]:
        c.start()
    w_v[tiles] = jnp.zeros((128, 128), BF16)
    scalars = [pltpu.make_async_copy(idx.at[i], sm.at[i], lsem.at[i]) for i in range(3)]

    def own_lists():
        for c in loads[:3]:
            c.wait()
        scalars[0].start()

    def weigh(s, total):
        at = pl.ds(pl.multiple_of(s * 128, 128), 128)
        value = (am_v[pl.ds(s, 1), :] * surf_v[:, at].astype(F32)).astype(BF16)
        ext[s] = value
        return total + value.astype(F32)

    def local_part():
        loads[3].wait()
        loads[4].wait()
        am_v[...] = am_v[...] * mask_v[...].astype(F32)
        total = jnp.zeros((columns, 128), F32)
        for q in range(parts):
            pieces[q].wait()
            total = lax.fori_loop(q * own // parts, (q + 1) * own // parts, weigh, total, unroll=4)
        s_acc[...] = total
        loads[5].wait()
        loads[6].wait()

    def slot_sum(which, t, shift, alive):
        live = sm[which, 2 * slots, t] * alive
        total = None
        for p in range(slots // 2):
            left, right = [], []
            for k in (2 * p, 2 * p + 1):
                block = sm[which, k, t] + shift
                good = (k < live) & (block >= 0) & (block < own)
                left.append(ext[jnp.clip(block, 0, own - 1)])
                right.append(w_v[jnp.where(good, sm[which, slots + k, t], tiles)])
            term = jnp.dot(
                jnp.concatenate(left, axis=1), jnp.concatenate(right, axis=0), preferred_element_type=F32
            )
            total = term if total is None else total + term
        return total

    def columns_of(t):
        return pl.ds(pl.multiple_of(t * 128, 128), 128)

    def own_targets():
        def body(t, carry):
            scaled[:, columns_of(t)] = slot_sum(0, t, -HALO, 1)
            return carry

        lax.fori_loop(0, tgt, body, 0)

    early = has_low & (me <= stride)

    @pl.when(early)
    def _():
        own_lists()
        local_part()
        scalars[0].wait()
        own_targets()

    known = me - 1 + ((me <= stride) | (me >= last)).astype(I32)

    @pl.when(has_low)
    def _():
        pl.semaphore_wait(barrier, known + my_mem)

    for o in range(1, stride + 1):
        @pl.when(me >= o)
        def _():
            tell(upper_in.at[o - 1], band(-o))

    def tell_mem_back(m, carry):
        tell(mem_in.at[my_mem], {"mem": m})
        return carry

    lax.fori_loop(0, jnp.where(has_low, my_mem, 0), tell_mem_back, 0)

    pl.when(jnp.logical_not(early))(own_lists)
    to_low = remote(idx.at[0], idx.at[2], isend.at[0], irecv.at[0], band(-1))
    to_up = remote(idx.at[0], idx.at[1], isend.at[1], irecv.at[1], band(1))

    @pl.when(has_low)
    def _():
        to_low.start()

    @pl.when(has_up)
    def _():
        pl.semaphore_wait(upper_in.at[0], 1)
        to_up.start()

    pl.when(jnp.logical_not(early))(local_part)

    ones = jnp.ones((8, 128), F32)
    s_row = row_dot(ones, s_acc[...], HIGHEST)[0:1]
    s_msg[...] = jnp.concatenate([s_row, jnp.zeros((1, 128 - columns), F32)], axis=1)

    first_row = remote(s_msg, rs0, zsend, zrecv, band(1))
    pl.when(me == 0)(first_row.start)

    @pl.when(me == 1)
    def _():
        first_row.wait_recv()
        s_msg[...] = s_msg[...] + rs0[...]

    def from_mem(m, to):
        return remote(s_msg, rxm.at[m], msend.at[to], mrecv.at[m], {"mem": to})

    def others(action):
        for m in range(mems):
            pl.when(has_low & (my_mem != m))(functools.partial(action, m))

    def send_mem(m):
        @pl.when(my_mem < m)
        def _():
            pl.semaphore_wait(mem_in.at[m], 1)

        from_mem(my_mem, m).start()

    others(send_mem)

    flat_w = w_v[0:tiles].reshape(tiles * 128, 128)
    sums = row_dot(jnp.ones((8, 128), BF16), flat_w)
    row_sums = jnp.concatenate([sums[0:1, q * 128 : (q + 1) * 128] for q in range(tiles)], axis=0)

    place = lax.broadcasted_iota(I32, (slots, tgt), 0)
    lane = lax.broadcasted_iota(I32, (slots, tgt), 1)

    def listed(i):
        block = idx[i, 0:slots, :]
        tile = idx[i, slots : 2 * slots, :]
        alive = place < idx[i, 2 * slots : 2 * slots + 1, :]
        return block, jnp.where(alive, tile, -1)

    @pl.when(has_low)
    def _():
        to_up.wait_recv()
        scalars[1].start()

    @pl.when(has_up)
    def _():
        to_low.wait_recv()
        scalars[2].start()

    b0, w0 = listed(0)
    b1, w1 = listed(1)
    b2, w2 = listed(2)
    from_low = (lane >= tgt - reach) & has_low
    from_up = (lane < reach) & has_up
    pair_b = (b0 - HALO, jnp.where(from_low, b1 - (HALO + own), b2 - HALO + own))
    pair_w = (w0, jnp.where(from_low, w1, jnp.where(from_up, w2, -1)))
    count = 2 * slots * tgt
    block_row = jnp.concatenate([x[k : k + 1] for x in pair_b for k in range(slots)], axis=1)
    tile_row = jnp.concatenate([x[k : k + 1] for x in pair_w for k in range(slots)], axis=1)
    at_block = (lax.broadcasted_iota(I32, (own, count), 0) == block_row).astype(F32).astype(BF16)
    at_tile = (lax.broadcasted_iota(I32, (tiles, count), 0) == tile_row).astype(F32).astype(BF16)
    reach_sum[...] = lax.dot_general(
        row_dot(at_block, at_tile), row_sums, (((1,), (0,)), ((), ())),
        preferred_element_type=F32, precision=HIGHEST,
    )

    def weigh_target(s, total):
        return total + ext[s].astype(F32) * reach_sum[pl.ds(s, 1), :]

    t_acc = lax.fori_loop(0, own, weigh_target, jnp.zeros((columns, 128), F32), unroll=4)
    t_row = row_dot(ones, t_acc, HIGHEST)[0:1]

    rxm[my_mem] = s_msg[...]
    others(lambda m: from_mem(m, m).wait_recv())
    e_row = rxm[0]
    for m in range(1, mems):
        e_row = e_row + rxm[m]
    per = columns // members
    e_sum = e_row[:, 0:per]
    for m in range(1, members):
        e_sum = e_sum + e_row[:, m * per : (m + 1) * per]
    e_sum = jnp.where(has_low, e_sum, 0.0)
    a_sum = jnp.sum(jnp.sum(ta_v[...], axis=0, keepdims=True), axis=1, keepdims=True)
    a_high = jnp.round(a_sum * 64.0) * (1.0 / 64.0)
    s_parts, e_parts = in_three(s_row), in_three(e_sum)
    used = 4 * columns + 3 * per + 2
    msg[...] = jnp.concatenate(
        [s_parts[0], t_row, s_parts[1], s_parts[2], *e_parts, a_high, a_sum - a_high,
         jnp.zeros((1, WORDS - used), F32)],
        axis=1,
    )

    def direct(q):
        return remote(msg, rx.at[me], dsend.at[q], drecv.at[me], {"band": q})

    def send_down(q, carry):
        direct(q).start()
        return carry

    lowest = jnp.where((me == 1) | (me >= last), 0, 1)
    lax.fori_loop(lowest, me, send_down, 0)

    for o in range(2, stride + 1):
        @pl.when(me + o < n)
        def _():
            pl.semaphore_wait(upper_in.at[o - 1], 1)

    ups = [remote(msg, rxw.at[o - 1], wsend.at[o - 1], wrecv.at[o - 1], band(o)) for o in range(1, stride)]
    for o, c in enumerate(ups, 1):
        pl.when(me + o < n)(c.start)

    pl.when(jnp.logical_not(early))(scalars[0].wait)

    @pl.when(has_low)
    def _():
        scalars[1].wait()

    @pl.when(has_up)
    def _():
        scalars[2].wait()

    def part_copy(side, i):
        return remote(
            psend.at[side, i], prec.at[1 - side, i], pssem.at[side, i], prsem.at[1 - side, i],
            band(2 * side - 1),
        )

    def for_side(side):
        def body(i, carry):
            if side == 0:
                psend[0, i] = slot_sum(1, tgt - reach + i, -(HALO + own), 1)
            else:
                psend[1, i] = slot_sum(2, i, own - HALO, 1)

            @pl.when(i > 0)
            def _():
                part_copy(side, i - 1).start()

            return carry

        lax.fori_loop(0, reach, body, 0)
        part_copy(side, reach - 1).start()

    pl.when(has_low)(functools.partial(for_side, 0))
    pl.when(has_up)(functools.partial(for_side, 1))

    pl.when(jnp.logical_not(early))(own_targets)

    def add_part(side, start):
        def body(i, carry):
            part_copy(1 - side, i).wait_recv()
            at = columns_of(start + i)
            scaled[:, at] = scaled[:, at] + prec[side, i]
            return carry

        lax.fori_loop(0, reach, body, 0)

    def divide(t, carry):
        at = columns_of(t)
        scaled[:, at] = scaled[:, at] / ta_v[pl.ds(t, 1), :]
        return carry

    pl.when(has_low)(functools.partial(add_part, 0, 0))
    pl.when(has_up)(functools.partial(add_part, 1, tgt - reach))
    lax.fori_loop(0, tgt, divide, 0)

    run[...] = msg[...]
    for o, c in enumerate(ups, 1):
        @pl.when(me >= o)
        def _():
            c.wait_recv()
            run[...] = run[...] + rxw[o - 1]

    chain = remote(run, rxp, csend, crecv, band(stride))

    @pl.when(me >= stride)
    def _():
        chain.wait_recv()
        run[...] = run[...] + rxp[...]

    pl.when(me + stride < n)(chain.start)

    def add_upper(q, total):
        remote(msg, rx.at[q], dsend.at[q], drecv.at[q], {"band": q}).wait_recv()
        return total + rx[q]

    is_first = me == 0
    between = lax.fori_loop(
        jnp.where(is_first, n, me + 1), jnp.where(me < last, last, me + 1), add_upper,
        jnp.zeros((1, WORDS), F32),
    )
    mid[...] = between
    hand = remote(mid, rx.at[2], hsend, drecv.at[2], band(-1))
    pl.when(me == 1)(hand.start)
    total = lax.fori_loop(1, jnp.where(is_first, 3, 1), add_upper, run[...] + between)
    tot_out[...] = lax.fori_loop(jnp.maximum(me + 1, last), n, add_upper, total)

    def sent(q, carry):
        direct(q).wait_send()
        return carry

    lax.fori_loop(lowest, me, sent, 0)
    pl.when(me == 0)(first_row.wait_send)
    pl.when(me == 1)(hand.wait_send)
    pl.when(me + stride < n)(chain.wait_send)
    for o, c in enumerate(ups, 1):
        pl.when(me + o < n)(c.wait_send)
    others(lambda m: from_mem(my_mem, m).wait_send())

    def parts_sent(side):
        def body(i, carry):
            part_copy(side, i).wait_send()
            return carry

        lax.fori_loop(0, reach, body, 0)

    @pl.when(has_low)
    def _():
        to_low.wait_send()
        parts_sent(0)

    @pl.when(has_up)
    def _():
        to_up.wait_send()
        parts_sent(1)


def last_kernel(shape, mems, tot, scaled, out, conserved, ensemble, done, mean_v, group_v, sems):
    columns, members, fields, snaps = shape
    per = columns // members

    def at(start, size):
        return tot[:, start : start + size]

    base = 4 * columns
    s = (at(0, columns) + at(2 * columns, columns)) + at(3 * columns, columns)
    e = (at(base, per) + at(base + per, per)) + at(base + 2 * per, per)
    total_area = at(base + 3 * per, 1) + at(base + 3 * per + 1, 1)
    step = (s - at(columns, columns)) / total_area
    diagonal = lax.broadcasted_iota(I32, (columns, columns), 0) == lax.broadcasted_iota(
        I32, (columns, columns), 1
    )
    fix = jnp.broadcast_to(jnp.sum(jnp.where(diagonal, step, 0.0), axis=1, keepdims=True), (columns, 128))
    mean = s / total_area
    for i in range(members * fields):
        mean_v[i // fields, i % fields : i % fields + 1, :] = mean[:, i * snaps : (i + 1) * snaps]
    group = e / total_area / float(members * mems)
    for f in range(fields):
        group_v[f : f + 1, :] = group[:, f * snaps : (f + 1) * snaps]
    pieces = 4
    copies = [
        pltpu.make_async_copy(mean_v, conserved, sems.at[pieces]),
        pltpu.make_async_copy(group_v, ensemble, sems.at[pieces + 1]),
    ]
    for q in range(pieces):
        rows = slice(q * columns // pieces, (q + 1) * columns // pieces)
        for b in range(out.shape[1] // 128):
            done[rows, b * 128 : (b + 1) * 128] = scaled[rows, b * 128 : (b + 1) * 128] + fix[rows]
        copies.append(pltpu.make_async_copy(done.at[rows], out.at[rows], sems.at[q]))
        copies[-1].start()
        if q == 0:
            copies[0].start()
            copies[1].start()
    for c in copies:
        c.wait()


def on_device(n, mems, surf, mask, area, tarea, tiles_in, tile_of, block_of, live):
    members, fields, snaps, cells = surf.shape
    columns = members * fields * snaps
    own = cells // 128
    tgt, slots = tile_of.shape
    tiles = tiles_in.shape[0]
    reach = HALO * tgt // own
    any_space = pl.BlockSpec(memory_space=pl.ANY)
    dma, plain = pltpu.SemaphoreType.DMA, pltpu.SemaphoreType.REGULAR
    rows = -(-(2 * slots + 1) // 8) * 8
    stride = n // 8
    scaled, tot = pl.pallas_call(
        functools.partial(main_kernel, n, mems, (columns, own, tgt, slots, tiles, members, reach)),
        out_shape=(pltpu.VMEM((columns, tgt * 128), F32), pltpu.VMEM((1, WORDS), F32)),
        in_specs=[any_space] * 8,
        out_specs=(pl.BlockSpec(memory_space=pltpu.VMEM),) * 2,
        scratch_shapes=[
            pltpu.VMEM((columns, cells), BF16),
            pltpu.VMEM((own, columns, 128), BF16),
            pltpu.VMEM((own, 128), F32),
            pltpu.VMEM((own, 128), I32),
            pltpu.VMEM((tgt, 128), F32),
            pltpu.VMEM((tiles + 1, 128, 128), BF16),
            pltpu.VMEM((3, rows, tgt), I32),
            pltpu.SMEM((3, rows, tgt), I32),
            pltpu.VMEM((columns, 128), F32),
            pltpu.VMEM((own, 128), F32),
            pltpu.VMEM((2, reach, columns, 128), F32),
            pltpu.VMEM((2, reach, columns, 128), F32),
            pltpu.VMEM((1, 128), F32),
            pltpu.VMEM((1, 128), F32),
            pltpu.VMEM((mems, 1, 128), F32),
            pltpu.VMEM((1, WORDS), F32),
            pltpu.VMEM((n, 1, WORDS), F32),
            pltpu.VMEM((1, WORDS), F32),
            pltpu.VMEM((stride - 1, 1, WORDS), F32),
            pltpu.VMEM((1, WORDS), F32),
            pltpu.VMEM((1, WORDS), F32),
            dma((7,)), dma((4,)), dma((2,)), dma((2,)), dma((mems,)), dma((mems,)),
            dma((n,)), dma((n,)), dma((stride - 1,)), dma((stride - 1,)), dma, dma,
            dma((2, reach)), dma((2, reach)), dma, dma, dma, plain((stride,)), plain((mems,)),
        ],
        compiler_params=pltpu.CompilerParams(collective_id=0, has_side_effects=True),
        name="regrid",
    )(
        surf.reshape(columns, cells),
        area.reshape(own, 128),
        mask.reshape(own, 128),
        tarea.reshape(tgt, 128),
        tiles_in,
        tile_of.T,
        block_of.T,
        live.reshape(1, tgt),
    )
    inside = pl.BlockSpec(memory_space=pltpu.VMEM)
    out, conserved, ensemble = pl.pallas_call(
        functools.partial(last_kernel, (columns, members, fields, snaps), mems),
        out_shape=(
            jax.ShapeDtypeStruct((columns, tgt * 128), F32),
            jax.ShapeDtypeStruct((members, fields, snaps), F32),
            jax.ShapeDtypeStruct((fields, snaps), F32),
        ),
        in_specs=[inside, inside],
        out_specs=(any_space,) * 3,
        scratch_shapes=[
            pltpu.VMEM((columns, tgt * 128), F32),
            pltpu.VMEM((members, fields, snaps), F32),
            pltpu.VMEM((fields, snaps), F32),
            dma((6,)),
        ],
        compiler_params=pltpu.CompilerParams(vmem_limit_bytes=8 * 2**20),
        name="finish",
    )(tot, scaled)
    return out.reshape(members, fields, snaps, tgt * 128), conserved, ensemble


def solution(mesh):
    placed = (
        P(("grp", "mem"), "fld", None, "band"),
        P("band"),
        P("band"),
        P("band"),
        P(),
        P("band", None),
        P("band", None),
        P("band"),
    )
    return jax.shard_map(
        functools.partial(on_device, mesh.shape["band"], mesh.shape["mem"]),
        mesh=mesh,
        in_specs=placed,
        out_specs=(
            P(("grp", "mem"), "fld", None, "band"),
            P(("grp", "mem"), "fld", None),
            P(("grp", "fld"), None),
        ),
        check_vma=False,
    )
```

```python
import functools

import jax
import jax.numpy as jnp
from jax import lax
from jax.experimental import pallas as pl
from jax.experimental.pallas import tpu as pltpu
from jax.sharding import PartitionSpec as P

MESH = pl.DeviceIdType.MESH
HALO = 32
F32, BF16, I32 = jnp.float32, jnp.bfloat16, jnp.int32
HIGHEST = lax.Precision.HIGHEST
WORDS = 384


def row_dot(a, b, precision=None):
    return lax.dot_general(
        a, b, (((1,), (1,)), ((), ())), preferred_element_type=F32, precision=precision
    )


def in_three(x):
    high = jnp.round(x * 0.25) * 4.0
    rest = x - high
    mid = jnp.round(rest * 131072.0) * (1.0 / 131072.0)
    return high, mid, rest - mid


def main_kernel(
    n, mems, shape,
    surf, area, mask, tarea, tiles_in, tile_of, block_of, live_in,
    scaled, tot_out,
    surf_v, ext, am_v, mask_v, ta_v, w_v, idx, packed, told, local, sm, s_acc, reach_sum, psend, prec,
    s_msg, rs0, rxm, msg, msg_up, rx0, rx, mid, rxw, run, rxp,
    lsem, ssem, isend, irecv, msend, mrecv, dsend, drecv, wsend, wrecv, csend, crecv,
    pssem, prsem, zsend, zrecv, hsend, upper_in, mem_in,
):
    columns, own, tgt, slots, tiles, members, reach = shape
    me = lax.axis_index("band")
    my_mem = lax.axis_index("mem")
    has_low = me > 0
    has_up = me < n - 1
    stride = n // 8
    last = n - n // 8
    early = has_low & (me <= stride)
    late = jnp.logical_not(early)

    def band(o):
        return {"band": me + o}

    def remote(src, dst, send, recv, where):
        return pltpu.make_async_remote_copy(
            src_ref=src, dst_ref=dst, send_sem=send, recv_sem=recv,
            device_id=where, device_id_type=MESH,
        )

    def tell(sem, where):
        pl.semaphore_signal(sem, inc=1, device_id=where, device_id_type=MESH)

    barrier = pltpu.get_barrier_semaphore()

    def tell_band(q, carry):
        tell(barrier, {"band": q})
        return carry

    lax.fori_loop(me + 1, jnp.where(me == 0, 2, n), tell_band, 0)
    lax.fori_loop(jnp.where(me == 0, last, n), n, tell_band, 0)

    def tell_mem(m, carry):
        tell(barrier, {"mem": m})
        return carry

    lax.fori_loop(jnp.where(has_low, my_mem + 1, mems), mems, tell_mem, 0)

    loads = [
        pltpu.make_async_copy(block_of, idx.at[0:slots], lsem.at[0]),
        pltpu.make_async_copy(tile_of, idx.at[slots : 2 * slots], lsem.at[1]),
        pltpu.make_async_copy(live_in, idx.at[2 * slots : 2 * slots + 1], lsem.at[2]),
        pltpu.make_async_copy(area, am_v, lsem.at[3]),
        pltpu.make_async_copy(mask, mask_v, lsem.at[4]),
        pltpu.make_async_copy(tiles_in, w_v.at[0:tiles], lsem.at[5]),
        pltpu.make_async_copy(tarea, ta_v, lsem.at[6]),
    ]
    parts = 4
    width = own * 128 // parts
    pieces = [
        pltpu.make_async_copy(
            surf.at[:, q * width : (q + 1) * width],
            surf_v.at[:, q * width : (q + 1) * width],
            ssem.at[q],
        )
        for q in range(parts)
    ]
    for c in loads[:5] + pieces + loads[5:]:
        c.start()
    w_v[tiles] = jnp.zeros((128, 128), BF16)

    place = lax.broadcasted_iota(I32, (slots, tgt), 0)
    lane = lax.broadcasted_iota(I32, (slots, tgt), 1)
    scalars = [pltpu.make_async_copy(local.at[i], sm.at[i], lsem.at[i]) for i in range(3)]

    def make_local(i, word, shift, valid):
        block = (word & 255) + shift
        good = valid & (block >= 0) & (block < own)
        tile = jnp.where(good, word >> 8, tiles)
        local[i] = jnp.clip(block, 0, own - 1) + 256 * tile

    def own_lists():
        for c in loads[:3]:
            c.wait()
        alive = place < idx[2 * slots : 2 * slots + 1, :]
        word = idx[0:slots, :] + 256 * jnp.where(alive, idx[slots : 2 * slots, :], tiles)
        packed[...] = word
        make_local(0, word, -HALO, alive)
        scalars[0].start()

    def weigh(s, total):
        at = pl.ds(pl.multiple_of(s * 128, 128), 128)
        value = (am_v[pl.ds(s, 1), :] * surf_v[:, at].astype(F32)).astype(BF16)
        ext[s] = value
        return total + value.astype(F32)

    def local_part():
        loads[3].wait()
        loads[4].wait()
        am_v[...] = am_v[...] * mask_v[...].astype(F32)
        total = jnp.zeros((columns, 128), F32)
        for q in range(parts):
            pieces[q].wait()
            total = lax.fori_loop(q * own // parts, (q + 1) * own // parts, weigh, total, unroll=4)
        s_acc[...] = total
        loads[5].wait()
        loads[6].wait()

    def slot_sum(which, t):
        total = None
        for p in range(slots // 2):
            left, right = [], []
            for k in (2 * p, 2 * p + 1):
                word = sm[which, k, t]
                left.append(ext[word & 255])
                right.append(w_v[word >> 8])
            term = jnp.dot(
                jnp.concatenate(left, axis=1), jnp.concatenate(right, axis=0), preferred_element_type=F32
            )
            total = term if total is None else total + term
        return total

    def columns_of(t):
        return pl.ds(pl.multiple_of(t * 128, 128), 128)

    def own_targets():
        def body(t, carry):
            scaled[:, columns_of(t)] = slot_sum(0, t)
            return carry

        lax.fori_loop(0, tgt, body, 0)

    @pl.when(early)
    def _():
        own_lists()
        local_part()
        scalars[0].wait()
        own_targets()

    known = me - 1 + ((me == 1) | (me >= last)).astype(I32)

    @pl.when(has_low)
    def _():
        pl.semaphore_wait(barrier, known + my_mem)

    pl.when(has_low)(lambda: tell(upper_in.at[0], band(-1)))
    for o in range(2, stride + 1):
        pl.when(me > o)(functools.partial(tell, upper_in.at[o - 1], band(-o)))

    def tell_mem_back(m, carry):
        tell(mem_in.at[my_mem], {"mem": m})
        return carry

    lax.fori_loop(0, jnp.where(has_low, my_mem, 0), tell_mem_back, 0)

    pl.when(late)(own_lists)
    to_low = remote(packed, told.at[1], isend.at[0], irecv.at[0], band(-1))
    to_up = remote(packed, told.at[0], isend.at[1], irecv.at[1], band(1))
    pl.when(has_low)(to_low.start)

    @pl.when(has_up)
    def _():
        pl.semaphore_wait(upper_in.at[0], 1)
        to_up.start()

    pl.when(late)(local_part)

    ones = jnp.ones((8, 128), F32)
    s_row = row_dot(ones, s_acc[...], HIGHEST)[0:1]
    s_msg[...] = jnp.concatenate([s_row, jnp.zeros((1, 128 - columns), F32)], axis=1)

    first_row = remote(s_msg, rs0, zsend.at[0], zrecv.at[0], band(1))
    pl.when(me == 0)(first_row.start)

    @pl.when(me == 1)
    def _():
        first_row.wait_recv()
        s_msg[...] = s_msg[...] + rs0[...]

    def from_mem(m, to):
        return remote(s_msg, rxm.at[m], msend.at[to], mrecv.at[m], {"mem": to})

    def others(action, which):
        for m in range(mems):
            pl.when(has_low & which(m))(functools.partial(action, m))

    others(lambda m: from_mem(my_mem, m).start(), lambda m: my_mem > m)

    flat_w = w_v[0:tiles].reshape(tiles * 128, 128)
    sums = row_dot(jnp.ones((8, 128), BF16), flat_w)
    row_sums = jnp.concatenate([sums[0:1, q * 128 : (q + 1) * 128] for q in range(tiles)], axis=0)

    def cell_sums(word):
        row = jnp.concatenate([word[k : k + 1] for k in range(slots)], axis=1)
        count = slots * tgt
        at_block = (lax.broadcasted_iota(I32, (own, count), 0) == (row & 255)).astype(F32).astype(BF16)
        at_tile = (lax.broadcasted_iota(I32, (tiles, count), 0) == (row >> 8)).astype(F32).astype(BF16)
        return lax.dot_general(
            row_dot(at_block, at_tile), row_sums, (((1,), (0,)), ((), ())),
            preferred_element_type=F32, precision=HIGHEST,
        )

    def weigh_target(s, total):
        return total + ext[s].astype(F32) * reach_sum[pl.ds(s, 1), :]

    reach_sum[...] = cell_sums(local[0])
    t_acc = lax.fori_loop(0, own, weigh_target, jnp.zeros((columns, 128), F32), unroll=4)

    pl.when(has_low)(to_up.wait_recv)
    pl.when(has_up)(to_low.wait_recv)

    def send_higher(m):
        pl.semaphore_wait(mem_in.at[m], 1)
        from_mem(my_mem, m).start()

    others(send_higher, lambda m: my_mem < m)

    from_low = (lane >= tgt - reach) & has_low
    from_up = (lane < reach) & has_up
    make_local(1, told[0], -(HALO + own), from_low)
    make_local(2, told[1], own - HALO, from_up)
    reach_sum[...] = cell_sums(jnp.where(lane < reach, local[2], local[1]))
    t_acc = lax.fori_loop(0, HALO, weigh_target, t_acc, unroll=4)
    t_acc = lax.fori_loop(own - HALO, own, weigh_target, t_acc, unroll=4)
    t_row = row_dot(ones, t_acc, HIGHEST)[0:1]
    scalars[1].start()
    scalars[2].start()

    def part_copy(side, i):
        return remote(
            psend.at[side, i], prec.at[1 - side, i], pssem.at[side, i], prsem.at[1 - side, i],
            band(2 * side - 1),
        )

    def for_side(side):
        def body(i, carry):
            psend[side, i] = slot_sum(1 + side, i + (tgt - reach if side == 0 else 0))

            @pl.when(i > 0)
            def _():
                part_copy(side, i - 1).start()

            return carry

        lax.fori_loop(0, reach, body, 0)
        part_copy(side, reach - 1).start()

    def for_neighbours():
        pl.when(late)(scalars[0].wait)
        scalars[1].wait()
        scalars[2].wait()
        pl.when(has_low)(functools.partial(for_side, 0))
        pl.when(has_up)(functools.partial(for_side, 1))

    pl.when(me == 1)(for_neighbours)

    rxm[my_mem] = s_msg[...]
    others(lambda m: from_mem(m, m).wait_recv(), lambda m: my_mem != m)
    e_row = rxm[0]
    for m in range(1, mems):
        e_row = e_row + rxm[m]
    per = columns // members
    e_sum = e_row[:, 0:per]
    for m in range(1, members):
        e_sum = e_sum + e_row[:, m * per : (m + 1) * per]
    e_sum = jnp.where(has_low, e_sum, 0.0)
    a_sum = jnp.sum(jnp.sum(ta_v[...], axis=0, keepdims=True), axis=1, keepdims=True)
    a_high = jnp.round(a_sum * 64.0) * (1.0 / 64.0)
    s_parts, e_parts = in_three(s_row), in_three(e_sum)
    used = 4 * columns + 3 * per + 2
    msg[...] = jnp.concatenate(
        [s_parts[0], t_row, s_parts[1], s_parts[2], *e_parts, a_high, a_sum - a_high,
         jnp.zeros((1, WORDS - used), F32)],
        axis=1,
    )

    def direct(q):
        return remote(msg, rx.at[me], dsend.at[q], drecv.at[me], {"band": q})

    def send_down(q, carry):
        direct(q).start()
        return carry

    lowest = jnp.where((me == 1) | (me >= last), 0, 1)
    lax.fori_loop(lowest, me, send_down, 0)

    from_first = remote(msg, rx0, zsend.at[1], zrecv.at[1], band(1))

    pl.when(me == 0)(from_first.start)

    msg_up[...] = msg[...]

    @pl.when(me == 1)
    def _():
        from_first.wait_recv()
        msg_up[...] = msg[...] + rx0[...]

    ups = [remote(msg_up, rxw.at[o - 1], wsend.at[o - 1], wrecv.at[o - 1], band(o)) for o in range(1, stride)]
    chain = remote(run, rxp, csend, crecv, band(stride))

    def to_higher(o):
        return has_low & (me + o < n)

    def send_up(o):
        if o > 1:
            pl.semaphore_wait(upper_in.at[o - 1], 1)
        if o < stride:
            ups[o - 1].start()

    for o in range(1, stride + 1):
        pl.when(to_higher(o))(functools.partial(send_up, o))

    pl.when(me != 1)(for_neighbours)
    pl.when(late)(own_targets)

    def add_part(side, start):
        def body(i, carry):
            part_copy(1 - side, i).wait_recv()
            at = columns_of(start + i)
            scaled[:, at] = scaled[:, at] + prec[side, i]
            return carry

        lax.fori_loop(0, reach, body, 0)

    def divide(t, carry):
        at = columns_of(t)
        scaled[:, at] = scaled[:, at] / ta_v[pl.ds(t, 1), :]
        return carry

    pl.when(has_low)(functools.partial(add_part, 0, 0))
    pl.when(has_up)(functools.partial(add_part, 1, tgt - reach))
    lax.fori_loop(0, tgt, divide, 0)

    run[...] = msg_up[...]

    def add_window(o):
        ups[o - 1].wait_recv()
        run[...] = run[...] + rxw[o - 1]

    for o in range(1, stride):
        pl.when(me > o)(functools.partial(add_window, o))

    @pl.when(me > stride)
    def _():
        chain.wait_recv()
        run[...] = run[...] + rxp[...]

    pl.when(to_higher(stride))(chain.start)

    def add_upper(q, total):
        remote(msg, rx.at[q], dsend.at[q], drecv.at[q], {"band": q}).wait_recv()
        return total + rx[q]

    is_first = me == 0
    between = lax.fori_loop(
        jnp.where(is_first, n, me + 1), jnp.where(me < last, last, me + 1), add_upper,
        jnp.zeros((1, WORDS), F32),
    )
    mid[...] = between
    hand = remote(mid, rx.at[2], hsend, drecv.at[2], band(-1))
    pl.when(me == 1)(hand.start)
    total = lax.fori_loop(1, jnp.where(is_first, 3, 1), add_upper, run[...] + between)
    tot_out[...] = lax.fori_loop(jnp.maximum(me + 1, last), n, add_upper, total)

    def sent(q, carry):
        direct(q).wait_send()
        return carry

    lax.fori_loop(lowest, me, sent, 0)
    @pl.when(me == 0)
    def _():
        first_row.wait_send()
        from_first.wait_send()

    pl.when(me == 1)(hand.wait_send)
    pl.when(to_higher(stride))(chain.wait_send)
    for o in range(1, stride):
        pl.when(to_higher(o))(ups[o - 1].wait_send)
    others(lambda m: from_mem(my_mem, m).wait_send(), lambda m: my_mem != m)

    def parts_sent(side):
        def body(i, carry):
            part_copy(side, i).wait_send()
            return carry

        lax.fori_loop(0, reach, body, 0)

    @pl.when(has_low)
    def _():
        to_low.wait_send()
        parts_sent(0)

    @pl.when(has_up)
    def _():
        to_up.wait_send()
        parts_sent(1)


def last_kernel(shape, mems, tot, scaled, out, conserved, ensemble, done, mean_v, group_v, sems):
    columns, members, fields, snaps = shape
    per = columns // members

    def at(start, size):
        return tot[:, start : start + size]

    base = 4 * columns
    s = (at(0, columns) + at(2 * columns, columns)) + at(3 * columns, columns)
    e = (at(base, per) + at(base + per, per)) + at(base + 2 * per, per)
    total_area = at(base + 3 * per, 1) + at(base + 3 * per + 1, 1)
    step = (s - at(columns, columns)) / total_area
    diagonal = lax.broadcasted_iota(I32, (columns, columns), 0) == lax.broadcasted_iota(
        I32, (columns, columns), 1
    )
    fix = jnp.broadcast_to(jnp.sum(jnp.where(diagonal, step, 0.0), axis=1, keepdims=True), (columns, 128))
    mean = s / total_area
    for i in range(members * fields):
        mean_v[i // fields, i % fields : i % fields + 1, :] = mean[:, i * snaps : (i + 1) * snaps]
    group = e / total_area / float(members * mems)
    for f in range(fields):
        group_v[f : f + 1, :] = group[:, f * snaps : (f + 1) * snaps]
    pieces = 4
    copies = [
        pltpu.make_async_copy(mean_v, conserved, sems.at[pieces]),
        pltpu.make_async_copy(group_v, ensemble, sems.at[pieces + 1]),
    ]
    for q in range(pieces):
        rows = slice(q * columns // pieces, (q + 1) * columns // pieces)
        for b in range(out.shape[1] // 128):
            done[rows, b * 128 : (b + 1) * 128] = scaled[rows, b * 128 : (b + 1) * 128] + fix[rows]
        copies.append(pltpu.make_async_copy(done.at[rows], out.at[rows], sems.at[q]))
        copies[-1].start()
        if q == 0:
            copies[0].start()
            copies[1].start()
    for c in copies:
        c.wait()


def on_device(n, mems, surf, mask, area, tarea, tiles_in, tile_of, block_of, live):
    members, fields, snaps, cells = surf.shape
    columns = members * fields * snaps
    own = cells // 128
    tgt, slots = tile_of.shape
    tiles = tiles_in.shape[0]
    reach = HALO * tgt // own
    any_space = pl.BlockSpec(memory_space=pl.ANY)
    dma, plain = pltpu.SemaphoreType.DMA, pltpu.SemaphoreType.REGULAR
    rows = -(-(2 * slots + 1) // 8) * 8
    stride = n // 8
    scaled, tot = pl.pallas_call(
        functools.partial(main_kernel, n, mems, (columns, own, tgt, slots, tiles, members, reach)),
        out_shape=(pltpu.VMEM((columns, tgt * 128), F32), pltpu.VMEM((1, WORDS), F32)),
        in_specs=[any_space] * 8,
        out_specs=(pl.BlockSpec(memory_space=pltpu.VMEM),) * 2,
        scratch_shapes=[
            pltpu.VMEM((columns, cells), BF16),
            pltpu.VMEM((own, columns, 128), BF16),
            pltpu.VMEM((own, 128), F32),
            pltpu.VMEM((own, 128), I32),
            pltpu.VMEM((tgt, 128), F32),
            pltpu.VMEM((tiles + 1, 128, 128), BF16),
            pltpu.VMEM((rows, tgt), I32),
            pltpu.VMEM((slots, tgt), I32),
            pltpu.VMEM((2, slots, tgt), I32),
            pltpu.VMEM((3, slots, tgt), I32),
            pltpu.SMEM((3, slots, tgt), I32),
            pltpu.VMEM((columns, 128), F32),
            pltpu.VMEM((own, 128), F32),
            pltpu.VMEM((2, reach, columns, 128), F32),
            pltpu.VMEM((2, reach, columns, 128), F32),
            pltpu.VMEM((1, 128), F32),
            pltpu.VMEM((1, 128), F32),
            pltpu.VMEM((mems, 1, 128), F32),
            pltpu.VMEM((1, WORDS), F32),
            pltpu.VMEM((1, WORDS), F32),
            pltpu.VMEM((1, WORDS), F32),
            pltpu.VMEM((n, 1, WORDS), F32),
            pltpu.VMEM((1, WORDS), F32),
            pltpu.VMEM((stride - 1, 1, WORDS), F32),
            pltpu.VMEM((1, WORDS), F32),
            pltpu.VMEM((1, WORDS), F32),
            dma((7,)), dma((4,)), dma((2,)), dma((2,)), dma((mems,)), dma((mems,)),
            dma((n,)), dma((n,)), dma((stride - 1,)), dma((stride - 1,)), dma, dma,
            dma((2, reach)), dma((2, reach)), dma((2,)), dma((2,)), dma, plain((stride,)), plain((mems,)),
        ],
        compiler_params=pltpu.CompilerParams(collective_id=0, has_side_effects=True),
        name="regrid",
    )(
        surf.reshape(columns, cells),
        area.reshape(own, 128),
        mask.reshape(own, 128),
        tarea.reshape(tgt, 128),
        tiles_in,
        tile_of.T,
        block_of.T,
        live.reshape(1, tgt),
    )
    inside = pl.BlockSpec(memory_space=pltpu.VMEM)
    out, conserved, ensemble = pl.pallas_call(
        functools.partial(last_kernel, (columns, members, fields, snaps), mems),
        out_shape=(
            jax.ShapeDtypeStruct((columns, tgt * 128), F32),
            jax.ShapeDtypeStruct((members, fields, snaps), F32),
            jax.ShapeDtypeStruct((fields, snaps), F32),
        ),
        in_specs=[inside, inside],
        out_specs=(any_space,) * 3,
        scratch_shapes=[
            pltpu.VMEM((columns, tgt * 128), F32),
            pltpu.VMEM((members, fields, snaps), F32),
            pltpu.VMEM((fields, snaps), F32),
            dma((6,)),
        ],
        compiler_params=pltpu.CompilerParams(vmem_limit_bytes=8 * 2**20),
        name="finish",
    )(tot, scaled)
    return out.reshape(members, fields, snaps, tgt * 128), conserved, ensemble


def solution(mesh):
    placed = (
        P(("grp", "mem"), "fld", None, "band"),
        P("band"),
        P("band"),
        P("band"),
        P(),
        P("band", None),
        P("band", None),
        P("band"),
    )
    return jax.shard_map(
        functools.partial(on_device, mesh.shape["band"], mesh.shape["mem"]),
        mesh=mesh,
        in_specs=placed,
        out_specs=(
            P(("grp", "mem"), "fld", None, "band"),
            P(("grp", "mem"), "fld", None),
            P(("grp", "fld"), None),
        ),
        check_vma=False,
    )
```

```python
import functools

import jax
import jax.numpy as jnp
from jax import lax
from jax.experimental import pallas as pl
from jax.experimental.pallas import tpu as pltpu
from jax.sharding import PartitionSpec as P

MESH = pl.DeviceIdType.MESH
HALO = 32
F32, BF16, I32 = jnp.float32, jnp.bfloat16, jnp.int32
HIGHEST = lax.Precision.HIGHEST
WORDS = 384


def row_dot(a, b, precision=None):
    return lax.dot_general(
        a, b, (((1,), (1,)), ((), ())), preferred_element_type=F32, precision=precision
    )


def in_three(x):
    high = jnp.round(x * 0.25) * 4.0
    rest = x - high
    mid = jnp.round(rest * 131072.0) * (1.0 / 131072.0)
    return high, mid, rest - mid


def main_kernel(
    n, mems, shape,
    surf, area, mask, tarea, tiles_in, tile_of, block_of, live_in,
    scaled, tot_out,
    surf_v, ext, am_v, mask_v, ta_v, w_v, idx, packed, told, local, sm, s_acc, reach_sum, psend, prec,
    s_msg, rs0, rxm, msg, msg_up, rx0, rx, mid, rxw, run, rxp,
    lsem, ssem, isend, irecv, msend, mrecv, dsend, drecv, wsend, wrecv, csend, crecv,
    pssem, prsem, zsend, zrecv, hsend, upper_in, mem_in,
):
    columns, own, tgt, slots, tiles, members, reach = shape
    me = lax.axis_index("band")
    my_mem = lax.axis_index("mem")
    has_low = me > 0
    has_up = me < n - 1
    stride = n // 8
    via = (lax.axis_index("grp") == 0) & (my_mem == 0) & (lax.axis_index("fld") == 0)
    last = jnp.where(via, n, 2)
    early = has_low & (me <= stride)
    late = jnp.logical_not(early)

    def band(o):
        return {"band": me + o}

    def remote(src, dst, send, recv, where):
        return pltpu.make_async_remote_copy(
            src_ref=src, dst_ref=dst, send_sem=send, recv_sem=recv,
            device_id=where, device_id_type=MESH,
        )

    def tell(sem, where):
        pl.semaphore_signal(sem, inc=1, device_id=where, device_id_type=MESH)

    barrier = pltpu.get_barrier_semaphore()

    def tell_band(q, carry):
        tell(barrier, {"band": q})
        return carry

    lax.fori_loop(me + 1, jnp.where(me == 0, 2, n), tell_band, 0)
    lax.fori_loop(jnp.where(me == 0, last, n), n, tell_band, 0)

    def tell_mem(m, carry):
        tell(barrier, {"mem": m})
        return carry

    lax.fori_loop(jnp.where(has_low, my_mem + 1, mems), mems, tell_mem, 0)

    loads = [
        pltpu.make_async_copy(block_of, idx.at[0:slots], lsem.at[0]),
        pltpu.make_async_copy(tile_of, idx.at[slots : 2 * slots], lsem.at[1]),
        pltpu.make_async_copy(live_in, idx.at[2 * slots : 2 * slots + 1], lsem.at[2]),
        pltpu.make_async_copy(area, am_v, lsem.at[3]),
        pltpu.make_async_copy(mask, mask_v, lsem.at[4]),
        pltpu.make_async_copy(tiles_in, w_v.at[0:tiles], lsem.at[5]),
        pltpu.make_async_copy(tarea, ta_v, lsem.at[6]),
    ]
    parts = 4
    width = own * 128 // parts
    pieces = [
        pltpu.make_async_copy(
            surf.at[:, q * width : (q + 1) * width],
            surf_v.at[:, q * width : (q + 1) * width],
            ssem.at[q],
        )
        for q in range(parts)
    ]
    for c in loads[:5] + pieces + loads[5:]:
        c.start()
    w_v[tiles] = jnp.zeros((128, 128), BF16)

    place = lax.broadcasted_iota(I32, (slots, tgt), 0)
    lane = lax.broadcasted_iota(I32, (slots, tgt), 1)
    scalars = [pltpu.make_async_copy(local.at[i], sm.at[i], lsem.at[i]) for i in range(3)]

    def make_local(i, word, shift, valid):
        block = (word & 255) + shift
        good = valid & (block >= 0) & (block < own)
        tile = jnp.where(good, word >> 8, tiles)
        local[i] = jnp.clip(block, 0, own - 1) + 256 * tile

    def own_lists():
        for c in loads[:3]:
            c.wait()
        alive = place < idx[2 * slots : 2 * slots + 1, :]
        word = idx[0:slots, :] + 256 * jnp.where(alive, idx[slots : 2 * slots, :], tiles)
        packed[...] = word
        make_local(0, word, -HALO, alive)
        scalars[0].start()

    def weigh(s, total):
        at = pl.ds(pl.multiple_of(s * 128, 128), 128)
        value = (am_v[pl.ds(s, 1), :] * surf_v[:, at].astype(F32)).astype(BF16)
        ext[s] = value
        return total + value.astype(F32)

    def local_part():
        loads[3].wait()
        loads[4].wait()
        am_v[...] = am_v[...] * mask_v[...].astype(F32)
        total = jnp.zeros((columns, 128), F32)
        for q in range(parts):
            pieces[q].wait()
            total = lax.fori_loop(q * own // parts, (q + 1) * own // parts, weigh, total, unroll=4)
        s_acc[...] = total
        loads[5].wait()
        loads[6].wait()

    def slot_sum(which, t):
        total = None
        for p in range(slots // 2):
            left, right = [], []
            for k in (2 * p, 2 * p + 1):
                word = sm[which, k, t]
                left.append(ext[word & 255])
                right.append(w_v[word >> 8])
            term = jnp.dot(
                jnp.concatenate(left, axis=1), jnp.concatenate(right, axis=0), preferred_element_type=F32
            )
            total = term if total is None else total + term
        return total

    def columns_of(t):
        return pl.ds(pl.multiple_of(t * 128, 128), 128)

    def own_targets():
        def body(t, carry):
            scaled[:, columns_of(t)] = slot_sum(0, t)
            return carry

        lax.fori_loop(0, tgt, body, 0)

    @pl.when(early)
    def _():
        own_lists()
        local_part()
        scalars[0].wait()
        own_targets()

    known = me - 1 + ((me == 1) | (me >= last)).astype(I32)

    @pl.when(has_low)
    def _():
        pl.semaphore_wait(barrier, known + my_mem)

    pl.when(has_low)(lambda: tell(upper_in.at[0], band(-1)))
    for o in range(2, stride + 1):
        pl.when(me > o)(functools.partial(tell, upper_in.at[o - 1], band(-o)))

    def tell_mem_back(m, carry):
        tell(mem_in.at[my_mem], {"mem": m})
        return carry

    lax.fori_loop(0, jnp.where(has_low, my_mem, 0), tell_mem_back, 0)

    pl.when(late)(own_lists)
    to_low = remote(packed, told.at[1], isend.at[0], irecv.at[0], band(-1))
    to_up = remote(packed, told.at[0], isend.at[1], irecv.at[1], band(1))
    pl.when(has_low)(to_low.start)

    pl.when(late)(local_part)

    ones = jnp.ones((8, 128), F32)
    s_row = row_dot(ones, s_acc[...], HIGHEST)[0:1]
    s_msg[...] = jnp.concatenate([s_row, jnp.zeros((1, 128 - columns), F32)], axis=1)

    first_row = remote(s_msg, rs0, zsend.at[0], zrecv.at[0], band(1))

    @pl.when(me == 0)
    def _():
        pl.semaphore_wait(upper_in.at[0], 1)
        first_row.start()


    @pl.when(me == 1)
    def _():
        first_row.wait_recv()
        s_msg[...] = s_msg[...] + rs0[...]

    def from_mem(m, to):
        return remote(s_msg, rxm.at[m], msend.at[to], mrecv.at[m], {"mem": to})

    def others(action, which):
        for m in range(mems):
            pl.when(has_low & which(m))(functools.partial(action, m))

    others(lambda m: from_mem(my_mem, m).start(), lambda m: my_mem > m)

    flat_w = w_v[0:tiles].reshape(tiles * 128, 128)
    sums = row_dot(jnp.ones((8, 128), BF16), flat_w)
    row_sums = jnp.concatenate([sums[0:1, q * 128 : (q + 1) * 128] for q in range(tiles)], axis=0)

    @pl.when(has_low & has_up)
    def _():
        pl.semaphore_wait(upper_in.at[0], 1)

    pl.when(has_up)(to_up.start)

    def cell_sums(word):
        row = jnp.concatenate([word[k : k + 1] for k in range(slots)], axis=1)
        count = slots * tgt
        at_block = (lax.broadcasted_iota(I32, (own, count), 0) == (row & 255)).astype(F32).astype(BF16)
        at_tile = (lax.broadcasted_iota(I32, (tiles, count), 0) == (row >> 8)).astype(F32).astype(BF16)
        return lax.dot_general(
            row_dot(at_block, at_tile), row_sums, (((1,), (0,)), ((), ())),
            preferred_element_type=F32, precision=HIGHEST,
        )

    def weigh_target(s, total):
        return total + ext[s].astype(F32) * reach_sum[pl.ds(s, 1), :]

    reach_sum[...] = cell_sums(local[0])
    t_acc = lax.fori_loop(0, own, weigh_target, jnp.zeros((columns, 128), F32), unroll=4)

    pl.when(has_low)(to_up.wait_recv)
    pl.when(has_up)(to_low.wait_recv)

    def send_higher(m):
        pl.semaphore_wait(mem_in.at[m], 1)
        from_mem(my_mem, m).start()

    others(send_higher, lambda m: my_mem < m)

    from_low = (lane >= tgt - reach) & has_low
    from_up = (lane < reach) & has_up
    make_local(1, told[0], -(HALO + own), from_low)
    make_local(2, told[1], own - HALO, from_up)
    reach_sum[...] = cell_sums(jnp.where(lane < reach, local[2], local[1]))
    t_acc = lax.fori_loop(0, HALO, weigh_target, t_acc, unroll=4)
    t_acc = lax.fori_loop(own - HALO, own, weigh_target, t_acc, unroll=4)
    t_row = row_dot(ones, t_acc, HIGHEST)[0:1]
    scalars[1].start()
    scalars[2].start()

    chunk = 2

    def part_copy(side, j):
        at = pl.ds(chunk * j, chunk)
        return remote(
            psend.at[side, at], prec.at[1 - side, at], pssem.at[side, j], prsem.at[1 - side, j],
            band(2 * side - 1),
        )

    def for_side(side):
        def body(i, carry):
            psend[side, i] = slot_sum(1 + side, i + (tgt - reach if side == 0 else 0))

            @pl.when((i > 0) & (lax.rem(i, chunk) == 0))
            def _():
                part_copy(side, lax.div(i, chunk) - 1).start()

            return carry

        lax.fori_loop(0, reach, body, 0)
        part_copy(side, reach // chunk - 1).start()

    def for_neighbours():
        pl.when(late)(scalars[0].wait)
        scalars[1].wait()
        scalars[2].wait()
        pl.when(has_low)(functools.partial(for_side, 0))
        pl.when(has_up)(functools.partial(for_side, 1))

    pl.when(me == 1)(for_neighbours)

    rxm[my_mem] = s_msg[...]
    others(lambda m: from_mem(m, m).wait_recv(), lambda m: my_mem != m)
    e_row = rxm[0]
    for m in range(1, mems):
        e_row = e_row + rxm[m]
    per = columns // members
    e_sum = e_row[:, 0:per]
    for m in range(1, members):
        e_sum = e_sum + e_row[:, m * per : (m + 1) * per]
    e_sum = jnp.where(has_low, e_sum, 0.0)
    a_sum = jnp.sum(jnp.sum(ta_v[...], axis=0, keepdims=True), axis=1, keepdims=True)
    a_high = jnp.round(a_sum * 64.0) * (1.0 / 64.0)
    s_parts, e_parts = in_three(s_row), in_three(e_sum)
    used = 4 * columns + 3 * per + 2
    msg[...] = jnp.concatenate(
        [s_parts[0], t_row, s_parts[1], s_parts[2], *e_parts, a_high, a_sum - a_high,
         jnp.zeros((1, WORDS - used), F32)],
        axis=1,
    )

    group, ways = 4, 8

    def direct(q):
        return remote(
            msg, rx.at[me], dsend.at[lax.rem(q, ways)], drecv.at[lax.div(me, group)], {"band": q}
        )

    lowest = jnp.where((me == 1) | (me >= last), 0, 1)

    def send_down(q, carry):
        @pl.when(q - ways >= lowest)
        def _():
            direct(q - ways).wait_send()

        direct(q).start()
        return carry

    lax.fori_loop(lowest, me, send_down, 0)

    from_first = remote(msg, rx0, zsend.at[1], zrecv.at[1], band(1))

    pl.when(me == 0)(from_first.start)

    msg_up[...] = msg[...]

    @pl.when(me == 1)
    def _():
        from_first.wait_recv()
        msg_up[...] = msg[...] + rx0[...]

    ups = [remote(msg_up, rxw.at[o - 1], wsend.at[o - 1], wrecv.at[o - 1], band(o)) for o in range(1, stride)]
    chain = remote(run, rxp, csend, crecv, band(stride))

    def to_higher(o):
        return has_low & (me + o < n)

    def send_up(o):
        if o > 1:
            pl.semaphore_wait(upper_in.at[o - 1], 1)
        if o < stride:
            ups[o - 1].start()

    for o in range(1, stride + 1):
        pl.when(to_higher(o))(functools.partial(send_up, o))

    pl.when(me != 1)(for_neighbours)
    pl.when(late)(own_targets)

    def add_part(side, start):
        def body(j, carry):
            part_copy(1 - side, j).wait_recv()
            for i in range(chunk):
                at = columns_of(start + chunk * j + i)
                scaled[:, at] = scaled[:, at] + prec[side, chunk * j + i]
            return carry

        lax.fori_loop(0, reach // chunk, body, 0)

    def divide(t, carry):
        at = columns_of(t)
        scaled[:, at] = scaled[:, at] / ta_v[pl.ds(t, 1), :]
        return carry

    pl.when(has_low)(functools.partial(add_part, 0, 0))
    pl.when(has_up)(functools.partial(add_part, 1, tgt - reach))
    lax.fori_loop(0, tgt, divide, 0)

    run[...] = msg_up[...]

    def add_window(o):
        ups[o - 1].wait_recv()
        run[...] = run[...] + rxw[o - 1]

    for o in range(1, stride):
        pl.when(me > o)(functools.partial(add_window, o))

    @pl.when(me > stride)
    def _():
        chain.wait_recv()
        run[...] = run[...] + rxp[...]

    pl.when(to_higher(stride))(chain.start)

    def sent(q, carry):
        direct(q).wait_send()
        return carry

    lax.fori_loop(jnp.maximum(lowest, me - ways), me, sent, 0)

    @pl.when(me == 0)
    def _():
        first_row.wait_send()
        from_first.wait_send()

    pl.when(to_higher(stride))(chain.wait_send)
    for o in range(1, stride):
        pl.when(to_higher(o))(ups[o - 1].wait_send)
    others(lambda m: from_mem(my_mem, m).wait_send(), lambda m: my_mem != m)

    def parts_sent(side):
        for j in range(reach // chunk):
            part_copy(side, j).wait_send()

    @pl.when(has_low)
    def _():
        to_low.wait_send()
        parts_sent(0)

    @pl.when(has_up)
    def _():
        to_up.wait_send()
        parts_sent(1)

    def arrived(start, count, g):
        at = rx.at[pl.ds(start, count)]
        remote(at, at, dsend.at[0], drecv.at[g], {"band": lax.rem(me + 1, n)}).wait_recv()
        for i in range(count):
            mid[...] = mid[...] + rx[start + i]

    mine = lax.div(me, group)
    near = jnp.where(via & (me == 0), 2, group - 1 - lax.rem(me, group))
    mid[...] = jnp.zeros((1, WORDS), F32)
    for count in range(1, group):
        pl.when(near == count)(functools.partial(arrived, me + 1, count, mine))

    def add_group(g, carry):
        arrived(group * g, group, g)
        return carry

    lax.fori_loop(jnp.where(via & (me == 0), n // group, mine + 1), n // group, add_group, 0)

    hand = remote(mid, rx.at[2], hsend, drecv.at[0], band(-1))
    pl.when(via & (me == 1))(hand.start)
    tot_out[...] = run[...] + mid[...]
    pl.when(via & (me == 1))(hand.wait_send)


def last_kernel(shape, mems, tot, scaled, out, conserved, ensemble, done, mean_v, group_v, sems):
    columns, members, fields, snaps = shape
    per = columns // members

    def at(start, size):
        return tot[:, start : start + size]

    base = 4 * columns
    s = (at(0, columns) + at(2 * columns, columns)) + at(3 * columns, columns)
    e = (at(base, per) + at(base + per, per)) + at(base + 2 * per, per)
    total_area = at(base + 3 * per, 1) + at(base + 3 * per + 1, 1)
    step = (s - at(columns, columns)) / total_area
    diagonal = lax.broadcasted_iota(I32, (columns, columns), 0) == lax.broadcasted_iota(
        I32, (columns, columns), 1
    )
    fix = jnp.broadcast_to(jnp.sum(jnp.where(diagonal, step, 0.0), axis=1, keepdims=True), (columns, 128))
    mean = s / total_area
    for i in range(members * fields):
        mean_v[i // fields, i % fields : i % fields + 1, :] = mean[:, i * snaps : (i + 1) * snaps]
    group = e / total_area / float(members * mems)
    for f in range(fields):
        group_v[f : f + 1, :] = group[:, f * snaps : (f + 1) * snaps]
    pieces = 4
    copies = [
        pltpu.make_async_copy(mean_v, conserved, sems.at[pieces]),
        pltpu.make_async_copy(group_v, ensemble, sems.at[pieces + 1]),
    ]
    for q in range(pieces):
        rows = slice(q * columns // pieces, (q + 1) * columns // pieces)
        for b in range(out.shape[1] // 128):
            done[rows, b * 128 : (b + 1) * 128] = scaled[rows, b * 128 : (b + 1) * 128] + fix[rows]
        copies.append(pltpu.make_async_copy(done.at[rows], out.at[rows], sems.at[q]))
        copies[-1].start()
        if q == 0:
            copies[0].start()
            copies[1].start()
    for c in copies:
        c.wait()


def on_device(n, mems, surf, mask, area, tarea, tiles_in, tile_of, block_of, live):
    members, fields, snaps, cells = surf.shape
    columns = members * fields * snaps
    own = cells // 128
    tgt, slots = tile_of.shape
    tiles = tiles_in.shape[0]
    reach = HALO * tgt // own
    any_space = pl.BlockSpec(memory_space=pl.ANY)
    dma, plain = pltpu.SemaphoreType.DMA, pltpu.SemaphoreType.REGULAR
    rows = -(-(2 * slots + 1) // 8) * 8
    stride = n // 8
    scaled, tot = pl.pallas_call(
        functools.partial(main_kernel, n, mems, (columns, own, tgt, slots, tiles, members, reach)),
        out_shape=(pltpu.VMEM((columns, tgt * 128), F32), pltpu.VMEM((1, WORDS), F32)),
        in_specs=[any_space] * 8,
        out_specs=(pl.BlockSpec(memory_space=pltpu.VMEM),) * 2,
        scratch_shapes=[
            pltpu.VMEM((columns, cells), BF16),
            pltpu.VMEM((own, columns, 128), BF16),
            pltpu.VMEM((own, 128), F32),
            pltpu.VMEM((own, 128), I32),
            pltpu.VMEM((tgt, 128), F32),
            pltpu.VMEM((tiles + 1, 128, 128), BF16),
            pltpu.VMEM((rows, tgt), I32),
            pltpu.VMEM((slots, tgt), I32),
            pltpu.VMEM((2, slots, tgt), I32),
            pltpu.VMEM((3, slots, tgt), I32),
            pltpu.SMEM((3, slots, tgt), I32),
            pltpu.VMEM((columns, 128), F32),
            pltpu.VMEM((own, 128), F32),
            pltpu.VMEM((2, reach, columns, 128), F32),
            pltpu.VMEM((2, reach, columns, 128), F32),
            pltpu.VMEM((1, 128), F32),
            pltpu.VMEM((1, 128), F32),
            pltpu.VMEM((mems, 1, 128), F32),
            pltpu.VMEM((1, WORDS), F32),
            pltpu.VMEM((1, WORDS), F32),
            pltpu.VMEM((1, WORDS), F32),
            pltpu.VMEM((n, 1, WORDS), F32),
            pltpu.VMEM((1, WORDS), F32),
            pltpu.VMEM((stride - 1, 1, WORDS), F32),
            pltpu.VMEM((1, WORDS), F32),
            pltpu.VMEM((1, WORDS), F32),
            dma((7,)), dma((4,)), dma((2,)), dma((2,)), dma((mems,)), dma((mems,)),
            dma((8,)), dma((n // 4,)), dma((stride - 1,)), dma((stride - 1,)), dma, dma,
            dma((2, reach // 2)), dma((2, reach // 2)), dma((2,)), dma((2,)), dma, plain((stride,)), plain((mems,)),
        ],
        compiler_params=pltpu.CompilerParams(collective_id=0, has_side_effects=True),
        name="regrid",
    )(
        surf.reshape(columns, cells),
        area.reshape(own, 128),
        mask.reshape(own, 128),
        tarea.reshape(tgt, 128),
        tiles_in,
        tile_of.T,
        block_of.T,
        live.reshape(1, tgt),
    )
    inside = pl.BlockSpec(memory_space=pltpu.VMEM)
    out, conserved, ensemble = pl.pallas_call(
        functools.partial(last_kernel, (columns, members, fields, snaps), mems),
        out_shape=(
            jax.ShapeDtypeStruct((columns, tgt * 128), F32),
            jax.ShapeDtypeStruct((members, fields, snaps), F32),
            jax.ShapeDtypeStruct((fields, snaps), F32),
        ),
        in_specs=[inside, inside],
        out_specs=(any_space,) * 3,
        scratch_shapes=[
            pltpu.VMEM((columns, tgt * 128), F32),
            pltpu.VMEM((members, fields, snaps), F32),
            pltpu.VMEM((fields, snaps), F32),
            dma((6,)),
        ],
        compiler_params=pltpu.CompilerParams(vmem_limit_bytes=8 * 2**20),
        name="finish",
    )(tot, scaled)
    return out.reshape(members, fields, snaps, tgt * 128), conserved, ensemble


def solution(mesh):
    placed = (
        P(("grp", "mem"), "fld", None, "band"),
        P("band"),
        P("band"),
        P("band"),
        P(),
        P("band", None),
        P("band", None),
        P("band"),
    )
    return jax.shard_map(
        functools.partial(on_device, mesh.shape["band"], mesh.shape["mem"]),
        mesh=mesh,
        in_specs=placed,
        out_specs=(
            P(("grp", "mem"), "fld", None, "band"),
            P(("grp", "mem"), "fld", None),
            P(("grp", "fld"), None),
        ),
        check_vma=False,
    )
```

```python
import functools

import jax
import jax.numpy as jnp
from jax import lax
from jax.experimental import pallas as pl
from jax.experimental.pallas import tpu as pltpu
from jax.sharding import PartitionSpec as P

MESH = pl.DeviceIdType.MESH
HALO = 32
F32, BF16, I32 = jnp.float32, jnp.bfloat16, jnp.int32
HIGHEST = lax.Precision.HIGHEST
WORDS = 384


def row_dot(a, b, precision=None):
    return lax.dot_general(
        a, b, (((1,), (1,)), ((), ())), preferred_element_type=F32, precision=precision
    )


def in_three(x):
    high = jnp.round(x * 0.25) * 4.0
    rest = x - high
    mid = jnp.round(rest * 131072.0) * (1.0 / 131072.0)
    return high, mid, rest - mid


def main_kernel(
    n, mems, shape,
    surf, area, mask, tarea, tiles_in, tile_of, block_of, live_in,
    scaled, tot_out,
    surf_v, ext, am_v, mask_v, ta_v, w_v, idx, packed, told, local, sm, s_acc, reach_sum, psend, prec,
    s_msg, rs0, rxm, msg, msg_up, rx0, rx, mid, rxw, run, rxp,
    lsem, ssem, isend, irecv, msend, mrecv, dsend, drecv, wsend, wrecv, csend, crecv,
    pssem, prsem, zsend, zrecv, hsend, upper_in, mem_in,
):
    columns, own, tgt, slots, tiles, members, reach = shape
    me = lax.axis_index("band")
    my_mem = lax.axis_index("mem")
    has_low = me > 0
    has_up = me < n - 1
    stride = n // 8
    via = (lax.axis_index("grp") == 0) & (my_mem == 0) & (lax.axis_index("fld") == 0)
    last = jnp.where(via, n, 2)
    early = has_low & (me <= stride)
    late = jnp.logical_not(early)

    def band(o):
        return {"band": me + o}

    def remote(src, dst, send, recv, where):
        return pltpu.make_async_remote_copy(
            src_ref=src, dst_ref=dst, send_sem=send, recv_sem=recv,
            device_id=where, device_id_type=MESH,
        )

    def tell(sem, where):
        pl.semaphore_signal(sem, inc=1, device_id=where, device_id_type=MESH)

    barrier = pltpu.get_barrier_semaphore()

    def tell_band(q, carry):
        tell(barrier, {"band": q})
        return carry

    lax.fori_loop(me + 1, jnp.where(me == 0, 2, n), tell_band, 0)
    lax.fori_loop(jnp.where(me == 0, last, n), n, tell_band, 0)

    def tell_mem(m, carry):
        tell(barrier, {"mem": m})
        return carry

    lax.fori_loop(jnp.where(has_low, my_mem + 1, mems), mems, tell_mem, 0)

    loads = [
        pltpu.make_async_copy(block_of, idx.at[0:slots], lsem.at[0]),
        pltpu.make_async_copy(tile_of, idx.at[slots : 2 * slots], lsem.at[1]),
        pltpu.make_async_copy(live_in, idx.at[2 * slots : 2 * slots + 1], lsem.at[2]),
        pltpu.make_async_copy(area, am_v, lsem.at[3]),
        pltpu.make_async_copy(mask, mask_v, lsem.at[4]),
        pltpu.make_async_copy(tiles_in, w_v.at[0:tiles], lsem.at[5]),
        pltpu.make_async_copy(tarea, ta_v, lsem.at[6]),
    ]
    parts = 4
    width = own * 128 // parts
    pieces = [
        pltpu.make_async_copy(
            surf.at[:, q * width : (q + 1) * width],
            surf_v.at[:, q * width : (q + 1) * width],
            ssem.at[q],
        )
        for q in range(parts)
    ]
    for c in loads[:5] + pieces + loads[5:]:
        c.start()
    w_v[tiles] = jnp.zeros((128, 128), BF16)

    place = lax.broadcasted_iota(I32, (slots, tgt), 0)
    lane = lax.broadcasted_iota(I32, (slots, tgt), 1)
    scalars = [pltpu.make_async_copy(local.at[i], sm.at[i], lsem.at[i]) for i in range(3)]

    def make_local(i, word, shift, valid):
        block = (word & 255) + shift
        good = valid & (block >= 0) & (block < own)
        tile = jnp.where(good, word >> 8, tiles)
        local[i] = jnp.clip(block, 0, own - 1) + 256 * tile

    def own_lists():
        for c in loads[:3]:
            c.wait()
        alive = place < idx[2 * slots : 2 * slots + 1, :]
        word = idx[0:slots, :] + 256 * jnp.where(alive, idx[slots : 2 * slots, :], tiles)
        packed[...] = word
        make_local(0, word, -HALO, alive)
        scalars[0].start()

    def weigh(s, total):
        at = pl.ds(pl.multiple_of(s * 128, 128), 128)
        value = (am_v[pl.ds(s, 1), :] * surf_v[:, at].astype(F32)).astype(BF16)
        ext[s] = value
        return total + value.astype(F32)

    def local_part():
        loads[3].wait()
        loads[4].wait()
        am_v[...] = am_v[...] * mask_v[...].astype(F32)
        total = jnp.zeros((columns, 128), F32)
        for q in range(parts):
            pieces[q].wait()
            total = lax.fori_loop(q * own // parts, (q + 1) * own // parts, weigh, total, unroll=4)
        s_acc[...] = total
        loads[5].wait()
        loads[6].wait()

    def slot_sum(which, t):
        total = None
        for p in range(slots // 2):
            left, right = [], []
            for k in (2 * p, 2 * p + 1):
                word = sm[which, k, t]
                left.append(ext[word & 255])
                right.append(w_v[word >> 8])
            term = jnp.dot(
                jnp.concatenate(left, axis=1), jnp.concatenate(right, axis=0), preferred_element_type=F32
            )
            total = term if total is None else total + term
        return total

    def columns_of(t):
        return pl.ds(pl.multiple_of(t * 128, 128), 128)

    def own_targets():
        def body(t, carry):
            scaled[:, columns_of(t)] = slot_sum(0, t)
            return carry

        lax.fori_loop(0, tgt, body, 0)

    @pl.when(early)
    def _():
        own_lists()
        local_part()
        scalars[0].wait()
        own_targets()

    known = me - 1 + ((me == 1) | (me >= last)).astype(I32)

    @pl.when(has_low)
    def _():
        pl.semaphore_wait(barrier, known + my_mem)

    pl.when(has_low)(lambda: tell(upper_in.at[0], band(-1)))
    for o in range(2, stride + 1):
        pl.when(me > o)(functools.partial(tell, upper_in.at[o - 1], band(-o)))

    def tell_mem_back(m, carry):
        tell(mem_in.at[my_mem], {"mem": m})
        return carry

    lax.fori_loop(0, jnp.where(has_low, my_mem, 0), tell_mem_back, 0)

    pl.when(late)(own_lists)
    to_low = remote(packed, told.at[1], isend.at[0], irecv.at[0], band(-1))
    to_up = remote(packed, told.at[0], isend.at[1], irecv.at[1], band(1))
    pl.when(has_low)(to_low.start)

    def send_list_up():
        pl.semaphore_wait(upper_in.at[0], 1)
        to_up.start()

    pl.when(early)(send_list_up)
    pl.when(late)(local_part)

    ones = jnp.ones((8, 128), F32)
    s_row = row_dot(ones, s_acc[...], HIGHEST)[0:1]
    s_msg[...] = jnp.concatenate([s_row, jnp.zeros((1, 128 - columns), F32)], axis=1)

    first_row = remote(s_msg, rs0, zsend.at[0], zrecv.at[0], band(1))

    @pl.when(me == 0)
    def _():
        send_list_up()
        first_row.start()

    def from_mem(m, to):
        return remote(s_msg, rxm.at[m], msend.at[to], mrecv.at[m], {"mem": to})

    def others(action, which):
        for m in range(mems):
            pl.when(has_low & which(m))(functools.partial(action, m))

    def send_lower(m):
        from_mem(my_mem, m).start()

    others(send_lower, lambda m: (my_mem > m) & (me > 1))

    flat_w = w_v[0:tiles].reshape(tiles * 128, 128)
    sums = row_dot(jnp.ones((8, 128), BF16), flat_w)
    row_sums = jnp.concatenate([sums[0:1, q * 128 : (q + 1) * 128] for q in range(tiles)], axis=0)

    pl.when(late & has_low & has_up)(send_list_up)

    def cell_sums(word):
        row = jnp.concatenate([word[k : k + 1] for k in range(slots)], axis=1)
        count = slots * tgt
        at_block = (lax.broadcasted_iota(I32, (own, count), 0) == (row & 255)).astype(F32).astype(BF16)
        at_tile = (lax.broadcasted_iota(I32, (tiles, count), 0) == (row >> 8)).astype(F32).astype(BF16)
        return lax.dot_general(
            row_dot(at_block, at_tile), row_sums, (((1,), (0,)), ((), ())),
            preferred_element_type=F32, precision=HIGHEST,
        )

    def weigh_target(s, total):
        return total + ext[s].astype(F32) * reach_sum[pl.ds(s, 1), :]

    reach_sum[...] = cell_sums(local[0])
    t_acc = lax.fori_loop(0, own, weigh_target, jnp.zeros((columns, 128), F32), unroll=4)

    @pl.when(me == 1)
    def _():
        first_row.wait_recv()
        s_msg[...] = s_msg[...] + rs0[...]

    others(send_lower, lambda m: (my_mem > m) & (me == 1))
    pl.when(has_low)(to_up.wait_recv)
    pl.when(has_up)(to_low.wait_recv)

    def send_higher(m):
        pl.semaphore_wait(mem_in.at[m], 1)
        from_mem(my_mem, m).start()

    others(send_higher, lambda m: my_mem < m)

    from_low = (lane >= tgt - reach) & has_low
    from_up = (lane < reach) & has_up
    make_local(1, told[0], -(HALO + own), from_low)
    make_local(2, told[1], own - HALO, from_up)
    reach_sum[...] = cell_sums(jnp.where(lane < reach, local[2], local[1]))
    t_acc = lax.fori_loop(0, HALO, weigh_target, t_acc, unroll=4)
    t_acc = lax.fori_loop(own - HALO, own, weigh_target, t_acc, unroll=4)
    t_row = row_dot(ones, t_acc, HIGHEST)[0:1]
    scalars[1].start()
    scalars[2].start()

    chunk = 2

    def part_copy(side, j):
        at = pl.ds(chunk * j, chunk)
        return remote(
            psend.at[side, at], prec.at[1 - side, at], pssem.at[side, j], prsem.at[1 - side, j],
            band(2 * side - 1),
        )

    def for_side(side):
        def body(i, carry):
            psend[side, i] = slot_sum(1 + side, i + (tgt - reach if side == 0 else 0))

            @pl.when((i > 0) & (lax.rem(i, chunk) == 0))
            def _():
                part_copy(side, lax.div(i, chunk) - 1).start()

            return carry

        lax.fori_loop(0, reach, body, 0)
        part_copy(side, reach // chunk - 1).start()

    def for_neighbours():
        scalars[1].wait()
        scalars[2].wait()
        pl.when(has_low)(functools.partial(for_side, 0))
        pl.when(has_up)(functools.partial(for_side, 1))

    pl.when(early)(for_neighbours)

    rxm[my_mem] = s_msg[...]
    others(lambda m: from_mem(m, m).wait_recv(), lambda m: my_mem != m)
    e_row = rxm[0]
    for m in range(1, mems):
        e_row = e_row + rxm[m]
    per = columns // members
    e_sum = e_row[:, 0:per]
    for m in range(1, members):
        e_sum = e_sum + e_row[:, m * per : (m + 1) * per]
    e_sum = jnp.where(has_low, e_sum, 0.0)
    a_sum = jnp.sum(jnp.sum(ta_v[...], axis=0, keepdims=True), axis=1, keepdims=True)
    a_high = jnp.round(a_sum * 64.0) * (1.0 / 64.0)
    s_parts, e_parts = in_three(s_row), in_three(e_sum)
    used = 4 * columns + 3 * per + 2
    msg[...] = jnp.concatenate(
        [s_parts[0], t_row, s_parts[1], s_parts[2], *e_parts, a_high, a_sum - a_high,
         jnp.zeros((1, WORDS - used), F32)],
        axis=1,
    )

    group, ways = 4, 8

    def direct(q):
        return remote(
            msg, rx.at[me], dsend.at[lax.rem(q, ways)], drecv.at[lax.div(me, group)], {"band": q}
        )

    lowest = jnp.where((me == 1) | (me >= last), 0, 1)

    def send_down(q, carry):
        @pl.when(q - ways >= lowest)
        def _():
            direct(q - ways).wait_send()

        direct(q).start()
        return carry

    lax.fori_loop(lowest, me, send_down, 0)

    from_first = remote(msg, rx0, zsend.at[1], zrecv.at[1], band(1))

    pl.when(me == 0)(from_first.start)

    msg_up[...] = msg[...]

    @pl.when(me == 1)
    def _():
        from_first.wait_recv()
        msg_up[...] = msg[...] + rx0[...]

    ups = [remote(msg_up, rxw.at[o - 1], wsend.at[o - 1], wrecv.at[o - 1], band(o)) for o in range(1, stride)]
    chain = remote(run, rxp, csend, crecv, band(stride))

    def to_higher(o):
        return has_low & (me + o < n)

    def send_up(o):
        if o > 1:
            pl.semaphore_wait(upper_in.at[o - 1], 1)
        if o < stride:
            ups[o - 1].start()

    for o in range(1, stride + 1):
        pl.when(to_higher(o))(functools.partial(send_up, o))

    pl.when(late)(for_neighbours)
    @pl.when(late)
    def _():
        scalars[0].wait()
        own_targets()


    run[...] = msg_up[...]

    def add_window(o):
        ups[o - 1].wait_recv()
        run[...] = run[...] + rxw[o - 1]

    for o in range(1, stride):
        pl.when(me > o)(functools.partial(add_window, o))

    @pl.when(me > stride)
    def _():
        chain.wait_recv()
        run[...] = run[...] + rxp[...]

    pl.when(to_higher(stride))(chain.start)

    def add_part(side, start):
        def body(j, carry):
            part_copy(1 - side, j).wait_recv()
            for i in range(chunk):
                at = columns_of(start + chunk * j + i)
                scaled[:, at] = scaled[:, at] + prec[side, chunk * j + i]
            return carry

        lax.fori_loop(0, reach // chunk, body, 0)

    def divide(t, carry):
        at = columns_of(t)
        scaled[:, at] = scaled[:, at] / ta_v[pl.ds(t, 1), :]
        return carry

    pl.when(has_low)(functools.partial(add_part, 0, 0))
    pl.when(has_up)(functools.partial(add_part, 1, tgt - reach))
    lax.fori_loop(0, tgt, divide, 0)

    def sent(q, carry):
        direct(q).wait_send()
        return carry

    lax.fori_loop(jnp.maximum(lowest, me - ways), me, sent, 0)

    @pl.when(me == 0)
    def _():
        first_row.wait_send()
        from_first.wait_send()

    pl.when(to_higher(stride))(chain.wait_send)
    for o in range(1, stride):
        pl.when(to_higher(o))(ups[o - 1].wait_send)
    others(lambda m: from_mem(my_mem, m).wait_send(), lambda m: my_mem != m)

    def parts_sent(side):
        for j in range(reach // chunk):
            part_copy(side, j).wait_send()

    @pl.when(has_low)
    def _():
        to_low.wait_send()
        parts_sent(0)

    @pl.when(has_up)
    def _():
        to_up.wait_send()
        parts_sent(1)

    def arrived(start, count, g):
        at = rx.at[pl.ds(start, count)]
        remote(at, at, dsend.at[0], drecv.at[g], {"band": lax.rem(me + 1, n)}).wait_recv()
        for i in range(count):
            mid[...] = mid[...] + rx[start + i]

    mine = lax.div(me, group)
    near = jnp.where(via & (me == 0), 2, group - 1 - lax.rem(me, group))
    mid[...] = jnp.zeros((1, WORDS), F32)
    for count in range(1, group):
        pl.when(near == count)(functools.partial(arrived, me + 1, count, mine))

    def add_group(g, carry):
        arrived(group * g, group, g)
        return carry

    lax.fori_loop(jnp.where(via & (me == 0), n // group, mine + 1), n // group, add_group, 0)

    hand = remote(mid, rx.at[2], hsend, drecv.at[0], band(-1))
    pl.when(via & (me == 1))(hand.start)
    tot_out[...] = run[...] + mid[...]
    pl.when(via & (me == 1))(hand.wait_send)


def last_kernel(shape, mems, tot, scaled, out, conserved, ensemble, done, mean_v, group_v, sems):
    columns, members, fields, snaps = shape
    per = columns // members

    def at(start, size):
        return tot[:, start : start + size]

    base = 4 * columns
    s = (at(0, columns) + at(2 * columns, columns)) + at(3 * columns, columns)
    e = (at(base, per) + at(base + per, per)) + at(base + 2 * per, per)
    total_area = at(base + 3 * per, 1) + at(base + 3 * per + 1, 1)
    step = (s - at(columns, columns)) / total_area
    diagonal = lax.broadcasted_iota(I32, (columns, columns), 0) == lax.broadcasted_iota(
        I32, (columns, columns), 1
    )
    fix = jnp.broadcast_to(jnp.sum(jnp.where(diagonal, step, 0.0), axis=1, keepdims=True), (columns, 128))
    mean = s / total_area
    for i in range(members * fields):
        mean_v[i // fields, i % fields : i % fields + 1, :] = mean[:, i * snaps : (i + 1) * snaps]
    group = e / total_area / float(members * mems)
    for f in range(fields):
        group_v[f : f + 1, :] = group[:, f * snaps : (f + 1) * snaps]
    pieces = 4
    copies = [
        pltpu.make_async_copy(mean_v, conserved, sems.at[pieces]),
        pltpu.make_async_copy(group_v, ensemble, sems.at[pieces + 1]),
    ]
    for q in range(pieces):
        rows = slice(q * columns // pieces, (q + 1) * columns // pieces)
        for b in range(out.shape[1] // 128):
            done[rows, b * 128 : (b + 1) * 128] = scaled[rows, b * 128 : (b + 1) * 128] + fix[rows]
        copies.append(pltpu.make_async_copy(done.at[rows], out.at[rows], sems.at[q]))
        copies[-1].start()
        if q == 0:
            copies[0].start()
            copies[1].start()
    for c in copies:
        c.wait()


def on_device(n, mems, surf, mask, area, tarea, tiles_in, tile_of, block_of, live):
    members, fields, snaps, cells = surf.shape
    columns = members * fields * snaps
    own = cells // 128
    tgt, slots = tile_of.shape
    tiles = tiles_in.shape[0]
    reach = HALO * tgt // own
    any_space = pl.BlockSpec(memory_space=pl.ANY)
    dma, plain = pltpu.SemaphoreType.DMA, pltpu.SemaphoreType.REGULAR
    rows = -(-(2 * slots + 1) // 8) * 8
    stride = n // 8
    scaled, tot = pl.pallas_call(
        functools.partial(main_kernel, n, mems, (columns, own, tgt, slots, tiles, members, reach)),
        out_shape=(pltpu.VMEM((columns, tgt * 128), F32), pltpu.VMEM((1, WORDS), F32)),
        in_specs=[any_space] * 8,
        out_specs=(pl.BlockSpec(memory_space=pltpu.VMEM),) * 2,
        scratch_shapes=[
            pltpu.VMEM((columns, cells), BF16),
            pltpu.VMEM((own, columns, 128), BF16),
            pltpu.VMEM((own, 128), F32),
            pltpu.VMEM((own, 128), I32),
            pltpu.VMEM((tgt, 128), F32),
            pltpu.VMEM((tiles + 1, 128, 128), BF16),
            pltpu.VMEM((rows, tgt), I32),
            pltpu.VMEM((slots, tgt), I32),
            pltpu.VMEM((2, slots, tgt), I32),
            pltpu.VMEM((3, slots, tgt), I32),
            pltpu.SMEM((3, slots, tgt), I32),
            pltpu.VMEM((columns, 128), F32),
            pltpu.VMEM((own, 128), F32),
            pltpu.VMEM((2, reach, columns, 128), F32),
            pltpu.VMEM((2, reach, columns, 128), F32),
            pltpu.VMEM((1, 128), F32),
            pltpu.VMEM((1, 128), F32),
            pltpu.VMEM((mems, 1, 128), F32),
            pltpu.VMEM((1, WORDS), F32),
            pltpu.VMEM((1, WORDS), F32),
            pltpu.VMEM((1, WORDS), F32),
            pltpu.VMEM((n, 1, WORDS), F32),
            pltpu.VMEM((1, WORDS), F32),
            pltpu.VMEM((stride - 1, 1, WORDS), F32),
            pltpu.VMEM((1, WORDS), F32),
            pltpu.VMEM((1, WORDS), F32),
            dma((7,)), dma((4,)), dma((2,)), dma((2,)), dma((mems,)), dma((mems,)),
            dma((8,)), dma((n // 4,)), dma((stride - 1,)), dma((stride - 1,)), dma, dma,
            dma((2, reach // 2)), dma((2, reach // 2)), dma((2,)), dma((2,)), dma, plain((stride,)), plain((mems,)),
        ],
        compiler_params=pltpu.CompilerParams(collective_id=0, has_side_effects=True),
        name="regrid",
    )(
        surf.reshape(columns, cells),
        area.reshape(own, 128),
        mask.reshape(own, 128),
        tarea.reshape(tgt, 128),
        tiles_in,
        tile_of.T,
        block_of.T,
        live.reshape(1, tgt),
    )
    inside = pl.BlockSpec(memory_space=pltpu.VMEM)
    out, conserved, ensemble = pl.pallas_call(
        functools.partial(last_kernel, (columns, members, fields, snaps), mems),
        out_shape=(
            jax.ShapeDtypeStruct((columns, tgt * 128), F32),
            jax.ShapeDtypeStruct((members, fields, snaps), F32),
            jax.ShapeDtypeStruct((fields, snaps), F32),
        ),
        in_specs=[inside, inside],
        out_specs=(any_space,) * 3,
        scratch_shapes=[
            pltpu.VMEM((columns, tgt * 128), F32),
            pltpu.VMEM((members, fields, snaps), F32),
            pltpu.VMEM((fields, snaps), F32),
            dma((6,)),
        ],
        compiler_params=pltpu.CompilerParams(vmem_limit_bytes=8 * 2**20),
        name="finish",
    )(tot, scaled)
    return out.reshape(members, fields, snaps, tgt * 128), conserved, ensemble


def solution(mesh):
    placed = (
        P(("grp", "mem"), "fld", None, "band"),
        P("band"),
        P("band"),
        P("band"),
        P(),
        P("band", None),
        P("band", None),
        P("band"),
    )
    return jax.shard_map(
        functools.partial(on_device, mesh.shape["band"], mesh.shape["mem"]),
        mesh=mesh,
        in_specs=placed,
        out_specs=(
            P(("grp", "mem"), "fld", None, "band"),
            P(("grp", "mem"), "fld", None),
            P(("grp", "fld"), None),
        ),
        check_vma=False,
    )
```

```python
import functools

import jax
import jax.numpy as jnp
from jax import lax
from jax.experimental import pallas as pl
from jax.experimental.pallas import tpu as pltpu
from jax.sharding import PartitionSpec as P

MESH = pl.DeviceIdType.MESH
HALO = 32
F32, BF16, I32 = jnp.float32, jnp.bfloat16, jnp.int32
HIGHEST = lax.Precision.HIGHEST
WORDS = 384


def row_dot(a, b, precision=None):
    return lax.dot_general(
        a, b, (((1,), (1,)), ((), ())), preferred_element_type=F32, precision=precision
    )


def in_three(x):
    high = jnp.round(x * 0.25) * 4.0
    rest = x - high
    mid = jnp.round(rest * 131072.0) * (1.0 / 131072.0)
    return high, mid, rest - mid


def main_kernel(
    n, mems, shape,
    surf, area, mask, tarea, tiles_in, tile_of, block_of, live_in,
    scaled, tot_out,
    surf_v, ext, am_v, mask_v, ta_v, w_v, idx, packed, told, local, sm, s_acc, reach_sum, psend, prec,
    s_msg, rs0, rxm, msg, msg_up, rx0, rx, mid, rxw, run, rxp, rtot,
    lsem, ssem, isend, irecv, msend, mrecv, dsend, drecv, wsend, wrecv, csend, crecv,
    pssem, prsem, zsend, zrecv, hsend, tsend, trecv, upper_in, mem_in, want,
):
    columns, own, tgt, slots, tiles, members, reach = shape
    me = lax.axis_index("band")
    my_mem = lax.axis_index("mem")
    has_low = me > 0
    has_up = me < n - 1
    stride = n // 8
    via = (lax.axis_index("grp") == 0) & (my_mem == 0) & (lax.axis_index("fld") == 0)
    last = jnp.where(via, n, 2)
    first = n // 4
    fan = 4
    is_first = me <= first
    early = has_low & (me <= stride)
    late = jnp.logical_not(early)

    def band(o):
        return {"band": me + o}

    def remote(src, dst, send, recv, where):
        return pltpu.make_async_remote_copy(
            src_ref=src, dst_ref=dst, send_sem=send, recv_sem=recv,
            device_id=where, device_id_type=MESH,
        )

    def tell(sem, where):
        pl.semaphore_signal(sem, inc=1, device_id=where, device_id_type=MESH)

    barrier = pltpu.get_barrier_semaphore()

    def tell_band(q, carry):
        tell(barrier, {"band": q})
        return carry

    lax.fori_loop(me + 1, jnp.where(me == 0, 2, n), tell_band, 0)
    lax.fori_loop(jnp.where(me == 0, last, n), n, tell_band, 0)

    def tell_mem(m, carry):
        tell(barrier, {"mem": m})
        return carry

    lax.fori_loop(jnp.where(has_low, my_mem + 1, mems), mems, tell_mem, 0)

    loads = [
        pltpu.make_async_copy(block_of, idx.at[0:slots], lsem.at[0]),
        pltpu.make_async_copy(tile_of, idx.at[slots : 2 * slots], lsem.at[1]),
        pltpu.make_async_copy(live_in, idx.at[2 * slots : 2 * slots + 1], lsem.at[2]),
        pltpu.make_async_copy(area, am_v, lsem.at[3]),
        pltpu.make_async_copy(mask, mask_v, lsem.at[4]),
        pltpu.make_async_copy(tiles_in, w_v.at[0:tiles], lsem.at[5]),
        pltpu.make_async_copy(tarea, ta_v, lsem.at[6]),
    ]
    parts = 4
    width = own * 128 // parts
    pieces = [
        pltpu.make_async_copy(
            surf.at[:, q * width : (q + 1) * width],
            surf_v.at[:, q * width : (q + 1) * width],
            ssem.at[q],
        )
        for q in range(parts)
    ]
    for c in loads[:5] + pieces + loads[5:]:
        c.start()
    w_v[tiles] = jnp.zeros((128, 128), BF16)

    place = lax.broadcasted_iota(I32, (slots, tgt), 0)
    lane = lax.broadcasted_iota(I32, (slots, tgt), 1)
    scalars = [pltpu.make_async_copy(local.at[i], sm.at[i], lsem.at[i]) for i in range(3)]

    def make_local(i, word, shift, valid):
        block = (word & 255) + shift
        good = valid & (block >= 0) & (block < own)
        tile = jnp.where(good, word >> 8, tiles)
        local[i] = jnp.clip(block, 0, own - 1) + 256 * tile

    def own_lists():
        for c in loads[:3]:
            c.wait()
        alive = place < idx[2 * slots : 2 * slots + 1, :]
        word = idx[0:slots, :] + 256 * jnp.where(alive, idx[slots : 2 * slots, :], tiles)
        packed[...] = word
        make_local(0, word, -HALO, alive)
        scalars[0].start()

    def weigh(s, total):
        at = pl.ds(pl.multiple_of(s * 128, 128), 128)
        value = (am_v[pl.ds(s, 1), :] * surf_v[:, at].astype(F32)).astype(BF16)
        ext[s] = value
        return total + value.astype(F32)

    def local_part():
        loads[3].wait()
        loads[4].wait()
        am_v[...] = am_v[...] * mask_v[...].astype(F32)
        total = jnp.zeros((columns, 128), F32)
        for q in range(parts):
            pieces[q].wait()
            total = lax.fori_loop(q * own // parts, (q + 1) * own // parts, weigh, total, unroll=4)
        s_acc[...] = total
        loads[5].wait()
        loads[6].wait()

    def slot_sum(which, t):
        total = None
        for p in range(slots // 2):
            left, right = [], []
            for k in (2 * p, 2 * p + 1):
                word = sm[which, k, t]
                left.append(ext[word & 255])
                right.append(w_v[word >> 8])
            term = jnp.dot(
                jnp.concatenate(left, axis=1), jnp.concatenate(right, axis=0), preferred_element_type=F32
            )
            total = term if total is None else total + term
        return total

    def columns_of(t):
        return pl.ds(pl.multiple_of(t * 128, 128), 128)

    def own_targets():
        def body(t, carry):
            scaled[:, columns_of(t)] = slot_sum(0, t)
            return carry

        lax.fori_loop(0, tgt, body, 0)

    @pl.when(early)
    def _():
        own_lists()
        local_part()
        scalars[0].wait()
        own_targets()

    known = me - 1 + ((me == 1) | (me >= last)).astype(I32)

    @pl.when(has_low)
    def _():
        pl.semaphore_wait(barrier, known + my_mem)

    pl.when(has_low)(lambda: tell(upper_in.at[0], band(-1)))
    for o in range(2, stride + 1):
        pl.when((me > o) & is_first)(functools.partial(tell, upper_in.at[o - 1], band(-o)))

    def ask():
        back = me - first - 1
        tell(want.at[lax.div(back, fan)], {"band": first + 1 - fan + lax.rem(back, fan)})

    pl.when(jnp.logical_not(is_first))(ask)

    def tell_mem_back(m, carry):
        tell(mem_in.at[my_mem], {"mem": m})
        return carry

    lax.fori_loop(0, jnp.where(has_low, my_mem, 0), tell_mem_back, 0)

    pl.when(late)(own_lists)
    to_low = remote(packed, told.at[1], isend.at[0], irecv.at[0], band(-1))
    to_up = remote(packed, told.at[0], isend.at[1], irecv.at[1], band(1))
    pl.when(has_low)(to_low.start)

    def send_list_up():
        pl.semaphore_wait(upper_in.at[0], 1)
        to_up.start()

    pl.when(early)(send_list_up)
    pl.when(late)(local_part)

    ones = jnp.ones((8, 128), F32)
    s_row = row_dot(ones, s_acc[...], HIGHEST)[0:1]
    s_msg[...] = jnp.concatenate([s_row, jnp.zeros((1, 128 - columns), F32)], axis=1)

    first_row = remote(s_msg, rs0, zsend.at[0], zrecv.at[0], band(1))

    @pl.when(me == 0)
    def _():
        send_list_up()
        first_row.start()

    def from_mem(m, to):
        return remote(s_msg, rxm.at[m], msend.at[to], mrecv.at[m], {"mem": to})

    def others(action, which):
        for m in range(mems):
            pl.when(has_low & which(m))(functools.partial(action, m))

    def send_lower(m):
        from_mem(my_mem, m).start()

    others(send_lower, lambda m: (my_mem > m) & (me > 1))

    flat_w = w_v[0:tiles].reshape(tiles * 128, 128)
    sums = row_dot(jnp.ones((8, 128), BF16), flat_w)
    row_sums = jnp.concatenate([sums[0:1, q * 128 : (q + 1) * 128] for q in range(tiles)], axis=0)

    pl.when(late & has_low & has_up)(send_list_up)

    def cell_sums(word):
        row = jnp.concatenate([word[k : k + 1] for k in range(slots)], axis=1)
        count = slots * tgt
        at_block = (lax.broadcasted_iota(I32, (own, count), 0) == (row & 255)).astype(F32).astype(BF16)
        at_tile = (lax.broadcasted_iota(I32, (tiles, count), 0) == (row >> 8)).astype(F32).astype(BF16)
        return lax.dot_general(
            row_dot(at_block, at_tile), row_sums, (((1,), (0,)), ((), ())),
            preferred_element_type=F32, precision=HIGHEST,
        )

    def weigh_target(s, total):
        return total + ext[s].astype(F32) * reach_sum[pl.ds(s, 1), :]

    reach_sum[...] = cell_sums(local[0])
    t_acc = lax.fori_loop(0, own, weigh_target, jnp.zeros((columns, 128), F32), unroll=4)

    @pl.when(me == 1)
    def _():
        first_row.wait_recv()
        s_msg[...] = s_msg[...] + rs0[...]

    others(send_lower, lambda m: (my_mem > m) & (me == 1))
    pl.when(has_low)(to_up.wait_recv)
    pl.when(has_up)(to_low.wait_recv)

    def send_higher(m):
        pl.semaphore_wait(mem_in.at[m], 1)
        from_mem(my_mem, m).start()

    others(send_higher, lambda m: my_mem < m)

    from_low = (lane >= tgt - reach) & has_low
    from_up = (lane < reach) & has_up
    make_local(1, told[0], -(HALO + own), from_low)
    make_local(2, told[1], own - HALO, from_up)
    reach_sum[...] = cell_sums(jnp.where(lane < reach, local[2], local[1]))
    t_acc = lax.fori_loop(0, HALO, weigh_target, t_acc, unroll=4)
    t_acc = lax.fori_loop(own - HALO, own, weigh_target, t_acc, unroll=4)
    t_row = row_dot(ones, t_acc, HIGHEST)[0:1]
    scalars[1].start()
    scalars[2].start()

    chunk = 2

    def part_copy(side, j):
        at = pl.ds(chunk * j, chunk)
        return remote(
            psend.at[side, at], prec.at[1 - side, at], pssem.at[side, j], prsem.at[1 - side, j],
            band(2 * side - 1),
        )

    def for_side(side):
        def body(i, carry):
            psend[side, i] = slot_sum(1 + side, i + (tgt - reach if side == 0 else 0))

            @pl.when((i > 0) & (lax.rem(i, chunk) == 0))
            def _():
                part_copy(side, lax.div(i, chunk) - 1).start()

            return carry

        lax.fori_loop(0, reach, body, 0)
        part_copy(side, reach // chunk - 1).start()

    def for_neighbours():
        scalars[1].wait()
        scalars[2].wait()
        pl.when(has_low)(functools.partial(for_side, 0))
        pl.when(has_up)(functools.partial(for_side, 1))

    parts_first = early & jnp.logical_not(via)
    pl.when(parts_first)(for_neighbours)

    rxm[my_mem] = s_msg[...]
    others(lambda m: from_mem(m, m).wait_recv(), lambda m: my_mem != m)
    e_row = rxm[0]
    for m in range(1, mems):
        e_row = e_row + rxm[m]
    per = columns // members
    e_sum = e_row[:, 0:per]
    for m in range(1, members):
        e_sum = e_sum + e_row[:, m * per : (m + 1) * per]
    e_sum = jnp.where(has_low, e_sum, 0.0)
    a_sum = jnp.sum(jnp.sum(ta_v[...], axis=0, keepdims=True), axis=1, keepdims=True)
    a_high = jnp.round(a_sum * 64.0) * (1.0 / 64.0)
    s_parts, e_parts = in_three(s_row), in_three(e_sum)
    used = 4 * columns + 3 * per + 2
    msg[...] = jnp.concatenate(
        [s_parts[0], t_row, s_parts[1], s_parts[2], *e_parts, a_high, a_sum - a_high,
         jnp.zeros((1, WORDS - used), F32)],
        axis=1,
    )

    group = 4

    def direct(q):
        return remote(msg, rx.at[me], dsend.at[q], drecv.at[lax.div(me, group)], {"band": q})

    lowest = jnp.where((me == 1) | (me >= last), 0, 1)
    highest = jnp.minimum(me, first + 1)

    def send_down(q, carry):
        direct(q).start()
        return carry

    lax.fori_loop(lowest, highest, send_down, 0)

    from_first = remote(msg, rx0, zsend.at[1], zrecv.at[1], band(1))

    pl.when(me == 0)(from_first.start)

    msg_up[...] = msg[...]

    @pl.when(me == 1)
    def _():
        from_first.wait_recv()
        msg_up[...] = msg[...] + rx0[...]

    ups = [remote(msg_up, rxw.at[o - 1], wsend.at[o - 1], wrecv.at[o - 1], band(o)) for o in range(1, stride)]
    chain = remote(run, rxp, csend, crecv, band(stride))

    def to_higher(o):
        return has_low & (me + o <= first)

    def send_up(o):
        if o > 1:
            pl.semaphore_wait(upper_in.at[o - 1], 1)
        if o < stride:
            ups[o - 1].start()

    for o in range(1, stride + 1):
        pl.when(to_higher(o))(functools.partial(send_up, o))

    pl.when(jnp.logical_not(parts_first))(for_neighbours)
    @pl.when(late)
    def _():
        scalars[0].wait()
        own_targets()


    run[...] = msg_up[...]

    def add_window(o):
        ups[o - 1].wait_recv()
        run[...] = run[...] + rxw[o - 1]

    for o in range(1, stride):
        pl.when((me > o) & is_first)(functools.partial(add_window, o))

    @pl.when((me > stride) & is_first)
    def _():
        chain.wait_recv()
        run[...] = run[...] + rxp[...]

    pl.when(to_higher(stride))(chain.start)

    def add_part(side, start):
        def body(j, carry):
            part_copy(1 - side, j).wait_recv()
            for i in range(chunk):
                at = columns_of(start + chunk * j + i)
                scaled[:, at] = scaled[:, at] + prec[side, chunk * j + i]
            return carry

        lax.fori_loop(0, reach // chunk, body, 0)

    def divide(t, carry):
        at = columns_of(t)
        scaled[:, at] = scaled[:, at] / ta_v[pl.ds(t, 1), :]
        return carry

    pl.when(has_low)(functools.partial(add_part, 0, 0))
    pl.when(has_up)(functools.partial(add_part, 1, tgt - reach))
    lax.fori_loop(0, tgt, divide, 0)

    def sent(q, carry):
        direct(q).wait_send()
        return carry

    lax.fori_loop(lowest, highest, sent, 0)

    @pl.when(me == 0)
    def _():
        first_row.wait_send()
        from_first.wait_send()

    pl.when(to_higher(stride))(chain.wait_send)
    for o in range(1, stride):
        pl.when(to_higher(o))(ups[o - 1].wait_send)
    others(lambda m: from_mem(my_mem, m).wait_send(), lambda m: my_mem != m)

    def parts_sent(side):
        for j in range(reach // chunk):
            part_copy(side, j).wait_send()

    @pl.when(has_low)
    def _():
        to_low.wait_send()
        parts_sent(0)

    @pl.when(has_up)
    def _():
        to_up.wait_send()
        parts_sent(1)

    def arrived(start, count, g):
        at = rx.at[pl.ds(start, count)]
        remote(at, at, dsend.at[0], drecv.at[g], {"band": lax.rem(me + 1, n)}).wait_recv()
        for i in range(count):
            mid[...] = mid[...] + rx[start + i]

    mine = lax.div(me, group)
    near = jnp.where(via & (me == 0), 2, group - 1 - lax.rem(me, group))
    mid[...] = jnp.zeros((1, WORDS), F32)
    for count in range(1, group):
        pl.when(is_first & (near == count))(functools.partial(arrived, me + 1, count, mine))

    def add_group(g, carry):
        arrived(group * g, group, g)
        return carry

    no_more = (via & (me == 0)) | jnp.logical_not(is_first)
    lax.fori_loop(jnp.where(no_more, n // group, mine + 1), n // group, add_group, 0)

    hand = remote(mid, rx.at[2], hsend, drecv.at[0], band(-1))
    pl.when(via & (me == 1))(hand.start)
    run[...] = run[...] + mid[...]

    def total_to(k):
        return remote(run, rtot, tsend.at[k], trecv, band(fan * (k + 1)))

    def give(k):
        pl.semaphore_wait(want.at[k], 1)
        total_to(k).start()

    count = -(-(n - first - 1) // fan)
    gives = [is_first & (me > first - fan) & (me + fan * (k + 1) < n) for k in range(count)]
    for k in range(count):
        pl.when(gives[k])(functools.partial(give, k))

    @pl.when(is_first)
    def _():
        tot_out[...] = run[...]

    @pl.when(jnp.logical_not(is_first))
    def _():
        remote(run, rtot, tsend.at[0], trecv, band(-1)).wait_recv()
        tot_out[...] = rtot[...]

    for k in range(count):
        pl.when(gives[k])(total_to(k).wait_send)
    pl.when(via & (me == 1))(hand.wait_send)


def last_kernel(shape, mems, tot, scaled, out, conserved, ensemble, done, mean_v, group_v, sems):
    columns, members, fields, snaps = shape
    per = columns // members

    def at(start, size):
        return tot[:, start : start + size]

    base = 4 * columns
    s = (at(0, columns) + at(2 * columns, columns)) + at(3 * columns, columns)
    e = (at(base, per) + at(base + per, per)) + at(base + 2 * per, per)
    total_area = at(base + 3 * per, 1) + at(base + 3 * per + 1, 1)
    step = (s - at(columns, columns)) / total_area
    diagonal = lax.broadcasted_iota(I32, (columns, columns), 0) == lax.broadcasted_iota(
        I32, (columns, columns), 1
    )
    fix = jnp.broadcast_to(jnp.sum(jnp.where(diagonal, step, 0.0), axis=1, keepdims=True), (columns, 128))
    mean = s / total_area
    for i in range(members * fields):
        mean_v[i // fields, i % fields : i % fields + 1, :] = mean[:, i * snaps : (i + 1) * snaps]
    group = e / total_area / float(members * mems)
    for f in range(fields):
        group_v[f : f + 1, :] = group[:, f * snaps : (f + 1) * snaps]
    pieces = 4
    copies = [
        pltpu.make_async_copy(mean_v, conserved, sems.at[pieces]),
        pltpu.make_async_copy(group_v, ensemble, sems.at[pieces + 1]),
    ]
    for q in range(pieces):
        rows = slice(q * columns // pieces, (q + 1) * columns // pieces)
        for b in range(out.shape[1] // 128):
            done[rows, b * 128 : (b + 1) * 128] = scaled[rows, b * 128 : (b + 1) * 128] + fix[rows]
        copies.append(pltpu.make_async_copy(done.at[rows], out.at[rows], sems.at[q]))
        copies[-1].start()
        if q == 0:
            copies[0].start()
            copies[1].start()
    for c in copies:
        c.wait()


def on_device(n, mems, surf, mask, area, tarea, tiles_in, tile_of, block_of, live):
    members, fields, snaps, cells = surf.shape
    columns = members * fields * snaps
    own = cells // 128
    tgt, slots = tile_of.shape
    tiles = tiles_in.shape[0]
    reach = HALO * tgt // own
    any_space = pl.BlockSpec(memory_space=pl.ANY)
    dma, plain = pltpu.SemaphoreType.DMA, pltpu.SemaphoreType.REGULAR
    rows = -(-(2 * slots + 1) // 8) * 8
    stride = n // 8
    scaled, tot = pl.pallas_call(
        functools.partial(main_kernel, n, mems, (columns, own, tgt, slots, tiles, members, reach)),
        out_shape=(pltpu.VMEM((columns, tgt * 128), F32), pltpu.VMEM((1, WORDS), F32)),
        in_specs=[any_space] * 8,
        out_specs=(pl.BlockSpec(memory_space=pltpu.VMEM),) * 2,
        scratch_shapes=[
            pltpu.VMEM((columns, cells), BF16),
            pltpu.VMEM((own, columns, 128), BF16),
            pltpu.VMEM((own, 128), F32),
            pltpu.VMEM((own, 128), I32),
            pltpu.VMEM((tgt, 128), F32),
            pltpu.VMEM((tiles + 1, 128, 128), BF16),
            pltpu.VMEM((rows, tgt), I32),
            pltpu.VMEM((slots, tgt), I32),
            pltpu.VMEM((2, slots, tgt), I32),
            pltpu.VMEM((3, slots, tgt), I32),
            pltpu.SMEM((3, slots, tgt), I32),
            pltpu.VMEM((columns, 128), F32),
            pltpu.VMEM((own, 128), F32),
            pltpu.VMEM((2, reach, columns, 128), F32),
            pltpu.VMEM((2, reach, columns, 128), F32),
            pltpu.VMEM((1, 128), F32),
            pltpu.VMEM((1, 128), F32),
            pltpu.VMEM((mems, 1, 128), F32),
            pltpu.VMEM((1, WORDS), F32),
            pltpu.VMEM((1, WORDS), F32),
            pltpu.VMEM((1, WORDS), F32),
            pltpu.VMEM((n, 1, WORDS), F32),
            pltpu.VMEM((1, WORDS), F32),
            pltpu.VMEM((stride - 1, 1, WORDS), F32),
            pltpu.VMEM((1, WORDS), F32),
            pltpu.VMEM((1, WORDS), F32),
            pltpu.VMEM((1, WORDS), F32),
            dma((7,)), dma((4,)), dma((2,)), dma((2,)), dma((mems,)), dma((mems,)),
            dma((n // 4 + 1,)), dma((n // 4,)), dma((stride - 1,)), dma((stride - 1,)), dma, dma,
            dma((2, reach // 2)), dma((2, reach // 2)), dma((2,)), dma((2,)), dma,
            dma((n // 4,)), dma, plain((stride,)), plain((mems,)), plain((n // 4,)),
        ],
        compiler_params=pltpu.CompilerParams(collective_id=0, has_side_effects=True),
        name="regrid",
    )(
        surf.reshape(columns, cells),
        area.reshape(own, 128),
        mask.reshape(own, 128),
        tarea.reshape(tgt, 128),
        tiles_in,
        tile_of.T,
        block_of.T,
        live.reshape(1, tgt),
    )
    inside = pl.BlockSpec(memory_space=pltpu.VMEM)
    out, conserved, ensemble = pl.pallas_call(
        functools.partial(last_kernel, (columns, members, fields, snaps), mems),
        out_shape=(
            jax.ShapeDtypeStruct((columns, tgt * 128), F32),
            jax.ShapeDtypeStruct((members, fields, snaps), F32),
            jax.ShapeDtypeStruct((fields, snaps), F32),
        ),
        in_specs=[inside, inside],
        out_specs=(any_space,) * 3,
        scratch_shapes=[
            pltpu.VMEM((columns, tgt * 128), F32),
            pltpu.VMEM((members, fields, snaps), F32),
            pltpu.VMEM((fields, snaps), F32),
            dma((6,)),
        ],
        compiler_params=pltpu.CompilerParams(vmem_limit_bytes=8 * 2**20),
        name="finish",
    )(tot, scaled)
    return out.reshape(members, fields, snaps, tgt * 128), conserved, ensemble


def solution(mesh):
    placed = (
        P(("grp", "mem"), "fld", None, "band"),
        P("band"),
        P("band"),
        P("band"),
        P(),
        P("band", None),
        P("band", None),
        P("band"),
    )
    return jax.shard_map(
        functools.partial(on_device, mesh.shape["band"], mesh.shape["mem"]),
        mesh=mesh,
        in_specs=placed,
        out_specs=(
            P(("grp", "mem"), "fld", None, "band"),
            P(("grp", "mem"), "fld", None),
            P(("grp", "fld"), None),
        ),
        check_vma=False,
    )
```

```python
import functools

import jax
import jax.numpy as jnp
from jax import lax
from jax.experimental import pallas as pl
from jax.experimental.pallas import tpu as pltpu
from jax.sharding import PartitionSpec as P

MESH = pl.DeviceIdType.MESH
HALO = 32
F32, BF16, I32 = jnp.float32, jnp.bfloat16, jnp.int32
HIGHEST = lax.Precision.HIGHEST
WORDS = 384


def row_dot(a, b, precision=None):
    return lax.dot_general(
        a, b, (((1,), (1,)), ((), ())), preferred_element_type=F32, precision=precision
    )


def in_three(x):
    high = jnp.round(x * 0.25) * 4.0
    rest = x - high
    mid = jnp.round(rest * 131072.0) * (1.0 / 131072.0)
    return high, mid, rest - mid


def main_kernel(
    n, mems, shape,
    surf, area, mask, tarea, tiles_in, tile_of, block_of, live_in,
    scaled, tot_out,
    surf_v, ext, am_v, mask_v, ta_v, w_v, idx, packed, told, local, sm, s_acc, reach_sum, psend, prec,
    s_msg, rs0, rxm, msg, msg_up, rx0, rx, mid, rxw, run, rtot,
    lsem, ssem, isend, irecv, msend, mrecv, dsend, drecv, wsend, wrecv,
    pssem, prsem, zsend, zrecv, hsend, tsend, trecv, upper_in, mem_in, want,
):
    columns, own, tgt, slots, tiles, members, reach = shape
    me = lax.axis_index("band")
    my_mem = lax.axis_index("mem")
    has_low = me > 0
    has_up = me < n - 1
    stride = n // 8
    via = (lax.axis_index("grp") == 0) & (my_mem == 0) & (lax.axis_index("fld") == 0)
    last = jnp.where(via, n, 2)
    first = stride
    fan = 2
    is_first = me <= first
    early = has_low & (me <= stride)
    late = jnp.logical_not(early)

    def band(o):
        return {"band": me + o}

    def remote(src, dst, send, recv, where):
        return pltpu.make_async_remote_copy(
            src_ref=src, dst_ref=dst, send_sem=send, recv_sem=recv,
            device_id=where, device_id_type=MESH,
        )

    def tell(sem, where):
        pl.semaphore_signal(sem, inc=1, device_id=where, device_id_type=MESH)

    barrier = pltpu.get_barrier_semaphore()

    def tell_band(q, carry):
        tell(barrier, {"band": q})
        return carry

    lax.fori_loop(me + 1, jnp.where(me == 0, 2, n), tell_band, 0)
    lax.fori_loop(jnp.where(me == 0, last, n), n, tell_band, 0)

    def tell_mem(m, carry):
        tell(barrier, {"mem": m})
        return carry

    lax.fori_loop(jnp.where(has_low, my_mem + 1, mems), mems, tell_mem, 0)

    loads = [
        pltpu.make_async_copy(block_of, idx.at[0:slots], lsem.at[0]),
        pltpu.make_async_copy(tile_of, idx.at[slots : 2 * slots], lsem.at[1]),
        pltpu.make_async_copy(live_in, idx.at[2 * slots : 2 * slots + 1], lsem.at[2]),
        pltpu.make_async_copy(area, am_v, lsem.at[3]),
        pltpu.make_async_copy(mask, mask_v, lsem.at[4]),
        pltpu.make_async_copy(tiles_in, w_v.at[0:tiles], lsem.at[5]),
        pltpu.make_async_copy(tarea, ta_v, lsem.at[6]),
    ]
    parts = 4
    width = own * 128 // parts
    pieces = [
        pltpu.make_async_copy(
            surf.at[:, q * width : (q + 1) * width],
            surf_v.at[:, q * width : (q + 1) * width],
            ssem.at[q],
        )
        for q in range(parts)
    ]
    for c in loads[:5] + pieces + loads[5:]:
        c.start()
    w_v[tiles] = jnp.zeros((128, 128), BF16)

    place = lax.broadcasted_iota(I32, (slots, tgt), 0)
    lane = lax.broadcasted_iota(I32, (slots, tgt), 1)
    scalars = [pltpu.make_async_copy(local.at[i], sm.at[i], lsem.at[i]) for i in range(3)]

    def make_local(i, word, shift, valid):
        block = (word & 255) + shift
        good = valid & (block >= 0) & (block < own)
        tile = jnp.where(good, word >> 8, tiles)
        local[i] = jnp.clip(block, 0, own - 1) + 256 * tile

    def own_lists():
        for c in loads[:3]:
            c.wait()
        alive = place < idx[2 * slots : 2 * slots + 1, :]
        word = idx[0:slots, :] + 256 * jnp.where(alive, idx[slots : 2 * slots, :], tiles)
        packed[...] = word
        make_local(0, word, -HALO, alive)
        scalars[0].start()

    def weigh(s, total):
        at = pl.ds(pl.multiple_of(s * 128, 128), 128)
        value = (am_v[pl.ds(s, 1), :] * surf_v[:, at].astype(F32)).astype(BF16)
        ext[s] = value
        return total + value.astype(F32)

    def local_part():
        loads[3].wait()
        loads[4].wait()
        am_v[...] = am_v[...] * mask_v[...].astype(F32)
        total = jnp.zeros((columns, 128), F32)
        for q in range(parts):
            pieces[q].wait()
            total = lax.fori_loop(q * own // parts, (q + 1) * own // parts, weigh, total, unroll=4)
        s_acc[...] = total
        loads[5].wait()
        loads[6].wait()

    def slot_sum(which, t):
        total = None
        for p in range(slots // 2):
            left, right = [], []
            for k in (2 * p, 2 * p + 1):
                word = sm[which, k, t]
                left.append(ext[word & 255])
                right.append(w_v[word >> 8])
            term = jnp.dot(
                jnp.concatenate(left, axis=1), jnp.concatenate(right, axis=0), preferred_element_type=F32
            )
            total = term if total is None else total + term
        return total

    def columns_of(t):
        return pl.ds(pl.multiple_of(t * 128, 128), 128)

    def own_targets():
        def body(t, carry):
            scaled[:, columns_of(t)] = slot_sum(0, t)
            return carry

        lax.fori_loop(0, tgt, body, 0)

    @pl.when(early)
    def _():
        own_lists()
        local_part()
        scalars[0].wait()
        own_targets()

    known = me - 1 + ((me == 1) | (me >= last)).astype(I32)

    @pl.when(has_low)
    def _():
        pl.semaphore_wait(barrier, known + my_mem)

    pl.when(has_low)(lambda: tell(upper_in.at[0], band(-1)))
    for o in range(2, stride):
        pl.when((me > o) & is_first)(functools.partial(tell, upper_in.at[o - 1], band(-o)))

    def ask():
        back = me - first - 1
        tell(want, {"band": first + 1 - fan + lax.rem(back, fan)})

    pl.when(jnp.logical_not(is_first))(ask)

    def tell_mem_back(m, carry):
        tell(mem_in.at[my_mem], {"mem": m})
        return carry

    lax.fori_loop(0, jnp.where(has_low, my_mem, 0), tell_mem_back, 0)

    pl.when(late)(own_lists)
    to_low = remote(packed, told.at[1], isend.at[0], irecv.at[0], band(-1))
    to_up = remote(packed, told.at[0], isend.at[1], irecv.at[1], band(1))
    pl.when(has_low)(to_low.start)

    def send_list_up():
        pl.semaphore_wait(upper_in.at[0], 1)
        to_up.start()

    pl.when(early)(send_list_up)
    pl.when(late)(local_part)

    ones = jnp.ones((8, 128), F32)
    s_row = row_dot(ones, s_acc[...], HIGHEST)[0:1]
    s_msg[...] = jnp.concatenate([s_row, jnp.zeros((1, 128 - columns), F32)], axis=1)

    first_row = remote(s_msg, rs0, zsend.at[0], zrecv.at[0], band(1))

    @pl.when(me == 0)
    def _():
        send_list_up()
        first_row.start()

    def from_mem(m, to):
        return remote(s_msg, rxm.at[m], msend.at[to], mrecv.at[m], {"mem": to})

    def others(action, which):
        for m in range(mems):
            pl.when(has_low & which(m))(functools.partial(action, m))

    def send_lower(m):
        from_mem(my_mem, m).start()

    others(send_lower, lambda m: (my_mem > m) & (me > 1))

    flat_w = w_v[0:tiles].reshape(tiles * 128, 128)
    sums = row_dot(jnp.ones((8, 128), BF16), flat_w)
    row_sums = jnp.concatenate([sums[0:1, q * 128 : (q + 1) * 128] for q in range(tiles)], axis=0)

    pl.when(late & has_low & has_up)(send_list_up)

    def cell_sums(word):
        row = jnp.concatenate([word[k : k + 1] for k in range(slots)], axis=1)
        count = slots * tgt
        at_block = (lax.broadcasted_iota(I32, (own, count), 0) == (row & 255)).astype(F32).astype(BF16)
        at_tile = (lax.broadcasted_iota(I32, (tiles, count), 0) == (row >> 8)).astype(F32).astype(BF16)
        return lax.dot_general(
            row_dot(at_block, at_tile), row_sums, (((1,), (0,)), ((), ())),
            preferred_element_type=F32, precision=HIGHEST,
        )

    def weigh_target(s, total):
        return total + ext[s].astype(F32) * reach_sum[pl.ds(s, 1), :]

    reach_sum[...] = cell_sums(local[0])
    t_acc = lax.fori_loop(0, own, weigh_target, jnp.zeros((columns, 128), F32), unroll=4)

    @pl.when(me == 1)
    def _():
        first_row.wait_recv()
        s_msg[...] = s_msg[...] + rs0[...]

    others(send_lower, lambda m: (my_mem > m) & (me == 1))
    pl.when(has_low)(to_up.wait_recv)
    pl.when(has_up)(to_low.wait_recv)

    def send_higher(m):
        pl.semaphore_wait(mem_in.at[m], 1)
        from_mem(my_mem, m).start()

    others(send_higher, lambda m: my_mem < m)

    from_low = (lane >= tgt - reach) & has_low
    from_up = (lane < reach) & has_up
    make_local(1, told[0], -(HALO + own), from_low)
    make_local(2, told[1], own - HALO, from_up)
    reach_sum[...] = cell_sums(jnp.where(lane < reach, local[2], local[1]))
    t_acc = lax.fori_loop(0, HALO, weigh_target, t_acc, unroll=4)
    t_acc = lax.fori_loop(own - HALO, own, weigh_target, t_acc, unroll=4)
    t_row = row_dot(ones, t_acc, HIGHEST)[0:1]
    scalars[1].start()
    scalars[2].start()

    chunk = 2

    def part_copy(side, j):
        at = pl.ds(chunk * j, chunk)
        return remote(
            psend.at[side, at], prec.at[1 - side, at], pssem.at[side, j], prsem.at[1 - side, j],
            band(2 * side - 1),
        )

    def for_side(side):
        def body(i, carry):
            psend[side, i] = slot_sum(1 + side, i + (tgt - reach if side == 0 else 0))

            @pl.when((i > 0) & (lax.rem(i, chunk) == 0))
            def _():
                part_copy(side, lax.div(i, chunk) - 1).start()

            return carry

        lax.fori_loop(0, reach, body, 0)
        part_copy(side, reach // chunk - 1).start()

    def for_neighbours():
        scalars[1].wait()
        scalars[2].wait()
        pl.when(has_low)(functools.partial(for_side, 0))
        pl.when(has_up)(functools.partial(for_side, 1))

    parts_first = early & jnp.logical_not(via)
    pl.when(parts_first)(for_neighbours)

    rxm[my_mem] = s_msg[...]
    others(lambda m: from_mem(m, m).wait_recv(), lambda m: my_mem != m)
    e_row = rxm[0]
    for m in range(1, mems):
        e_row = e_row + rxm[m]
    per = columns // members
    e_sum = e_row[:, 0:per]
    for m in range(1, members):
        e_sum = e_sum + e_row[:, m * per : (m + 1) * per]
    e_sum = jnp.where(has_low, e_sum, 0.0)
    a_sum = jnp.sum(jnp.sum(ta_v[...], axis=0, keepdims=True), axis=1, keepdims=True)
    a_high = jnp.round(a_sum * 64.0) * (1.0 / 64.0)
    s_parts, e_parts = in_three(s_row), in_three(e_sum)
    used = 4 * columns + 3 * per + 2
    msg[...] = jnp.concatenate(
        [s_parts[0], t_row, s_parts[1], s_parts[2], *e_parts, a_high, a_sum - a_high,
         jnp.zeros((1, WORDS - used), F32)],
        axis=1,
    )

    group = 4

    def direct(q):
        return remote(msg, rx.at[me], dsend.at[q], drecv.at[lax.div(me, group)], {"band": q})

    lowest = jnp.where((me == 1) | (me >= last), 0, 1)
    highest = jnp.minimum(me, first + 1)

    def send_down(q, carry):
        direct(q).start()
        return carry

    lax.fori_loop(lowest, highest, send_down, 0)

    from_first = remote(msg, rx0, zsend.at[1], zrecv.at[1], band(1))

    pl.when(me == 0)(from_first.start)

    pl.when(jnp.logical_not(parts_first))(for_neighbours)

    msg_up[...] = msg[...]

    @pl.when(me == 1)
    def _():
        from_first.wait_recv()
        msg_up[...] = msg[...] + rx0[...]

    ups = [remote(msg_up, rxw.at[o - 1], wsend.at[o - 1], wrecv.at[o - 1], band(o)) for o in range(1, stride)]

    def to_higher(o):
        return has_low & (me + o <= first)

    def send_up(o):
        if o > 1:
            pl.semaphore_wait(upper_in.at[o - 1], 1)
        ups[o - 1].start()

    for o in range(1, stride):
        pl.when(to_higher(o))(functools.partial(send_up, o))

    @pl.when(late)
    def _():
        scalars[0].wait()
        own_targets()


    run[...] = msg_up[...]

    def add_window(o):
        ups[o - 1].wait_recv()
        run[...] = run[...] + rxw[o - 1]

    for o in range(1, stride):
        pl.when((me > o) & is_first)(functools.partial(add_window, o))

    def add_part(side, start):
        def body(j, carry):
            part_copy(1 - side, j).wait_recv()
            for i in range(chunk):
                at = columns_of(start + chunk * j + i)
                scaled[:, at] = scaled[:, at] + prec[side, chunk * j + i]
            return carry

        lax.fori_loop(0, reach // chunk, body, 0)

    def divide(t, carry):
        at = columns_of(t)
        scaled[:, at] = scaled[:, at] / ta_v[pl.ds(t, 1), :]
        return carry

    pl.when(has_low)(functools.partial(add_part, 0, 0))
    pl.when(has_up)(functools.partial(add_part, 1, tgt - reach))
    lax.fori_loop(0, tgt, divide, 0)

    def sent(q, carry):
        direct(q).wait_send()
        return carry

    lax.fori_loop(lowest, highest, sent, 0)

    @pl.when(me == 0)
    def _():
        first_row.wait_send()
        from_first.wait_send()

    for o in range(1, stride):
        pl.when(to_higher(o))(ups[o - 1].wait_send)
    others(lambda m: from_mem(my_mem, m).wait_send(), lambda m: my_mem != m)

    def parts_sent(side):
        for j in range(reach // chunk):
            part_copy(side, j).wait_send()

    @pl.when(has_low)
    def _():
        to_low.wait_send()
        parts_sent(0)

    @pl.when(has_up)
    def _():
        to_up.wait_send()
        parts_sent(1)

    def arrived(start, count, g):
        at = rx.at[pl.ds(start, count)]
        remote(at, at, dsend.at[0], drecv.at[g], {"band": lax.rem(me + 1, n)}).wait_recv()
        for i in range(count):
            mid[...] = mid[...] + rx[start + i]

    mine = lax.div(me, group)
    near = jnp.where(via & (me == 0), 2, group - 1 - lax.rem(me, group))
    mid[...] = jnp.zeros((1, WORDS), F32)
    for count in range(1, group):
        pl.when(is_first & (near == count))(functools.partial(arrived, me + 1, count, mine))

    def add_group(g, carry):
        arrived(group * g, group, g)
        return carry

    no_more = (via & (me == 0)) | jnp.logical_not(is_first)
    lax.fori_loop(jnp.where(no_more, n // group, mine + 1), n // group, add_group, 0)

    hand = remote(mid, rx.at[2], hsend, drecv.at[0], band(-1))
    pl.when(via & (me == 1))(hand.start)
    run[...] = run[...] + mid[...]

    def total_to(p, words, to):
        return remote(words, to, tsend, trecv, {"band": p})

    def give(count):
        pl.semaphore_wait(want, count)
        for k in range(count):
            total_to(me + fan * (k + 1), run, rtot).start()

    rest = n - first - 1
    gives = [(me == first + 1 - fan + r, len(range(r, rest, fan))) for r in range(fan)]
    for mine_to_give, count in gives:
        pl.when(mine_to_give)(functools.partial(give, count))

    @pl.when(is_first)
    def _():
        tot_out[...] = run[...]

    @pl.when(jnp.logical_not(is_first))
    def _():
        total_to(me - 1, run, rtot).wait_recv()
        tot_out[...] = rtot[...]

    for mine_to_give, count in gives:
        pl.when(mine_to_give)(total_to(me + 1, rx.at[0:count], rx.at[0:count]).wait_send)
    pl.when(via & (me == 1))(hand.wait_send)


def last_kernel(shape, mems, tot, scaled, out, conserved, ensemble, done, mean_v, group_v, sems):
    columns, members, fields, snaps = shape
    per = columns // members

    def at(start, size):
        return tot[:, start : start + size]

    base = 4 * columns
    s = (at(0, columns) + at(2 * columns, columns)) + at(3 * columns, columns)
    e = (at(base, per) + at(base + per, per)) + at(base + 2 * per, per)
    total_area = at(base + 3 * per, 1) + at(base + 3 * per + 1, 1)
    step = (s - at(columns, columns)) / total_area
    diagonal = lax.broadcasted_iota(I32, (columns, columns), 0) == lax.broadcasted_iota(
        I32, (columns, columns), 1
    )
    fix = jnp.broadcast_to(jnp.sum(jnp.where(diagonal, step, 0.0), axis=1, keepdims=True), (columns, 128))
    mean = s / total_area
    for i in range(members * fields):
        mean_v[i // fields, i % fields : i % fields + 1, :] = mean[:, i * snaps : (i + 1) * snaps]
    group = e / total_area / float(members * mems)
    for f in range(fields):
        group_v[f : f + 1, :] = group[:, f * snaps : (f + 1) * snaps]
    pieces = 4
    copies = [
        pltpu.make_async_copy(mean_v, conserved, sems.at[pieces]),
        pltpu.make_async_copy(group_v, ensemble, sems.at[pieces + 1]),
    ]
    for q in range(pieces):
        rows = slice(q * columns // pieces, (q + 1) * columns // pieces)
        for b in range(out.shape[1] // 128):
            done[rows, b * 128 : (b + 1) * 128] = scaled[rows, b * 128 : (b + 1) * 128] + fix[rows]
        copies.append(pltpu.make_async_copy(done.at[rows], out.at[rows], sems.at[q]))
        copies[-1].start()
        if q == 0:
            copies[0].start()
            copies[1].start()
    for c in copies:
        c.wait()


def on_device(n, mems, surf, mask, area, tarea, tiles_in, tile_of, block_of, live):
    members, fields, snaps, cells = surf.shape
    columns = members * fields * snaps
    own = cells // 128
    tgt, slots = tile_of.shape
    tiles = tiles_in.shape[0]
    reach = HALO * tgt // own
    any_space = pl.BlockSpec(memory_space=pl.ANY)
    dma, plain = pltpu.SemaphoreType.DMA, pltpu.SemaphoreType.REGULAR
    rows = -(-(2 * slots + 1) // 8) * 8
    stride = n // 8
    scaled, tot = pl.pallas_call(
        functools.partial(main_kernel, n, mems, (columns, own, tgt, slots, tiles, members, reach)),
        out_shape=(pltpu.VMEM((columns, tgt * 128), F32), pltpu.VMEM((1, WORDS), F32)),
        in_specs=[any_space] * 8,
        out_specs=(pl.BlockSpec(memory_space=pltpu.VMEM),) * 2,
        scratch_shapes=[
            pltpu.VMEM((columns, cells), BF16),
            pltpu.VMEM((own, columns, 128), BF16),
            pltpu.VMEM((own, 128), F32),
            pltpu.VMEM((own, 128), I32),
            pltpu.VMEM((tgt, 128), F32),
            pltpu.VMEM((tiles + 1, 128, 128), BF16),
            pltpu.VMEM((rows, tgt), I32),
            pltpu.VMEM((slots, tgt), I32),
            pltpu.VMEM((2, slots, tgt), I32),
            pltpu.VMEM((3, slots, tgt), I32),
            pltpu.SMEM((3, slots, tgt), I32),
            pltpu.VMEM((columns, 128), F32),
            pltpu.VMEM((own, 128), F32),
            pltpu.VMEM((2, reach, columns, 128), F32),
            pltpu.VMEM((2, reach, columns, 128), F32),
            pltpu.VMEM((1, 128), F32),
            pltpu.VMEM((1, 128), F32),
            pltpu.VMEM((mems, 1, 128), F32),
            pltpu.VMEM((1, WORDS), F32),
            pltpu.VMEM((1, WORDS), F32),
            pltpu.VMEM((1, WORDS), F32),
            pltpu.VMEM((n, 1, WORDS), F32),
            pltpu.VMEM((1, WORDS), F32),
            pltpu.VMEM((stride - 1, 1, WORDS), F32),
            pltpu.VMEM((1, WORDS), F32),
            pltpu.VMEM((1, WORDS), F32),
            dma((7,)), dma((4,)), dma((2,)), dma((2,)), dma((mems,)), dma((mems,)),
            dma((stride + 1,)), dma((n // 4,)), dma((stride - 1,)), dma((stride - 1,)),
            dma((2, reach // 2)), dma((2, reach // 2)), dma((2,)), dma((2,)), dma,
            dma, dma, plain((stride - 1,)), plain((mems,)), plain,
        ],
        compiler_params=pltpu.CompilerParams(collective_id=0, has_side_effects=True),
        name="regrid",
    )(
        surf.reshape(columns, cells),
        area.reshape(own, 128),
        mask.reshape(own, 128),
        tarea.reshape(tgt, 128),
        tiles_in,
        tile_of.T,
        block_of.T,
        live.reshape(1, tgt),
    )
    inside = pl.BlockSpec(memory_space=pltpu.VMEM)
    out, conserved, ensemble = pl.pallas_call(
        functools.partial(last_kernel, (columns, members, fields, snaps), mems),
        out_shape=(
            jax.ShapeDtypeStruct((columns, tgt * 128), F32),
            jax.ShapeDtypeStruct((members, fields, snaps), F32),
            jax.ShapeDtypeStruct((fields, snaps), F32),
        ),
        in_specs=[inside, inside],
        out_specs=(any_space,) * 3,
        scratch_shapes=[
            pltpu.VMEM((columns, tgt * 128), F32),
            pltpu.VMEM((members, fields, snaps), F32),
            pltpu.VMEM((fields, snaps), F32),
            dma((6,)),
        ],
        compiler_params=pltpu.CompilerParams(vmem_limit_bytes=8 * 2**20),
        name="finish",
    )(tot, scaled)
    return out.reshape(members, fields, snaps, tgt * 128), conserved, ensemble


def solution(mesh):
    placed = (
        P(("grp", "mem"), "fld", None, "band"),
        P("band"),
        P("band"),
        P("band"),
        P(),
        P("band", None),
        P("band", None),
        P("band"),
    )
    return jax.shard_map(
        functools.partial(on_device, mesh.shape["band"], mesh.shape["mem"]),
        mesh=mesh,
        in_specs=placed,
        out_specs=(
            P(("grp", "mem"), "fld", None, "band"),
            P(("grp", "mem"), "fld", None),
            P(("grp", "fld"), None),
        ),
        check_vma=False,
    )
```

```python
import functools

import jax
import jax.numpy as jnp
from jax import lax
from jax.experimental import pallas as pl
from jax.experimental.pallas import tpu as pltpu
from jax.sharding import PartitionSpec as P

MESH = pl.DeviceIdType.MESH
HALO = 32
F32, BF16, I32 = jnp.float32, jnp.bfloat16, jnp.int32
HIGHEST = lax.Precision.HIGHEST
WORDS = 384


def row_dot(a, b, precision=None):
    return lax.dot_general(
        a, b, (((1,), (1,)), ((), ())), preferred_element_type=F32, precision=precision
    )


def in_three(x):
    high = jnp.round(x * 0.25) * 4.0
    rest = x - high
    mid = jnp.round(rest * 131072.0) * (1.0 / 131072.0)
    return high, mid, rest - mid


def main_kernel(
    n, mems, shape,
    surf, area, mask, tarea, tiles_in, tile_of, block_of, live_in,
    scaled, tot_out,
    surf_v, ext, am_v, mask_v, ta_v, w_v, idx, packed, told, local, sm, s_acc, reach_sum, psend, prec,
    s_msg, rs0, rxm, msg, msg_up, rx0, rx, mid, rxw, run, rtot,
    lsem, ssem, isend, irecv, msend, mrecv, dsend, drecv, wsend, wrecv,
    pssem, prsem, zsend, zrecv, hsend, tsend, trecv, upper_in, mem_in, want,
):
    columns, own, tgt, slots, tiles, members, reach = shape
    me = lax.axis_index("band")
    my_mem = lax.axis_index("mem")
    has_low = me > 0
    has_up = me < n - 1
    stride = n // 8
    via = (lax.axis_index("grp") == 0) & (my_mem == 0) & (lax.axis_index("fld") == 0)
    last = jnp.where(via, n, 2)
    first = stride
    fan = 2
    is_first = me <= first
    early = has_low & (me <= stride)
    late = jnp.logical_not(early)

    def band(o):
        return {"band": me + o}

    def remote(src, dst, send, recv, where):
        return pltpu.make_async_remote_copy(
            src_ref=src, dst_ref=dst, send_sem=send, recv_sem=recv,
            device_id=where, device_id_type=MESH,
        )

    def tell(sem, where):
        pl.semaphore_signal(sem, inc=1, device_id=where, device_id_type=MESH)

    barrier = pltpu.get_barrier_semaphore()

    def tell_band(q, carry):
        tell(barrier, {"band": q})
        return carry

    lax.fori_loop(me + 1, jnp.where(me == 0, 2, n), tell_band, 0)
    lax.fori_loop(jnp.where(me == 0, last, n), n, tell_band, 0)

    def tell_mem(m, carry):
        tell(barrier, {"mem": m})
        return carry

    lax.fori_loop(jnp.where(has_low, my_mem + 1, mems), mems, tell_mem, 0)

    loads = [
        pltpu.make_async_copy(block_of, idx.at[0:slots], lsem.at[0]),
        pltpu.make_async_copy(tile_of, idx.at[slots : 2 * slots], lsem.at[1]),
        pltpu.make_async_copy(live_in, idx.at[2 * slots : 2 * slots + 1], lsem.at[2]),
        pltpu.make_async_copy(area, am_v, lsem.at[3]),
        pltpu.make_async_copy(mask, mask_v, lsem.at[4]),
        pltpu.make_async_copy(tiles_in, w_v.at[0:tiles], lsem.at[5]),
        pltpu.make_async_copy(tarea, ta_v, lsem.at[6]),
    ]
    parts = 4
    width = own * 128 // parts
    pieces = [
        pltpu.make_async_copy(
            surf.at[:, q * width : (q + 1) * width],
            surf_v.at[:, q * width : (q + 1) * width],
            ssem.at[q],
        )
        for q in range(parts)
    ]
    for c in loads[:5] + pieces + loads[5:]:
        c.start()
    w_v[tiles] = jnp.zeros((128, 128), BF16)

    place = lax.broadcasted_iota(I32, (slots, tgt), 0)
    lane = lax.broadcasted_iota(I32, (slots, tgt), 1)
    scalars = [pltpu.make_async_copy(local.at[i], sm.at[i], lsem.at[i]) for i in range(3)]

    def make_local(i, word, shift, valid):
        block = (word & 255) + shift
        good = valid & (block >= 0) & (block < own)
        tile = jnp.where(good, word >> 8, tiles)
        local[i] = jnp.clip(block, 0, own - 1) + 256 * tile

    def own_lists():
        for c in loads[:3]:
            c.wait()
        alive = place < idx[2 * slots : 2 * slots + 1, :]
        word = idx[0:slots, :] + 256 * jnp.where(alive, idx[slots : 2 * slots, :], tiles)
        packed[...] = word
        make_local(0, word, -HALO, alive)
        scalars[0].start()

    def weigh(s, total):
        at = pl.ds(pl.multiple_of(s * 128, 128), 128)
        value = (am_v[pl.ds(s, 1), :] * surf_v[:, at].astype(F32)).astype(BF16)
        ext[s] = value
        return total + value.astype(F32)

    def local_part():
        loads[3].wait()
        loads[4].wait()
        am_v[...] = am_v[...] * mask_v[...].astype(F32)
        total = jnp.zeros((columns, 128), F32)
        for q in range(parts):
            pieces[q].wait()
            total = lax.fori_loop(q * own // parts, (q + 1) * own // parts, weigh, total, unroll=4)
        s_acc[...] = total
        loads[5].wait()
        loads[6].wait()

    def slot_sum(which, t):
        total = None
        for p in range(slots // 2):
            left, right = [], []
            for k in (2 * p, 2 * p + 1):
                word = sm[which, k, t]
                left.append(ext[word & 255])
                right.append(w_v[word >> 8])
            term = jnp.dot(
                jnp.concatenate(left, axis=1), jnp.concatenate(right, axis=0), preferred_element_type=F32
            )
            total = term if total is None else total + term
        return total

    def columns_of(t):
        return pl.ds(pl.multiple_of(t * 128, 128), 128)

    def own_targets():
        def body(t, carry):
            scaled[:, columns_of(t)] = slot_sum(0, t)
            return carry

        lax.fori_loop(0, tgt, body, 0)

    @pl.when(early)
    def _():
        own_lists()
        local_part()
        scalars[0].wait()
        own_targets()

    known = me - 1 + ((me == 1) | (me >= last)).astype(I32)

    @pl.when(has_low)
    def _():
        pl.semaphore_wait(barrier, known + my_mem)

    pl.when(has_low)(lambda: tell(upper_in.at[0], band(-1)))
    for o in range(2, stride):
        pl.when((me > o) & is_first)(functools.partial(tell, upper_in.at[o - 1], band(-o)))

    def ask():
        back = me - first - 1
        tell(want, {"band": first + 1 - fan + lax.rem(back, fan)})

    pl.when(jnp.logical_not(is_first))(ask)

    def tell_mem_back(m, carry):
        tell(mem_in.at[my_mem], {"mem": m})
        return carry

    lax.fori_loop(0, jnp.where(has_low, my_mem, 0), tell_mem_back, 0)

    pl.when(late)(own_lists)
    to_low = remote(packed, told.at[1], isend.at[0], irecv.at[0], band(-1))
    to_up = remote(packed, told.at[0], isend.at[1], irecv.at[1], band(1))
    pl.when(has_low)(to_low.start)

    def send_list_up():
        pl.semaphore_wait(upper_in.at[0], 1)
        to_up.start()

    pl.when(early)(send_list_up)
    pl.when(late)(local_part)

    ones = jnp.ones((8, 128), F32)
    s_row = row_dot(ones, s_acc[...], HIGHEST)[0:1]
    s_msg[...] = jnp.concatenate([s_row, jnp.zeros((1, 128 - columns), F32)], axis=1)

    first_row = remote(s_msg, rs0, zsend.at[0], zrecv.at[0], band(1))

    @pl.when(me == 0)
    def _():
        send_list_up()
        first_row.start()

    def from_mem(m, to):
        return remote(s_msg, rxm.at[m], msend.at[to], mrecv.at[m], {"mem": to})

    def others(action, which):
        for m in range(mems):
            pl.when(has_low & which(m))(functools.partial(action, m))

    def send_lower(m):
        from_mem(my_mem, m).start()

    others(send_lower, lambda m: (my_mem > m) & (me > 1))

    flat_w = w_v[0:tiles].reshape(tiles * 128, 128)
    sums = row_dot(jnp.ones((8, 128), BF16), flat_w)
    row_sums = jnp.concatenate([sums[0:1, q * 128 : (q + 1) * 128] for q in range(tiles)], axis=0)

    pl.when(late & has_low & has_up)(send_list_up)

    def cell_sums(word):
        row = jnp.concatenate([word[k : k + 1] for k in range(slots)], axis=1)
        count = slots * tgt
        at_block = (lax.broadcasted_iota(I32, (own, count), 0) == (row & 255)).astype(F32).astype(BF16)
        at_tile = (lax.broadcasted_iota(I32, (tiles, count), 0) == (row >> 8)).astype(F32).astype(BF16)
        return lax.dot_general(
            row_dot(at_block, at_tile), row_sums, (((1,), (0,)), ((), ())),
            preferred_element_type=F32, precision=HIGHEST,
        )

    def weigh_target(s, total):
        return total + ext[s].astype(F32) * reach_sum[pl.ds(s, 1), :]

    reach_sum[...] = cell_sums(local[0])
    t_acc = lax.fori_loop(0, own, weigh_target, jnp.zeros((columns, 128), F32), unroll=4)

    @pl.when(me == 1)
    def _():
        first_row.wait_recv()
        s_msg[...] = s_msg[...] + rs0[...]

    others(send_lower, lambda m: (my_mem > m) & (me == 1))

    def send_higher(m):
        pl.semaphore_wait(mem_in.at[m], 1)
        from_mem(my_mem, m).start()

    others(send_higher, lambda m: my_mem < m)
    pl.when(has_low)(to_up.wait_recv)
    pl.when(has_up)(to_low.wait_recv)

    from_low = (lane >= tgt - reach) & has_low
    from_up = (lane < reach) & has_up
    make_local(1, told[0], -(HALO + own), from_low)
    make_local(2, told[1], own - HALO, from_up)
    reach_sum[...] = cell_sums(jnp.where(lane < reach, local[2], local[1]))
    t_acc = lax.fori_loop(0, HALO, weigh_target, t_acc, unroll=4)
    t_acc = lax.fori_loop(own - HALO, own, weigh_target, t_acc, unroll=4)
    t_row = row_dot(ones, t_acc, HIGHEST)[0:1]
    scalars[1].start()
    scalars[2].start()

    chunk = 2

    def part_copy(side, j):
        at = pl.ds(chunk * j, chunk)
        return remote(
            psend.at[side, at], prec.at[1 - side, at], pssem.at[side, j], prsem.at[1 - side, j],
            band(2 * side - 1),
        )

    def for_side(side):
        def body(i, carry):
            psend[side, i] = slot_sum(1 + side, i + (tgt - reach if side == 0 else 0))

            @pl.when((i > 0) & (lax.rem(i, chunk) == 0))
            def _():
                part_copy(side, lax.div(i, chunk) - 1).start()

            return carry

        lax.fori_loop(0, reach, body, 0)
        part_copy(side, reach // chunk - 1).start()

    def for_neighbours():
        scalars[1].wait()
        scalars[2].wait()
        pl.when(has_low)(functools.partial(for_side, 0))
        pl.when(has_up)(functools.partial(for_side, 1))

    parts_first = early & jnp.logical_not(via)
    pl.when(parts_first)(for_neighbours)

    rxm[my_mem] = s_msg[...]
    others(lambda m: from_mem(m, m).wait_recv(), lambda m: my_mem != m)
    e_row = rxm[0]
    for m in range(1, mems):
        e_row = e_row + rxm[m]
    per = columns // members
    e_sum = e_row[:, 0:per]
    for m in range(1, members):
        e_sum = e_sum + e_row[:, m * per : (m + 1) * per]
    e_sum = jnp.where(has_low, e_sum, 0.0)
    a_sum = jnp.sum(jnp.sum(ta_v[...], axis=0, keepdims=True), axis=1, keepdims=True)
    a_high = jnp.round(a_sum * 64.0) * (1.0 / 64.0)
    s_parts, e_parts = in_three(s_row), in_three(e_sum)
    used = 4 * columns + 3 * per + 2
    msg[...] = jnp.concatenate(
        [s_parts[0], t_row, s_parts[1], s_parts[2], *e_parts, a_high, a_sum - a_high,
         jnp.zeros((1, WORDS - used), F32)],
        axis=1,
    )

    group = 4

    def direct(q):
        return remote(msg, rx.at[me], dsend.at[q], drecv.at[lax.div(me, group)], {"band": q})

    lowest = jnp.where((me == 1) | (me >= last), 0, 1)
    highest = jnp.minimum(me, first + 1)

    def send_down(q, carry):
        direct(q).start()
        return carry

    lax.fori_loop(lowest, highest, send_down, 0)

    from_first = remote(msg, rx0, zsend.at[1], zrecv.at[1], band(1))

    pl.when(me == 0)(from_first.start)

    pl.when(jnp.logical_not(parts_first))(for_neighbours)

    msg_up[...] = msg[...]

    @pl.when(me == 1)
    def _():
        from_first.wait_recv()
        msg_up[...] = msg[...] + rx0[...]

    ups = [remote(msg_up, rxw.at[o - 1], wsend.at[o - 1], wrecv.at[o - 1], band(o)) for o in range(1, stride)]

    def to_higher(o):
        return has_low & (me + o <= first)

    def send_up(o):
        if o > 1:
            pl.semaphore_wait(upper_in.at[o - 1], 1)
        ups[o - 1].start()

    for o in range(1, stride):
        pl.when(to_higher(o))(functools.partial(send_up, o))

    @pl.when(late)
    def _():
        scalars[0].wait()
        own_targets()


    run[...] = msg_up[...]

    def add_window(o):
        ups[o - 1].wait_recv()
        run[...] = run[...] + rxw[o - 1]

    for o in range(1, stride):
        pl.when((me > o) & is_first)(functools.partial(add_window, o))

    def arrived(start, count, g):
        at = rx.at[pl.ds(start, count)]
        remote(at, at, dsend.at[0], drecv.at[g], {"band": lax.rem(me + 1, n)}).wait_recv()
        for i in range(count):
            mid[...] = mid[...] + rx[start + i]

    def gather():
        mine = lax.div(me, group)
        near = jnp.where(via & (me == 0), 2, group - 1 - lax.rem(me, group))
        mid[...] = jnp.zeros((1, WORDS), F32)
        for count in range(1, group):
            pl.when(is_first & (near == count))(functools.partial(arrived, me + 1, count, mine))

        def add_group(g, carry):
            arrived(group * g, group, g)
            return carry

        no_more = (via & (me == 0)) | jnp.logical_not(is_first)
        lax.fori_loop(jnp.where(no_more, n // group, mine + 1), n // group, add_group, 0)

    hands = via & (me == 1)
    hand = remote(mid, rx.at[2], hsend, drecv.at[0], band(-1))

    @pl.when(hands)
    def _():
        gather()
        hand.start()

    def add_part(side, start):
        def body(j, carry):
            part_copy(1 - side, j).wait_recv()
            for i in range(chunk):
                at = columns_of(start + chunk * j + i)
                scaled[:, at] = scaled[:, at] + prec[side, chunk * j + i]
            return carry

        lax.fori_loop(0, reach // chunk, body, 0)

    def divide(t, carry):
        at = columns_of(t)
        scaled[:, at] = scaled[:, at] / ta_v[pl.ds(t, 1), :]
        return carry

    pl.when(has_low)(functools.partial(add_part, 0, 0))
    pl.when(has_up)(functools.partial(add_part, 1, tgt - reach))
    lax.fori_loop(0, tgt, divide, 0)

    def sent(q, carry):
        direct(q).wait_send()
        return carry

    lax.fori_loop(lowest, highest, sent, 0)

    @pl.when(me == 0)
    def _():
        first_row.wait_send()
        from_first.wait_send()

    for o in range(1, stride):
        pl.when(to_higher(o))(ups[o - 1].wait_send)
    others(lambda m: from_mem(my_mem, m).wait_send(), lambda m: my_mem != m)

    def parts_sent(side):
        for j in range(reach // chunk):
            part_copy(side, j).wait_send()

    @pl.when(has_low)
    def _():
        to_low.wait_send()
        parts_sent(0)

    @pl.when(has_up)
    def _():
        to_up.wait_send()
        parts_sent(1)

    pl.when(jnp.logical_not(hands))(gather)
    run[...] = run[...] + mid[...]

    def total_to(p, words, to):
        return remote(words, to, tsend, trecv, {"band": p})

    def give(count):
        pl.semaphore_wait(want, count)
        for k in range(count):
            total_to(me + fan * (k + 1), run, rtot).start()

    rest = n - first - 1
    gives = [(me == first + 1 - fan + r, len(range(r, rest, fan))) for r in range(fan)]
    for mine_to_give, count in gives:
        pl.when(mine_to_give)(functools.partial(give, count))

    @pl.when(is_first)
    def _():
        tot_out[...] = run[...]

    @pl.when(jnp.logical_not(is_first))
    def _():
        total_to(me - 1, run, rtot).wait_recv()
        tot_out[...] = rtot[...]

    for mine_to_give, count in gives:
        pl.when(mine_to_give)(total_to(me + 1, rx.at[0:count], rx.at[0:count]).wait_send)
    pl.when(hands)(hand.wait_send)


def last_kernel(shape, mems, tot, scaled, out, conserved, ensemble, done, mean_v, group_v, sems):
    columns, members, fields, snaps = shape
    per = columns // members

    def at(start, size):
        return tot[:, start : start + size]

    base = 4 * columns
    s = (at(0, columns) + at(2 * columns, columns)) + at(3 * columns, columns)
    e = (at(base, per) + at(base + per, per)) + at(base + 2 * per, per)
    total_area = at(base + 3 * per, 1) + at(base + 3 * per + 1, 1)
    step = (s - at(columns, columns)) / total_area
    diagonal = lax.broadcasted_iota(I32, (columns, columns), 0) == lax.broadcasted_iota(
        I32, (columns, columns), 1
    )
    fix = jnp.broadcast_to(jnp.sum(jnp.where(diagonal, step, 0.0), axis=1, keepdims=True), (columns, 128))
    mean = s / total_area
    for i in range(members * fields):
        mean_v[i // fields, i % fields : i % fields + 1, :] = mean[:, i * snaps : (i + 1) * snaps]
    group = e / total_area / float(members * mems)
    for f in range(fields):
        group_v[f : f + 1, :] = group[:, f * snaps : (f + 1) * snaps]
    pieces = 4
    copies = [
        pltpu.make_async_copy(mean_v, conserved, sems.at[pieces]),
        pltpu.make_async_copy(group_v, ensemble, sems.at[pieces + 1]),
    ]
    for q in range(pieces):
        rows = slice(q * columns // pieces, (q + 1) * columns // pieces)
        for b in range(out.shape[1] // 128):
            done[rows, b * 128 : (b + 1) * 128] = scaled[rows, b * 128 : (b + 1) * 128] + fix[rows]
        copies.append(pltpu.make_async_copy(done.at[rows], out.at[rows], sems.at[q]))
        copies[-1].start()
        if q == 0:
            copies[0].start()
            copies[1].start()
    for c in copies:
        c.wait()


def on_device(n, mems, surf, mask, area, tarea, tiles_in, tile_of, block_of, live):
    members, fields, snaps, cells = surf.shape
    columns = members * fields * snaps
    own = cells // 128
    tgt, slots = tile_of.shape
    tiles = tiles_in.shape[0]
    reach = HALO * tgt // own
    any_space = pl.BlockSpec(memory_space=pl.ANY)
    dma, plain = pltpu.SemaphoreType.DMA, pltpu.SemaphoreType.REGULAR
    rows = -(-(2 * slots + 1) // 8) * 8
    stride = n // 8
    scaled, tot = pl.pallas_call(
        functools.partial(main_kernel, n, mems, (columns, own, tgt, slots, tiles, members, reach)),
        out_shape=(pltpu.VMEM((columns, tgt * 128), F32), pltpu.VMEM((1, WORDS), F32)),
        in_specs=[any_space] * 8,
        out_specs=(pl.BlockSpec(memory_space=pltpu.VMEM),) * 2,
        scratch_shapes=[
            pltpu.VMEM((columns, cells), BF16),
            pltpu.VMEM((own, columns, 128), BF16),
            pltpu.VMEM((own, 128), F32),
            pltpu.VMEM((own, 128), I32),
            pltpu.VMEM((tgt, 128), F32),
            pltpu.VMEM((tiles + 1, 128, 128), BF16),
            pltpu.VMEM((rows, tgt), I32),
            pltpu.VMEM((slots, tgt), I32),
            pltpu.VMEM((2, slots, tgt), I32),
            pltpu.VMEM((3, slots, tgt), I32),
            pltpu.SMEM((3, slots, tgt), I32),
            pltpu.VMEM((columns, 128), F32),
            pltpu.VMEM((own, 128), F32),
            pltpu.VMEM((2, reach, columns, 128), F32),
            pltpu.VMEM((2, reach, columns, 128), F32),
            pltpu.VMEM((1, 128), F32),
            pltpu.VMEM((1, 128), F32),
            pltpu.VMEM((mems, 1, 128), F32),
            pltpu.VMEM((1, WORDS), F32),
            pltpu.VMEM((1, WORDS), F32),
            pltpu.VMEM((1, WORDS), F32),
            pltpu.VMEM((n, 1, WORDS), F32),
            pltpu.VMEM((1, WORDS), F32),
            pltpu.VMEM((stride - 1, 1, WORDS), F32),
            pltpu.VMEM((1, WORDS), F32),
            pltpu.VMEM((1, WORDS), F32),
            dma((7,)), dma((4,)), dma((2,)), dma((2,)), dma((mems,)), dma((mems,)),
            dma((stride + 1,)), dma((n // 4,)), dma((stride - 1,)), dma((stride - 1,)),
            dma((2, reach // 2)), dma((2, reach // 2)), dma((2,)), dma((2,)), dma,
            dma, dma, plain((stride - 1,)), plain((mems,)), plain,
        ],
        compiler_params=pltpu.CompilerParams(collective_id=0, has_side_effects=True),
        name="regrid",
    )(
        surf.reshape(columns, cells),
        area.reshape(own, 128),
        mask.reshape(own, 128),
        tarea.reshape(tgt, 128),
        tiles_in,
        tile_of.T,
        block_of.T,
        live.reshape(1, tgt),
    )
    inside = pl.BlockSpec(memory_space=pltpu.VMEM)
    out, conserved, ensemble = pl.pallas_call(
        functools.partial(last_kernel, (columns, members, fields, snaps), mems),
        out_shape=(
            jax.ShapeDtypeStruct((columns, tgt * 128), F32),
            jax.ShapeDtypeStruct((members, fields, snaps), F32),
            jax.ShapeDtypeStruct((fields, snaps), F32),
        ),
        in_specs=[inside, inside],
        out_specs=(any_space,) * 3,
        scratch_shapes=[
            pltpu.VMEM((columns, tgt * 128), F32),
            pltpu.VMEM((members, fields, snaps), F32),
            pltpu.VMEM((fields, snaps), F32),
            dma((6,)),
        ],
        compiler_params=pltpu.CompilerParams(vmem_limit_bytes=8 * 2**20),
        name="finish",
    )(tot, scaled)
    return out.reshape(members, fields, snaps, tgt * 128), conserved, ensemble


def solution(mesh):
    placed = (
        P(("grp", "mem"), "fld", None, "band"),
        P("band"),
        P("band"),
        P("band"),
        P(),
        P("band", None),
        P("band", None),
        P("band"),
    )
    return jax.shard_map(
        functools.partial(on_device, mesh.shape["band"], mesh.shape["mem"]),
        mesh=mesh,
        in_specs=placed,
        out_specs=(
            P(("grp", "mem"), "fld", None, "band"),
            P(("grp", "mem"), "fld", None),
            P(("grp", "fld"), None),
        ),
        check_vma=False,
    )
```
